32 devices in a mesh: blk: 16 (over z, y, x), obs: 2 (over core).
Axes of the slice: x: 2, y: 2, z: 4, core: 2. Of those that a mesh axis runs over, the one named last changes fastest.
Arguments:
- populations: float32 [16, 19, 32, 1024], P('blk', None, 'obs'), may hold values from 0.011111111 to 0.533333333, as said below
- block_faces: int32 [16, 4], P('blk'), may hold values from 0 to 15, as said below
- block_edges: int32 [16, 4], P('blk'), may hold values from 0 to 15, as said below
- probe_cell: int32 [4096], P(('blk', 'obs')), may hold values from 0 to 16383
- history: bfloat16 [4096, 512], P(('blk', 'obs')), may hold values from -6 to 6
- panel_count: int32 [32], P(('blk', 'obs')), may hold values from 0 to 128, as said below
- panel_owner: int32 [4096], P(('blk', 'obs')), may hold values from 0 to 1023, as said below
- panel_pos: bfloat16 [3, 2048], P(None, ('blk', 'obs')), may hold values from -1 to 1
- panel_normal: bfloat16 [3, 2048], P(None, ('blk', 'obs')), may hold values from -0.625 to 0.625
- observers: float32 [3, 1024], P(None, 'obs'), may hold values from -8 to 8, as said below
Outputs:
- populations_out: float32 [16, 19, 32, 1024], P('blk', None, 'obs')
- spectrum: float32 [2, 512, 128], P('obs', 'blk')
The draws below stay inside these ranges and needn't reach their ends.
Inputs may be any that keep to these rules, and one draw needn't show every extreme that they name: `populations`: every population is positive. The blocks form a lattice of 4 by 4 blocks along y and z, periodic in both, one block deep in x; block_faces[b] names the blocks beside b at -y, +y, -z, +z. block_edges[b] names the blocks at (-y,-z), (-y,+z), (+y,-z), (+y,+z) of b: the y neighbour's z neighbour, which is the z neighbour's y neighbour. The eight face and edge neighbours of a block are distinct and differ from it. The live slots of a device are its first panel_count slots. The counts of the devices at one obs index sum to 1024. `panel_owner`: in a live slot of the device at blk index b and obs index o the value is q * 64 + j: slot j of the owner at blk index q and the same obs index. Every owner slot receives exactly one live panel. A device sends at most 8 live panels to one owner, and its live panels go to the owners in numbers that differ by at most one. Dead slots hold arbitrary values of the range. `observers`: every observer lies at a distance of 4 to 8 from the anchor (0, 0, 0).
All inputs are finite; a program needn't handle non-finite values.
Results may differ from the reference program's by a relative error of at most 0.0032.
The reference program's roundings to bfloat16 on the way (of `recent`, `owned`, `transform_table` and `spectra`) count: a program that leaves them out, or rounds other values in their place, can miss the bound.
Values may be sent and summed in bfloat16 or wider, within the bound.
A program may use at most 128 MiB of HBM per device.

```python
import math
import jax
import jax.numpy as jnp
from jax import lax

BS = 32
STEPS = 4
LZ = 4
SAMPLES = 256
BINS = 64
OBSERVERS = 1024
P_OWN = 64
BLOCKS = 16
LY = 4
SLAB = 16
S_DEV = 128
PANELS = 2048
SLOTS = 4096
N_OBS = 2


velocity_list = [(0, 0, 0), (1, 0, 0), (-1, 0, 0), (0, 1, 0), (0, -1, 0), (0, 0, 1), (0, 0, -1), (1, 1, 0), (-1, -1, 0), (1, -1, 0), (-1, 1, 0), (1, 0, 1), (-1, 0, -1), (1, 0, -1), (-1, 0, 1), (0, 1, 1), (0, -1, -1), (0, 1, -1), (0, -1, 1)]


weight_list = [1.0 / 3.0] + [1.0 / 18.0] * 6 + [1.0 / 36.0] * 12


def draw_populations(key, part):
    shape = (BLOCKS, 19, BS, BS * BS)
    weights = jnp.array(weight_list, jnp.float32)[None, :, None, None]
    noise = jnp.clip(jax.random.normal(key, shape, jnp.float32), -6.0, 6.0)
    return weights * (1.0 + 0.1 * noise)


def lattice(key):
    order = jax.random.permutation(jax.random.fold_in(key, 11), BLOCKS).astype(jnp.int32)
    placed = jnp.argsort(order).astype(jnp.int32)
    row_index = placed // LZ
    column_index = placed % LZ

    def beside(move_y, move_z):
        return order[(row_index + move_y) % LY * LZ + (column_index + move_z) % LZ]
    faces_list = jnp.stack([beside(-1, 0), beside(1, 0), beside(0, -1), beside(0, 1)], axis=1)
    edges_list = jnp.stack([beside(-1, -1), beside(-1, 1), beside(1, -1), beside(1, 1)], axis=1)
    return (faces_list.astype(jnp.int32), edges_list.astype(jnp.int32))


def draw_block_faces(key, part):
    return lattice(key)[0]


def draw_block_edges(key, part):
    return lattice(key)[1]


def ownership(key):
    groups = SLOTS // (S_DEV * BLOCKS)

    def one_group(subkey):
        shuffle = jax.random.permutation(jax.random.fold_in(subkey, 1), BLOCKS).astype(jnp.int32)
        halves = BLOCKS // 2
        surplus = jax.random.randint(jax.random.fold_in(subkey, 2), (halves,), 0, P_OWN + 1).astype(jnp.int32)
        surplus = surplus.at[0].set(P_OWN)
        paired = jnp.concatenate([P_OWN + surplus, P_OWN - surplus]).astype(jnp.int32)
        counts = jnp.zeros((BLOCKS,), jnp.int32).at[shuffle].set(paired)
        starts = jnp.cumsum(counts) - counts
        slot_index = jnp.arange(S_DEV, dtype=jnp.int32)
        global_rank = starts[:, None] + slot_index[None, :]
        alive_slot = slot_index[None, :] < counts[:, None]
        relabel = jax.random.permutation(jax.random.fold_in(subkey, 3), BLOCKS).astype(jnp.int32)
        spots = jax.random.permutation(jax.random.fold_in(subkey, 4), P_OWN).astype(jnp.int32)
        target = relabel[global_rank % BLOCKS]
        position = spots[jnp.minimum(global_rank // BLOCKS, P_OWN - 1)]
        filler = jax.random.randint(jax.random.fold_in(subkey, 5), (BLOCKS, S_DEV), 0, BLOCKS * P_OWN).astype(jnp.int32)
        owners = jnp.where(alive_slot, target * P_OWN + position, filler).astype(jnp.int32)
        return (counts, owners)
    counts, owners = jax.vmap(one_group)(jax.random.split(jax.random.fold_in(key, 23), groups))
    counts = counts.transpose(1, 0).reshape(-1).astype(jnp.int32)
    owners = owners.transpose(1, 0, 2).reshape(-1).astype(jnp.int32)
    return (counts, owners)


def draw_panel_count(key, part):
    return ownership(key)[0]


def draw_panel_owner(key, part):
    return ownership(key)[1]


def draw_observers(key, part):
    first_key, second_key, third_key = jax.random.split(key, 3)
    radius = jax.random.uniform(first_key, (OBSERVERS,), jnp.float32, 4.0, 8.0)
    height = jax.random.uniform(second_key, (OBSERVERS,), jnp.float32, -1.0, 1.0)
    heading = jax.random.uniform(third_key, (OBSERVERS,), jnp.float32, 0.0, 2.0 * math.pi)
    spread = jnp.sqrt(jnp.maximum(1.0 - height * height, 0.0))
    return jnp.stack([radius * spread * jnp.cos(heading), radius * spread * jnp.sin(heading), radius * height])


def with_ends(drawn, own_key, least, largest):
    spot = [jax.random.randint(jax.random.fold_in(own_key, axis), (), 0, length) for axis, length in enumerate(drawn.shape)]
    longest = drawn.shape.index(max(drawn.shape))
    neighbour = spot[:longest] + [(spot[longest] + 1) % drawn.shape[longest]] + spot[longest + 1:]
    return drawn.at[tuple(spot)].set(least).at[tuple(neighbour)].set(largest)


def block_levels(key, dims, cuts, low, largest):
    level = 1.0
    for dim, blocks in cuts:
        heights = jax.random.uniform(jax.random.fold_in(jax.random.fold_in(key, 6), dim), (blocks,), jnp.float32, low / len(cuts), largest / len(cuts))
        level = level * jnp.repeat(jnp.exp(heights), dims[dim] // blocks).reshape((-1,) + (1,) * (len(dims) - 1 - dim))
    return level


def normal_values(own_key, dims, deviation, most, pieces=(), kind=jnp.bfloat16):
    result = jax.random.normal(own_key, dims, jnp.float32) * deviation
    if len(pieces) > 0:
        result = block_levels(own_key, dims, pieces, -0.22, 0.18) * result
    return jnp.clip(result, min=-most, max=most).astype(kind)


def setup_inputs(seed: int = 0) -> dict:
    splits = jax.random.split(jax.random.key(seed), 11)
    return {
        "populations": draw_populations(jax.random.fold_in(splits[10], 71), 0),
        "block_faces": draw_block_faces(jax.random.fold_in(splits[10], 71), 0),
        "block_edges": draw_block_edges(jax.random.fold_in(splits[10], 71), 0),
        "probe_cell": with_ends(jax.random.randint(splits[3], (SLOTS,), 0, SLAB * BS * BS), jax.random.fold_in(splits[3], 1), 0, (SLAB * BS * BS) - 1).astype(jnp.int32),
        "history": normal_values(splits[4], (SLOTS, 2 * SAMPLES), 1.0, 6.0, ((0, 32),)),
        "panel_count": draw_panel_count(jax.random.fold_in(splits[10], 71), 0),
        "panel_owner": draw_panel_owner(jax.random.fold_in(splits[10], 71), 0),
        "panel_pos": jnp.clip(jax.random.uniform(splits[7], (3, PANELS), jnp.float32, -1.0, 1.0) * block_levels(splits[7], (3, PANELS), ((1, 32),), -0.4, 0.0), -1.0, 1.0).astype(jnp.bfloat16),
        "panel_normal": normal_values(splits[8], (3, PANELS), (2.0 / PANELS ** 0.5), 0.625, ((1, 32),)),
        "observers": draw_observers(jax.random.fold_in(splits[10], 71), 0),
    }


velocity_list = [(0, 0, 0), (1, 0, 0), (-1, 0, 0), (0, 1, 0), (0, -1, 0), (0, 0, 1), (0, 0, -1), (1, 1, 0), (-1, -1, 0), (1, -1, 0), (-1, 1, 0), (1, 0, 1), (-1, 0, -1), (1, 0, -1), (-1, 0, 1), (0, 1, 1), (0, -1, -1), (0, 1, -1), (0, -1, 1)]
weight_list = [1.0 / 3.0] + [1.0 / 18.0] * 6 + [1.0 / 36.0] * 12
relax_rate = 1.6
pressure_gain = 60.0
sound_speed = 0.5

def component(axis_number, extra):
    values = jnp.array([velocity[axis_number] for velocity in velocity_list], jnp.float32)
    return values.reshape((19,) + extra)

def collide(field):
    extra = (1,) * (field.ndim - 1)
    along_x = component(0, extra)
    along_y = component(1, extra)
    along_z = component(2, extra)
    weights = jnp.array(weight_list, jnp.float32).reshape((19,) + extra)
    density = lax.optimization_barrier(jnp.sum(field, axis=0))
    speed_x = lax.optimization_barrier(jnp.sum(along_x * field, axis=0)) / density
    speed_y = lax.optimization_barrier(jnp.sum(along_y * field, axis=0)) / density
    speed_z = lax.optimization_barrier(jnp.sum(along_z * field, axis=0)) / density
    projected = along_x * speed_x + along_y * speed_y + along_z * speed_z
    squared = speed_x * speed_x + speed_y * speed_y + speed_z * speed_z
    equilibrium = weights * density * (1.0 + 3.0 * projected + 4.5 * projected * projected - 1.5 * squared)
    return field + relax_rate * (equilibrium - field)

def propagate(padded):
    width_x = padded.shape[1] - 2
    width_y = padded.shape[2] - 2
    width_z = padded.shape[3] - 2
    parts = []
    for number, velocity in enumerate(velocity_list):
        shift_x, shift_y, shift_z = velocity
        parts.append(padded[number, 1 - shift_x:1 - shift_x + width_x, 1 - shift_y:1 - shift_y + width_y, 1 - shift_z:1 - shift_z + width_z])
    return jnp.stack(parts)

def pad_blocks(collided, block_faces, block_edges):
    top_index = BS - 1
    wrapped = jnp.concatenate([collided[:, :, -1:], collided, collided[:, :, :1]], axis=2)
    below_rows = wrapped[:, :, :, top_index:BS, :][block_faces[:, 0]]
    above_rows = wrapped[:, :, :, 0:1, :][block_faces[:, 1]]
    tall_block = jnp.concatenate([below_rows, wrapped, above_rows], axis=3)
    near_core = wrapped[:, :, :, :, top_index:BS][block_faces[:, 2]]
    far_core = wrapped[:, :, :, :, 0:1][block_faces[:, 3]]
    corner_ll = wrapped[:, :, :, top_index:BS, top_index:BS][block_edges[:, 0]]
    corner_lh = wrapped[:, :, :, top_index:BS, 0:1][block_edges[:, 1]]
    corner_hl = wrapped[:, :, :, 0:1, top_index:BS][block_edges[:, 2]]
    corner_hh = wrapped[:, :, :, 0:1, 0:1][block_edges[:, 3]]
    near_plane = jnp.concatenate([corner_ll, near_core, corner_hl], axis=3)
    far_plane = jnp.concatenate([corner_lh, far_core, corner_hh], axis=3)
    return jnp.concatenate([near_plane, tall_block, far_plane], axis=4)

def transform_table():
    moments = jnp.arange(SAMPLES, dtype=jnp.int32)[:, None]
    harmonics = jnp.arange(BINS, dtype=jnp.int32)[None, :] + 1
    turns = moments * harmonics % SAMPLES
    phases = turns.astype(jnp.float32) * (2.0 * math.pi / SAMPLES)
    return jnp.concatenate([jnp.cos(phases), -jnp.sin(phases)], axis=1).astype(jnp.bfloat16)

def radiate(spectra, place, normal, listen):
    values = spectra.astype(jnp.float32)
    press_real = values[0:BINS].T
    press_imag = values[BINS:2 * BINS].T
    rate_real = values[2 * BINS:3 * BINS].T
    rate_imag = values[3 * BINS:4 * BINS].T
    offsets = listen[:, None, :] - place.astype(jnp.float32)[:, :, None]
    distance_sq = lax.optimization_barrier(jnp.sum(offsets * offsets, axis=0))
    distance = jnp.sqrt(distance_sq)
    facing = lax.optimization_barrier(jnp.sum(normal.astype(jnp.float32)[:, :, None] * offsets, axis=0))
    far_term = facing / (4.0 * math.pi * sound_speed * distance_sq)
    near_term = facing / (4.0 * math.pi * distance_sq * distance)
    angular = (jnp.arange(BINS, dtype=jnp.float32) + 1.0) * (2.0 * math.pi / SAMPLES)
    phases = angular[None, :, None] * (distance / sound_speed)[:, None, :]
    cosine = jnp.cos(phases)
    sine_part = jnp.sin(phases)
    weight_real = far_term[:, None, :] * rate_real[:, :, None] + near_term[:, None, :] * press_real[:, :, None]
    weight_imag = far_term[:, None, :] * rate_imag[:, :, None] + near_term[:, None, :] * press_imag[:, :, None]
    real_part = lax.optimization_barrier(jnp.sum(weight_real * cosine + weight_imag * sine_part, axis=0))
    imag_part = lax.optimization_barrier(jnp.sum(weight_imag * cosine - weight_real * sine_part, axis=0))
    return jnp.concatenate([real_part, imag_part], axis=0).T

def reference(populations, block_faces, block_edges, probe_cell, history, panel_count, panel_owner, panel_pos, panel_normal, observers):
    field = populations.reshape(BLOCKS, 19, BS, BS, BS)
    device_of = jnp.arange(SLOTS, dtype=jnp.int32) // S_DEV
    block_of = device_of // N_OBS
    group_of = device_of % N_OBS
    depth = group_of * (BS // N_OBS) + probe_cell // (BS * BS)
    across = probe_cell % (BS * BS)
    readings = []
    for turn_index in range(STEPS):
        collided = jax.vmap(collide)(field)
        field = jax.vmap(propagate)(pad_blocks(collided, block_faces, block_edges))
        density = lax.optimization_barrier(jnp.sum(field, axis=1)).reshape(BLOCKS, BS, BS * BS)
        readings.append(density[block_of, depth, across])
    gained = pressure_gain * (jnp.stack(readings, axis=1) - 1.0)
    previous = jnp.concatenate([history[:, SAMPLES - 1:SAMPLES].astype(jnp.float32), gained[:, :-1]], axis=1)
    rate_values = gained - previous
    recent = jnp.concatenate([history[:, STEPS:SAMPLES], gained.astype(jnp.bfloat16), history[:, SAMPLES + STEPS:], rate_values.astype(jnp.bfloat16)], axis=1)
    slot_local = jnp.arange(SLOTS, dtype=jnp.int32) % S_DEV
    alive_slot = slot_local < panel_count[device_of]
    target = (panel_owner // P_OWN * N_OBS + group_of) * P_OWN + panel_owner % P_OWN
    target = jnp.where(alive_slot, target, PANELS).astype(jnp.int32)
    owned = jnp.zeros((PANELS, 2 * SAMPLES), jnp.bfloat16).at[target].set(recent, mode='drop')
    spectra = jnp.dot(owned.reshape(PANELS * 2, SAMPLES), transform_table(), preferred_element_type=jnp.float32).astype(jnp.bfloat16).reshape(PANELS, 4 * BINS)
    block_size = 256 if PANELS % 256 == 0 else PANELS
    counted = PANELS // block_size
    spectra_blocks = spectra.T.reshape(4 * BINS, counted, block_size).transpose(1, 0, 2)
    place_blocks = panel_pos.reshape(3, counted, block_size).transpose(1, 0, 2)
    normal_blocks = panel_normal.reshape(3, counted, block_size).transpose(1, 0, 2)

    def accumulate(total, inputs):
        return (total + radiate(inputs[0], inputs[1], inputs[2], observers), None)
    total, unused_out = lax.scan(accumulate, jnp.zeros((OBSERVERS, 2 * BINS), jnp.float32), (spectra_blocks, place_blocks, normal_blocks))
    return (field.reshape(BLOCKS, 19, BS, BS * BS), total.reshape(N_OBS, OBSERVERS // N_OBS, 2 * BINS))
```

```python
import functools
import math

import jax
import jax.numpy as jnp
from jax import lax
from jax.experimental import pallas as pl
from jax.experimental.pallas import tpu as pltpu
from jax.sharding import PartitionSpec as P

BS = 32
STEPS = 4
SAMPLES = 256
BINS = 64
P_OWN = 64


velocity_list = [
    (0, 0, 0),
    (1, 0, 0),
    (-1, 0, 0),
    (0, 1, 0),
    (0, -1, 0),
    (0, 0, 1),
    (0, 0, -1),
    (1, 1, 0),
    (-1, -1, 0),
    (1, -1, 0),
    (-1, 1, 0),
    (1, 0, 1),
    (-1, 0, -1),
    (1, 0, -1),
    (-1, 0, 1),
    (0, 1, 1),
    (0, -1, -1),
    (0, 1, -1),
    (0, -1, 1),
]
weight_list = [1.0 / 3.0] + [1.0 / 18.0] * 6 + [1.0 / 36.0] * 12
x_moving = [1, 2, 7, 8, 9, 10, 11, 12, 13, 14]
y_upward = [3, 7, 10, 15, 17]
y_downward = [4, 8, 9, 16, 18]
z_upward = [5, 11, 14, 15, 18]
z_downward = [6, 12, 13, 16, 17]
relax_rate = 1.6
pressure_gain = 60.0
sound_speed = 0.5


x_plus = [1, 7, 9, 11, 13]
x_minus = [2, 8, 10, 12, 14]
x_order = x_plus + x_minus
still = [0, 3, 4, 5, 6, 15, 16, 17, 18]
LANES = 128
FACE = 256


def collide_tile(f):
    sums = [None] * 19
    gaps = [None] * 19
    for number in range(1, 19, 2):
        sums[number] = f[number] + f[number + 1]
        gaps[number] = f[number] - f[number + 1]
    density = f[0]
    for number in range(1, 19, 2):
        density = density + sums[number]
    speeds = []
    for axis in range(3):
        total = None
        for number in range(1, 19, 2):
            sign = velocity_list[number][axis]
            if sign == 0:
                continue
            if total is None:
                total = gaps[number]
            elif sign == 1:
                total = total + gaps[number]
            else:
                total = total - gaps[number]
        speeds.append(total)
    inverse = 1.0 / density
    speeds = [speed * inverse for speed in speeds]
    squared = speeds[0] * speeds[0] + speeds[1] * speeds[1] + speeds[2] * speeds[2]
    base = 1.0 - 1.5 * squared
    keep = 1.0 - relax_rate
    out = [None] * 19
    out[0] = keep * f[0] + ((relax_rate * weight_list[0]) * density) * base
    scaled = {}
    thrice = {}
    for weight in sorted(set(weight_list[1:])):
        scaled[weight] = (relax_rate * weight) * density
        thrice[weight] = 3.0 * scaled[weight]
    for number in range(1, 19, 2):
        projected = None
        for axis in range(3):
            sign = velocity_list[number][axis]
            if sign == 0:
                continue
            if projected is None:
                projected = speeds[axis]
            elif sign == 1:
                projected = projected + speeds[axis]
            else:
                projected = projected - speeds[axis]
        weight = weight_list[number]
        even = scaled[weight] * (base + 4.5 * (projected * projected))
        odd = thrice[weight] * projected
        out[number] = keep * f[number] + (even + odd)
        out[number + 1] = keep * f[number + 1] + (even - odd)
    return out


def lane_of(shape):
    return lax.broadcasted_iota(jnp.int32, shape, 1)


def turned(value, amount):
    amount = amount % value.shape[1]
    return value if amount == 0 else pltpu.roll(value, amount, 1)


def pushed(value, low, high, sign):
    if sign == 1:
        return jnp.concatenate([low, value[:-1]], axis=0)
    return jnp.concatenate([value[1:], high], axis=0)


def shift_of(number):
    return velocity_list[number][1] * BS + velocity_list[number][2]


face_sets = [y_downward, y_upward, z_downward, z_upward]


def collide_all(field_ref, rolled_ref, moving_ref, edge_ref, piece_ref, rim_ref):
    depth = field_ref.shape[1]
    tiles = field_ref.shape[2] // LANES
    spot = lane_of((depth, LANES)) % BS
    quarter = lane_of((depth, LANES)) // BS
    for half in range(tiles // 4):
        packed = [jnp.zeros((depth, LANES), jnp.float32) for piece in range(2)]
        for u in range(4):
            tile = half * 4 + u
            lanes = slice(tile * LANES, (tile + 1) * LANES)
            out = collide_tile([field_ref[number, :, lanes] for number in range(19)])
            for number in range(19):
                if number in still:
                    rolled_ref[tile + 1, number] = turned(out[number], shift_of(number))
                else:
                    moving_ref[tile, x_order.index(number)] = out[number]
            for place, number in enumerate(x_plus):
                edge_ref[0, place, tile : tile + 1, :] = out[number][depth - 1 : depth]
            for place, number in enumerate(x_minus):
                edge_ref[1, place, tile : tile + 1, :] = out[number][0:1]
            for side, (chosen, begin) in enumerate([(z_downward, 0), (z_upward, BS - 1)]):
                for j, number in enumerate(chosen):
                    moved = turned(out[number] - weight_list[number], 8 * u + j - begin)
                    packed[side] = jnp.where(spot == 8 * u + j, moved, packed[side])
            for side, (chosen, at, begin) in enumerate(
                [(y_downward, 0, 0), (y_upward, tiles - 1, LANES - BS)]
            ):
                if tile != at:
                    continue
                values = [out[number] - weight_list[number] for number in chosen]
                row = jnp.zeros((depth, LANES), jnp.float32)
                for j in range(4):
                    row = jnp.where(quarter == j, turned(values[j], j * BS - begin), row)
                store_piece(piece_ref, rim_ref, side, 0, row)
                store_piece(piece_ref, rim_ref, side, 1, turned(values[4], -begin))
        for side in range(2):
            store_piece(piece_ref, rim_ref, 2 + side, half, packed[side])


def store_piece(piece_ref, rim_ref, piece, half, value):
    depth = value.shape[0]
    lanes = slice(half * LANES, (half + 1) * LANES)
    piece_ref[piece, :, lanes] = value.astype(jnp.bfloat16)
    rim_ref[piece, 0, :, lanes] = value[depth - 1 : depth]
    rim_ref[piece, 1, :, lanes] = value[0:1]


def roll_moving(rolled_ref, moving_ref, near_ref):
    tiles = moving_ref.shape[0]
    for tile in range(tiles):
        for place, number in enumerate(x_order):
            low = near_ref[0, place % 5, tile : tile + 1, :]
            high = near_ref[1, place % 5, tile : tile + 1, :]
            value = pushed(moving_ref[tile, place], low, high, velocity_list[number][0])
            rolled_ref[tile + 1, number] = turned(value, shift_of(number))


def finish_step(face, edge, got_ref, rim_got_ref, rolled_ref, field_ref, density_ref):
    depth = field_ref.shape[1]
    tiles = field_ref.shape[2] // LANES
    lane = lane_of((depth, LANES))
    spot = lane % BS

    def arrived(piece, source, half):
        chosen = face_sets[piece]
        lanes = slice(half * LANES, (half + 1) * LANES)
        value = got_ref[source, :, lanes].astype(jnp.float32)
        low = rim_got_ref[source, 0, :, lanes]
        high = rim_got_ref[source, 1, :, lanes]
        for j, number in enumerate(chosen):
            sign = velocity_list[number][0]
            if sign == 0:
                continue
            if piece < 2:
                if j // 4 != half:
                    continue
                wanted = lane // BS == j % 4
            else:
                wanted = lane % 8 == j
            base = got_ref[source, :, lanes].astype(jnp.float32)
            value = jnp.where(wanted, pushed(base, low, high, sign), value)
        return value

    corners = {15: (0, 0, 1), 17: (1, 1, 31), 18: (2, 1, 65), 16: (3, 0, 31)}
    corner_lane = {15: 0, 17: BS - 1, 18: LANES - BS, 16: LANES - 1}
    for piece, source, pad, begin in [(1, face[0], 0, 0), (0, face[1], tiles + 1, LANES - BS)]:
        halves = [arrived(piece, source, half) for half in range(2)]
        for j, number in enumerate(face_sets[piece]):
            shift_z = velocity_list[number][2]
            value = turned(halves[j // 4], begin + shift_z - j % 4 * BS)
            if number in corners:
                which, half, amount = corners[number]
                lanes = slice(half * LANES, (half + 1) * LANES)
                corner = turned(got_ref[edge[which], :, lanes].astype(jnp.float32), amount)
                value = jnp.where(lane == corner_lane[number], corner, value)
            rolled_ref[pad, number] = value + weight_list[number]
    columns = {}
    for piece, source, rim in [(3, face[2], 0), (2, face[3], BS - 1)]:
        chosen = face_sets[piece]
        halves = [arrived(piece, source, half) for half in range(2)]
        for tile in range(tiles):
            for j, number in enumerate(chosen):
                shift_y = velocity_list[number][1]
                amount = rim - 8 * (tile % 4) - j + BS * shift_y
                column = turned(halves[tile // 4], amount) + weight_list[number]
                value = jnp.where(spot == rim, column, rolled_ref[tile + 1, number])
                if shift_y != 0:
                    rolled_ref[tile + 1, number] = value
                else:
                    columns[tile, number] = value
                    field_ref[number, :, tile * LANES : (tile + 1) * LANES] = value
    for tile in range(tiles):
        lanes = slice(tile * LANES, (tile + 1) * LANES)
        total = None
        for number, (_, shift_y, shift_z) in enumerate(velocity_list):
            if shift_y == 0 and shift_z != 0:
                value = field_ref[number, :, lanes]
            else:
                value = rolled_ref[tile + 1, number]
                if shift_y == 1:
                    value = jnp.where(lane < BS, rolled_ref[tile, number], value)
                elif shift_y == -1:
                    value = jnp.where(lane >= LANES - BS, rolled_ref[tile + 2, number], value)
                field_ref[number, :, lanes] = value
            total = value if total is None else total + value
        density_ref[:, lanes] = total


def window_kernel(
    blocks, ring, face_ref, rim_face_ref, start_ref, field_ref, density_ref,
    rolled_ref, moving_ref, edge_ref, near_ref, piece_ref, rim_ref,
    send_ref, got_even, got_odd, rim_send_ref, rim_got_even, rim_got_odd,
    edge_send, edge_got, send_sem, got_sem, rim_send_sem, rim_got_sem,
):
    mesh_ids = pl.DeviceIdType.MESH
    me = lax.axis_index("blk")
    side = lax.axis_index("obs")
    right = lax.rem(side + 1, ring)
    left = lax.rem(side + ring - 1, ring)
    sides = [side, right] if ring == 2 else [side, right, left]
    barrier = pltpu.get_barrier_semaphore()

    def greet(distance, carry):
        peer = lax.rem(me + distance, blocks)
        for other in sides:
            pl.semaphore_signal(barrier, inc=1, device_id=(peer, other), device_id_type=mesh_ids)
        return carry

    for beside in sides[1:]:
        pl.semaphore_signal(barrier, inc=1, device_id=(me, beside), device_id_type=mesh_ids)
    lax.fori_loop(1, blocks, greet, 0)
    face = [face_ref[0, k] for k in range(4)]
    edge = [rim_face_ref[0, k] for k in range(4)]
    field_ref[...] = start_ref[...]

    def one_step(step, got_ref, rim_got_ref):
        collide_all(field_ref, rolled_ref, moving_ref, edge_ref, piece_ref, rim_ref)

        if rim_got_ref is rim_got_even:

            @pl.when(step == 0)
            def _():
                pl.semaphore_wait(barrier, len(sides) * blocks - 1)

        edges = [
            pltpu.make_async_remote_copy(
                src_ref=edge_ref.at[way],
                dst_ref=near_ref.at[step, way],
                send_sem=edge_send.at[step, way],
                recv_sem=edge_got.at[step, way],
                device_id=(me, beside),
                device_id_type=mesh_ids,
            )
            for way, beside in enumerate([right, left])
        ]
        for copy in edges:
            copy.start()

        def copies_to(distance):
            peer = lax.rem(me + distance, blocks)
            copies = [
                pltpu.make_async_remote_copy(
                    src_ref=send_ref.at[distance],
                    dst_ref=got_ref.at[me],
                    send_sem=send_sem.at[step, distance],
                    recv_sem=got_sem.at[step, distance],
                    device_id=(peer, side),
                    device_id_type=mesh_ids,
                )
            ]
            if ring == 2:
                copies.append(
                    pltpu.make_async_remote_copy(
                        src_ref=rim_send_ref.at[distance],
                        dst_ref=rim_got_ref.at[me],
                        send_sem=rim_send_sem.at[step, distance, 0],
                        recv_sem=rim_got_sem.at[step, distance, 0],
                        device_id=(peer, right),
                        device_id_type=mesh_ids,
                    )
                )
            else:
                for way, other in enumerate([right, left]):
                    copies.append(
                        pltpu.make_async_remote_copy(
                            src_ref=rim_send_ref.at[distance, way],
                            dst_ref=rim_got_ref.at[me, way],
                            send_sem=rim_send_sem.at[step, distance, way],
                            recv_sem=rim_got_sem.at[step, distance, way],
                            device_id=(peer, other),
                            device_id_type=mesh_ids,
                        )
                    )
            return copies

        def begin(distance, inner):
            peer = lax.rem(me + distance, blocks)
            up = (peer == face[1]) | (peer == edge[2]) | (peer == edge[3])
            piece = jnp.where(peer == face[3], 3, jnp.where(peer == face[2], 2, up.astype(jnp.int32)))
            send_ref[distance] = piece_ref[piece]
            rim_send_ref[distance] = rim_ref[piece]
            for copy in copies_to(distance):
                copy.start()
            return inner

        def finish(distance, inner):
            for copy in copies_to(distance):
                copy.wait()
            return inner

        lax.fori_loop(1, blocks, begin, 0)
        for copy in edges:
            copy.wait()
        roll_moving(rolled_ref, moving_ref, near_ref.at[step])
        lax.fori_loop(1, blocks, finish, 0)
        finish_step(
            face, edge, got_ref, rim_got_ref,
            rolled_ref, field_ref, density_ref.at[step],
        )

    def two_steps(turn, carry):
        one_step(turn * 2, got_even, rim_got_even)
        one_step(turn * 2 + 1, got_odd, rim_got_odd)
        return carry

    lax.fori_loop(0, STEPS // 2, two_steps, 0)


def call(kernel, outs, scalars, *arrays, scratch=()):
    vmem = pl.BlockSpec(memory_space=pltpu.VMEM)
    smem = pl.BlockSpec(memory_space=pltpu.SMEM)
    shapes = [jax.ShapeDtypeStruct(shape, jnp.float32) for shape in outs]
    return pl.pallas_call(
        kernel,
        out_shape=shapes,
        in_specs=[smem] * len(scalars) + [vmem] * len(arrays),
        out_specs=[vmem] * len(outs),
        scratch_shapes=[pltpu.VMEM(shape, jnp.float32) for shape in scratch],
    )(*scalars, *arrays)


def transform_table():
    moments = jnp.arange(SAMPLES, dtype=jnp.int32)[:, None]
    harmonics = jnp.arange(BINS, dtype=jnp.int32)[None, :] + 1
    turns = moments * harmonics % SAMPLES
    phases = turns.astype(jnp.float32) * (2.0 * math.pi / SAMPLES)
    return jnp.concatenate([jnp.cos(phases), -jnp.sin(phases)], axis=1).astype(jnp.bfloat16)


def greet_peers(blocks):
    me = lax.axis_index("blk")
    side = lax.axis_index("obs")
    barrier = pltpu.get_barrier_semaphore()

    def greet(distance, carry):
        pl.semaphore_signal(
            barrier, inc=1, device_id=(lax.rem(me + distance, blocks), side),
            device_id_type=pl.DeviceIdType.MESH,
        )
        return carry

    lax.fori_loop(1, blocks, greet, 0)
    return barrier


def swap_pieces(blocks, send_ref, got_ref, send_sem, got_sem):
    me = lax.axis_index("blk")
    side = lax.axis_index("obs")

    def copy_to(distance):
        peer = lax.rem(me + distance, blocks)
        return pltpu.make_async_remote_copy(
            src_ref=send_ref.at[peer],
            dst_ref=got_ref.at[me],
            send_sem=send_sem.at[distance],
            recv_sem=got_sem.at[distance],
            device_id=(peer, side),
            device_id_type=pl.DeviceIdType.MESH,
        )

    def begin(distance, inner):
        copy_to(distance).start()
        return inner

    def finish(distance, inner):
        copy_to(distance).wait()
        return inner

    lax.fori_loop(1, blocks, begin, 0)
    lax.fori_loop(1, blocks, finish, 0)


def exchange_kernel(blocks, source_ref, out_ref, got_ref, send_sem, got_sem):
    me = lax.axis_index("blk")
    barrier = greet_peers(blocks)
    got_ref[me] = source_ref[me]
    pl.semaphore_wait(barrier, blocks - 1)
    swap_pieces(blocks, source_ref, got_ref, send_sem, got_sem)
    out_ref[...] = got_ref[...]


def radiate_kernel(
    blocks, panel_ref, listen_ref, out_ref,
    real_ref, imag_ref, full_ref, send_ref, got_ref, send_sem, got_sem,
):
    barrier = greet_peers(blocks)
    listeners = listen_ref.shape[1]
    real_ref[...] = jnp.zeros_like(real_ref)
    imag_ref[...] = jnp.zeros_like(imag_ref)
    step_angle = 2.0 * math.pi / SAMPLES / sound_speed

    def accumulate(block_number, carry):
        begin = pl.multiple_of(block_number * 8, 8)
        panel = panel_ref[pl.ds(begin, 8), :]
        distance_sq = None
        facing = None
        for axis in range(3):
            at = 4 * BINS + axis
            offset = listen_ref[axis : axis + 1, :] - panel[:, at : at + 1]
            square = offset * offset
            along = panel[:, at + 3 : at + 4] * offset
            distance_sq = square if distance_sq is None else distance_sq + square
            facing = along if facing is None else facing + along
        distance = jnp.sqrt(distance_sq)
        far_term = facing / (4.0 * math.pi * sound_speed * distance_sq)
        ratio = sound_speed / distance
        angle = step_angle * distance
        turn_cos = jnp.cos(angle)
        turn_sin = jnp.sin(angle)
        wave_cos = far_term * turn_cos
        wave_sin = far_term * turn_sin
        for k in range(BINS):
            press_real = panel[:, k : k + 1]
            press_imag = panel[:, BINS + k : BINS + k + 1]
            rate_real = panel[:, 2 * BINS + k : 2 * BINS + k + 1]
            rate_imag = panel[:, 3 * BINS + k : 3 * BINS + k + 1]
            mixed_real = rate_real + ratio * press_real
            mixed_imag = rate_imag + ratio * press_imag
            real_ref[k] += mixed_real * wave_cos + mixed_imag * wave_sin
            imag_ref[k] += mixed_imag * wave_cos - mixed_real * wave_sin
            if k + 1 < BINS:
                wave_cos, wave_sin = (
                    wave_cos * turn_cos - wave_sin * turn_sin,
                    wave_sin * turn_cos + wave_cos * turn_sin,
                )
        return carry

    lax.fori_loop(0, panel_ref.shape[0] // 8, accumulate, 0)
    both = jnp.concatenate([jnp.sum(real_ref[...], axis=1), jnp.sum(imag_ref[...], axis=1)], axis=0)
    full_ref[...] = both.T
    chunk = out_ref.shape[0]
    for number in range(blocks):
        send_ref[number] = full_ref[number * chunk : (number + 1) * chunk]
    me = lax.axis_index("blk")
    got_ref[me] = send_ref[me]
    pl.semaphore_wait(barrier, blocks - 1)
    swap_pieces(blocks, send_ref, got_ref, send_sem, got_sem)
    out_ref[...] = jnp.sum(got_ref[...], axis=0)


def route_slots(payload, owners, alive_slot, blocks):
    count_slots = payload.shape[0]
    capacity = -(-count_slots // blocks)
    target = owners // P_OWN
    member = (
        (target[:, None] == jnp.arange(blocks, dtype=jnp.int32)[None, :]) & alive_slot[:, None]
    ).astype(jnp.int32)
    before = jnp.cumsum(member, axis=0) - member
    order_within = jnp.sum(before * member, axis=1)
    slot_label = jnp.where(alive_slot, target * capacity + order_within, -1)
    matches = slot_label[:, None] == jnp.arange(blocks * capacity, dtype=jnp.int32)[None, :]
    source = jnp.sum(
        jnp.where(matches, jnp.arange(count_slots, dtype=jnp.int32)[:, None], 0), axis=0
    )
    filled = jnp.any(matches, axis=0)
    outgoing = jnp.take(payload, source, axis=0).reshape(blocks, capacity, payload.shape[1])
    spots = jnp.where(filled, jnp.take(owners, source) % P_OWN, -1).reshape(blocks, capacity, 1)
    return jnp.concatenate([outgoing, spots.astype(jnp.bfloat16)], axis=2)


def settle(incoming):
    width = incoming.shape[-1] - 1
    flat = incoming.reshape(-1, width + 1)
    spots = flat[:, width].astype(jnp.int32)
    choose = (spots[:, None] == jnp.arange(P_OWN, dtype=jnp.int32)[None, :]).astype(jnp.bfloat16)
    return jnp.einsum(
        "rp,rw->pw", choose, flat[:, :width], preferred_element_type=jnp.float32
    ).astype(jnp.bfloat16)


def body(
    populations,
    block_faces,
    block_edges,
    probe_cell,
    history,
    panel_count,
    panel_owner,
    panel_pos,
    panel_normal,
    observers,
):
    blocks = lax.axis_size("blk")
    lattice_state = populations[0]
    slab_depth = lattice_state.shape[1]
    lane_count = lattice_state.shape[2]
    ring = lax.axis_size("obs")
    tiles = lane_count // LANES
    vmem = pl.BlockSpec(memory_space=pltpu.VMEM)
    smem = pl.BlockSpec(memory_space=pltpu.SMEM)
    wide = jnp.float32
    half = jnp.bfloat16
    lattice_state, densities = pl.pallas_call(
        functools.partial(window_kernel, blocks, ring),
        out_shape=[
            jax.ShapeDtypeStruct((19, slab_depth, lane_count), jnp.float32),
            jax.ShapeDtypeStruct((STEPS, slab_depth, lane_count), jnp.float32),
        ],
        in_specs=[smem, smem, vmem],
        out_specs=[vmem, vmem],
        scratch_shapes=[
            pltpu.VMEM((tiles + 2, 19, slab_depth, LANES), wide),
            pltpu.VMEM((tiles, len(x_order), slab_depth, LANES), wide),
            pltpu.VMEM((2, 5, tiles, LANES), wide),
            pltpu.VMEM((STEPS, 2, 5, tiles, LANES), wide),
            pltpu.VMEM((4, slab_depth, FACE), half),
            pltpu.VMEM((4, 2, 1, FACE), wide),
            pltpu.VMEM((blocks, slab_depth, FACE), half),
            pltpu.VMEM((blocks, slab_depth, FACE), half),
            pltpu.VMEM((blocks, slab_depth, FACE), half),
            pltpu.VMEM((blocks, 2, 1, FACE), wide),
            pltpu.VMEM((blocks, 2, 1, FACE), wide),
            pltpu.VMEM((blocks, 2, 1, FACE), wide),
        ]
        + [pltpu.SemaphoreType.DMA((STEPS, 2))] * 2
        + [pltpu.SemaphoreType.DMA((STEPS, blocks))] * 2
        + [pltpu.SemaphoreType.DMA((STEPS, blocks, 2))] * 2,
        compiler_params=pltpu.CompilerParams(collective_id=0, has_side_effects=True),
    )(block_faces, block_edges, lattice_state)
    populations_out = lattice_state.reshape(1, 19, slab_depth, lane_count)
    readings = [jnp.take(density.reshape(-1), probe_cell) for density in densities]
    gained = pressure_gain * (jnp.stack(readings, axis=1) - 1.0)
    previous = jnp.concatenate(
        [history[:, SAMPLES - 1 : SAMPLES].astype(jnp.float32), gained[:, :-1]], axis=1
    )
    rate_values = gained - previous
    recent = jnp.concatenate(
        [
            history[:, STEPS:SAMPLES],
            gained.astype(jnp.bfloat16),
            history[:, SAMPLES + STEPS :],
            rate_values.astype(jnp.bfloat16),
        ],
        axis=1,
    )
    transform = transform_table()
    count_slots = recent.shape[0]
    alive_slot = jnp.arange(count_slots, dtype=jnp.int32) < panel_count[0]
    outgoing = route_slots(recent, panel_owner, alive_slot, blocks)
    incoming = pl.pallas_call(
        functools.partial(exchange_kernel, blocks),
        out_shape=jax.ShapeDtypeStruct(outgoing.shape, outgoing.dtype),
        in_specs=[vmem],
        out_specs=vmem,
        scratch_shapes=[pltpu.VMEM(outgoing.shape, outgoing.dtype)]
        + [pltpu.SemaphoreType.DMA((blocks,))] * 2,
        compiler_params=pltpu.CompilerParams(collective_id=1, has_side_effects=True),
    )(outgoing)
    owned = settle(incoming).reshape(P_OWN, 2, SAMPLES)
    spectra = (
        jnp.einsum("pgt,tk->pgk", owned, transform, preferred_element_type=jnp.float32)
        .astype(jnp.bfloat16)
        .reshape(P_OWN, 4 * BINS)
    )
    panels = jnp.concatenate([spectra, panel_pos.T, panel_normal.T], axis=1)
    gathered = lax.all_gather(panels, "obs", axis=0, tiled=True).astype(jnp.float32)
    listeners = observers.shape[1]
    chunk = listeners // blocks
    spectrum = pl.pallas_call(
        functools.partial(radiate_kernel, blocks),
        out_shape=jax.ShapeDtypeStruct((chunk, 2 * BINS), jnp.float32),
        in_specs=[vmem, vmem],
        out_specs=vmem,
        scratch_shapes=[
            pltpu.VMEM(shape, jnp.float32)
            for shape in [
                (BINS, 8, listeners), (BINS, 8, listeners), (listeners, 2 * BINS),
                (blocks, chunk, 2 * BINS), (blocks, chunk, 2 * BINS),
            ]
        ]
        + [pltpu.SemaphoreType.DMA((blocks,))] * 2,
        compiler_params=pltpu.CompilerParams(collective_id=2, has_side_effects=True),
    )(gathered, observers)
    return (populations_out, spectrum[None])


def solution(mesh):
    placed = (
        P("blk", None, "obs", None),
        P("blk", None),
        P("blk", None),
        P(("blk", "obs")),
        P(("blk", "obs"), None),
        P(("blk", "obs")),
        P(("blk", "obs")),
        P(None, ("blk", "obs")),
        P(None, ("blk", "obs")),
        P(None, "obs"),
    )
    return jax.shard_map(
        body,
        mesh=mesh,
        in_specs=placed,
        out_specs=(P("blk", None, "obs", None), P("obs", "blk", None)),
        check_vma=False,
    )
```

```python
import functools
import math

import jax
import jax.numpy as jnp
import numpy as np
from jax import lax
from jax.experimental import pallas as pl
from jax.experimental.pallas import tpu as pltpu
from jax.sharding import PartitionSpec as P

BS = 32
STEPS = 4
SAMPLES = 256
BINS = 64
P_OWN = 64


velocity_list = [
    (0, 0, 0),
    (1, 0, 0),
    (-1, 0, 0),
    (0, 1, 0),
    (0, -1, 0),
    (0, 0, 1),
    (0, 0, -1),
    (1, 1, 0),
    (-1, -1, 0),
    (1, -1, 0),
    (-1, 1, 0),
    (1, 0, 1),
    (-1, 0, -1),
    (1, 0, -1),
    (-1, 0, 1),
    (0, 1, 1),
    (0, -1, -1),
    (0, 1, -1),
    (0, -1, 1),
]
weight_list = [1.0 / 3.0] + [1.0 / 18.0] * 6 + [1.0 / 36.0] * 12
x_moving = [1, 2, 7, 8, 9, 10, 11, 12, 13, 14]
y_upward = [3, 7, 10, 15, 17]
y_downward = [4, 8, 9, 16, 18]
z_upward = [5, 11, 14, 15, 18]
z_downward = [6, 12, 13, 16, 17]
relax_rate = 1.6
pressure_gain = 60.0
sound_speed = 0.5


x_plus = [1, 7, 9, 11, 13]
x_minus = [2, 8, 10, 12, 14]
x_order = x_plus + x_minus
still = [0, 3, 4, 5, 6, 15, 16, 17, 18]
LANES = 128
FACE = 256


def collide_tile(f):
    sums = [None] * 19
    gaps = [None] * 19
    for number in range(1, 19, 2):
        sums[number] = f[number] + f[number + 1]
        gaps[number] = f[number] - f[number + 1]
    density = f[0]
    for number in range(1, 19, 2):
        density = density + sums[number]
    speeds = []
    for axis in range(3):
        total = None
        for number in range(1, 19, 2):
            sign = velocity_list[number][axis]
            if sign == 0:
                continue
            if total is None:
                total = gaps[number]
            elif sign == 1:
                total = total + gaps[number]
            else:
                total = total - gaps[number]
        speeds.append(total)
    inverse = 1.0 / density
    speeds = [speed * inverse for speed in speeds]
    squared = speeds[0] * speeds[0] + speeds[1] * speeds[1] + speeds[2] * speeds[2]
    base = 1.0 - 1.5 * squared
    keep = 1.0 - relax_rate
    out = [None] * 19
    out[0] = keep * f[0] + ((relax_rate * weight_list[0]) * density) * base
    scaled = {}
    thrice = {}
    for weight in sorted(set(weight_list[1:])):
        scaled[weight] = (relax_rate * weight) * density
        thrice[weight] = 3.0 * scaled[weight]
    for number in range(1, 19, 2):
        projected = None
        for axis in range(3):
            sign = velocity_list[number][axis]
            if sign == 0:
                continue
            if projected is None:
                projected = speeds[axis]
            elif sign == 1:
                projected = projected + speeds[axis]
            else:
                projected = projected - speeds[axis]
        weight = weight_list[number]
        even = scaled[weight] * (base + 4.5 * (projected * projected))
        odd = thrice[weight] * projected
        out[number] = keep * f[number] + (even + odd)
        out[number + 1] = keep * f[number + 1] + (even - odd)
    return out


def lane_of(shape):
    return lax.broadcasted_iota(jnp.int32, shape, 1)


def turned(value, amount):
    amount = amount % value.shape[1]
    return value if amount == 0 else pltpu.roll(value, amount, 1)


def pushed(value, low, high, sign):
    if sign == 1:
        return jnp.concatenate([low, value[:-1]], axis=0)
    return jnp.concatenate([value[1:], high], axis=0)


def shift_of(number):
    return velocity_list[number][1] * BS + velocity_list[number][2]


face_sets = [y_downward, y_upward, z_downward, z_upward]


def pack_tile(values, tile, tiles, chosen_numbers, columns, rows):
    depth = values[chosen_numbers[0]].shape[0]
    spot = lane_of((depth, LANES)) % BS
    quarter = lane_of((depth, LANES)) // BS
    u = tile % 4
    for side, (chosen, begin) in enumerate([(z_downward, 0), (z_upward, BS - 1)]):
        for j, number in enumerate(chosen):
            if number in chosen_numbers:
                moved = turned(values[number] - weight_list[number], 8 * u + j - begin)
                columns[side] = jnp.where(spot == 8 * u + j, moved, columns[side])
    for side, (chosen, at, begin) in enumerate(
        [(y_downward, 0, 0), (y_upward, tiles - 1, LANES - BS)]
    ):
        if tile != at:
            continue
        for j, number in enumerate(chosen):
            if number in chosen_numbers:
                moved = turned(values[number] - weight_list[number], j % 4 * BS - begin)
                rows[side][j // 4] = jnp.where(quarter == j % 4, moved, rows[side][j // 4])


def collide_all(field_ref, rolled_ref, moving_ref, edge_ref, draft_ref):
    depth = field_ref.shape[1]
    tiles = field_ref.shape[2] // LANES
    blank = jnp.zeros((depth, LANES), jnp.float32)
    rows = [[blank, blank], [blank, blank]]
    for half in range(tiles // 4):
        columns = [blank, blank]
        for u in range(4):
            tile = half * 4 + u
            lanes = slice(tile * LANES, (tile + 1) * LANES)
            out = collide_tile([field_ref[number, :, lanes] for number in range(19)])
            for number in range(19):
                if number in still:
                    rolled_ref[tile + 1, number] = turned(out[number], shift_of(number))
                else:
                    moving_ref[tile, x_order.index(number)] = out[number]
            for place, number in enumerate(x_plus):
                edge_ref[0, place, tile : tile + 1, :] = out[number][depth - 1 : depth]
            for place, number in enumerate(x_minus):
                edge_ref[1, place, tile : tile + 1, :] = out[number][0:1]
            pack_tile(out, tile, tiles, still, columns, rows)
        for side in range(2):
            draft_ref[2 + side, :, half * LANES : (half + 1) * LANES] = columns[side]
    for side in range(2):
        for half in range(2):
            draft_ref[side, :, half * LANES : (half + 1) * LANES] = rows[side][half]


def shifted(moving_ref, near_ref, tile, number):
    place = x_order.index(number)
    low = near_ref[0, place % 5, tile : tile + 1, :]
    high = near_ref[1, place % 5, tile : tile + 1, :]
    return pushed(moving_ref[tile, place], low, high, velocity_list[number][0])


def pack_moving(moving_ref, near_ref, draft_ref, piece_ref):
    tiles = moving_ref.shape[0]
    crossing = x_order[1:5] + x_order[6:]

    def draft(piece, half):
        return draft_ref[piece, :, half * LANES : (half + 1) * LANES]

    rows = [[draft(side, half) for half in range(2)] for side in range(2)]
    for half in range(tiles // 4):
        columns = [draft(2 + side, half) for side in range(2)]
        for u in range(4):
            tile = half * 4 + u
            values = {}
            for number in crossing:
                if velocity_list[number][1] == 0 or tile in (0, tiles - 1):
                    values[number] = shifted(moving_ref, near_ref, tile, number)
            pack_tile(values, tile, tiles, list(values), columns, rows)
        for side in range(2):
            piece_ref[2 + side, :, half * LANES : (half + 1) * LANES] = columns[side].astype(jnp.bfloat16)
    for side in range(2):
        for half in range(2):
            piece_ref[side, :, half * LANES : (half + 1) * LANES] = rows[side][half].astype(jnp.bfloat16)


def roll_moving(rolled_ref, moving_ref, near_ref):
    tiles = moving_ref.shape[0]
    for tile in range(tiles):
        for number in x_order:
            value = shifted(moving_ref, near_ref, tile, number)
            rolled_ref[tile + 1, number] = turned(value, shift_of(number))


def finish_step(face, edge, got_ref, rolled_ref, field_ref, density_ref):
    depth = field_ref.shape[1]
    tiles = field_ref.shape[2] // LANES
    lane = lane_of((depth, LANES))
    spot = lane % BS

    def arrived(source, half):
        return got_ref[source, :, half * LANES : (half + 1) * LANES].astype(jnp.float32)

    corners = {15: (0, 0, 1), 17: (1, 1, 31), 18: (2, 1, 65), 16: (3, 0, 31)}
    corner_lane = {15: 0, 17: BS - 1, 18: LANES - BS, 16: LANES - 1}
    for piece, source, pad, begin in [(1, face[0], 0, 0), (0, face[1], tiles + 1, LANES - BS)]:
        halves = [arrived(source, half) for half in range(2)]
        for j, number in enumerate(face_sets[piece]):
            shift_z = velocity_list[number][2]
            value = turned(halves[j // 4], begin + shift_z - j % 4 * BS)
            if number in corners:
                which, half, amount = corners[number]
                corner = turned(arrived(edge[which], half), amount)
                value = jnp.where(lane == corner_lane[number], corner, value)
            rolled_ref[pad, number] = value + weight_list[number]
    columns = {}
    for piece, source, rim in [(3, face[2], 0), (2, face[3], BS - 1)]:
        chosen = face_sets[piece]
        halves = [arrived(source, half) for half in range(2)]
        for tile in range(tiles):
            for j, number in enumerate(chosen):
                shift_y = velocity_list[number][1]
                amount = rim - 8 * (tile % 4) - j + BS * shift_y
                column = turned(halves[tile // 4], amount) + weight_list[number]
                value = jnp.where(spot == rim, column, rolled_ref[tile + 1, number])
                if shift_y != 0:
                    rolled_ref[tile + 1, number] = value
                else:
                    columns[tile, number] = value
                    field_ref[number, :, tile * LANES : (tile + 1) * LANES] = value
    for tile in range(tiles):
        lanes = slice(tile * LANES, (tile + 1) * LANES)
        total = None
        for number, (_, shift_y, shift_z) in enumerate(velocity_list):
            if shift_y == 0 and shift_z != 0:
                value = field_ref[number, :, lanes]
            else:
                value = rolled_ref[tile + 1, number]
                if shift_y == 1:
                    value = jnp.where(lane < BS, rolled_ref[tile, number], value)
                elif shift_y == -1:
                    value = jnp.where(lane >= LANES - BS, rolled_ref[tile + 2, number], value)
                field_ref[number, :, lanes] = value
            total = value if total is None else total + value
        density_ref[:, lanes] = total


def joined(left, right, left_axis, right_axis):
    return lax.dot_general(
        left.astype(jnp.bfloat16), right.astype(jnp.bfloat16),
        (((left_axis,), (right_axis,)), ((), ())), preferred_element_type=jnp.float32,
    )


def rows_of(shape):
    return lax.broadcasted_iota(jnp.int32, shape, 0)


def route(blocks, owner_ref, count, history_ref, select_ref, send_ref):
    slots = owner_ref.shape[1]
    room = send_ref.shape[1]
    width = history_ref.shape[1]
    owner = owner_ref[...]
    alive = lane_of((1, slots)) < count
    target = lax.shift_right_logical(owner, P_OWN.bit_length() - 1)
    spot = lax.bitwise_and(owner, P_OWN - 1)
    member = jnp.where((rows_of((blocks, slots)) == target) & alive, 1.0, 0.0)
    earlier = jnp.where(rows_of((slots, slots)) < lane_of((slots, slots)), 1.0, 0.0)
    before = joined(member, earlier, 1, 0)
    order = jnp.sum(before * member, axis=0, keepdims=True).astype(jnp.int32)
    label = jnp.where(alive, target * room + order, -1)
    select = jnp.where(rows_of((blocks * room, slots)) == label, 1.0, 0.0)
    select_ref[...] = select.astype(jnp.bfloat16)
    moved = joined(select, history_ref[...], 1, 0)
    spots = joined(select, jnp.where(rows_of((P_OWN, slots)) == spot, 1.0, 0.0), 1, 1)
    for block in range(blocks):
        rows = slice(block * room, (block + 1) * room)
        send_ref[block, :, 0:width] = moved[rows].astype(jnp.bfloat16)
        send_ref[block, :, width : width + P_OWN] = spots[rows].astype(jnp.bfloat16)


def unpacked(got_ref, flat_ref):
    blocks, room = got_ref.shape[0], got_ref.shape[1]
    for block in range(blocks):
        flat_ref[block * room : (block + 1) * room, :] = got_ref[block].astype(jnp.float32)


def settle_history(got_ref, flat_ref, choose_ref, table_ref, partial_ref):
    unpacked(got_ref, flat_ref)
    choose = flat_ref[:, 2 * SAMPLES : 2 * SAMPLES + P_OWN].astype(jnp.bfloat16)
    choose_ref[...] = choose
    owned = joined(choose, flat_ref[:, 0 : 2 * SAMPLES], 0, 0)
    for field in range(2):
        partial_ref[:, field * 2 * BINS : (field + 1) * 2 * BINS] = joined(
            owned[:, field * SAMPLES : (field + 1) * SAMPLES], table_ref[...], 1, 0
        )


def reading_of(density_ref, cell_ref, probe_ref):
    depth = density_ref.shape[0]
    count = density_ref.shape[1]
    excess = density_ref[...] - 1.0
    parts = []
    for _ in range(3):
        part = excess.astype(jnp.bfloat16).astype(jnp.float32)
        parts.append(part)
        excess = excess - part
    found = joined(jnp.concatenate(parts, axis=0), cell_ref[...], 1, 0)
    layers = found[0:depth] + found[depth : 2 * depth] + found[2 * depth : 3 * depth]
    layer = lax.div(probe_ref[...], count)
    mine = rows_of(layers.shape) == layer
    return jnp.sum(jnp.where(mine, layers, 0.0), axis=0, keepdims=True)


def window_kernel(
    blocks, ring, face_ref, rim_face_ref, count_ref, start_ref, owner_ref, probe_ref, history_ref,
    place_ref, normal_ref, table_ref, tail_ref, field_ref, spectra_ref, place_out_ref,
    density_ref, rolled_ref, moving_ref, edge_ref, near_ref, draft_ref, piece_ref,
    send_ref, got_even, got_odd, select_ref, cell_ref, past_send, past_got, flat_ref, choose_ref,
    partial_ref, fresh_ref, fresh_send, fresh_got, fresh_flat, done_ref, done_got, spot_ref, spot_got,
    edge_send, edge_got, send_sem, got_sem, past_send_sem, past_got_sem, fresh_send_sem, fresh_got_sem,
    done_send_sem, done_got_sem, spot_send_sem, spot_got_sem,
):
    mesh_ids = pl.DeviceIdType.MESH
    me = lax.axis_index("blk")
    side = lax.axis_index("obs")
    right = lax.rem(side + 1, ring)
    left = lax.rem(side + ring - 1, ring)
    barrier = pltpu.get_barrier_semaphore()
    slots = owner_ref.shape[1]

    def greet(distance, carry):
        peer = lax.rem(me + distance, blocks)
        pl.semaphore_signal(barrier, inc=1, device_id=(peer, side), device_id_type=mesh_ids)
        return carry

    for distance in range(1, ring):
        beside = lax.rem(side + distance, ring)
        pl.semaphore_signal(barrier, inc=1, device_id=(me, beside), device_id_type=mesh_ids)
    lax.fori_loop(1, blocks, greet, 0)
    face = [face_ref[0, k] for k in range(4)]
    edge = [rim_face_ref[0, k] for k in range(4)]
    field_ref[...] = start_ref[...]
    route(blocks, owner_ref, count_ref[0], history_ref, select_ref, past_send)
    cell = lax.rem(probe_ref[...], start_ref.shape[2])
    cell_ref[...] = jnp.where(rows_of(cell_ref.shape) == cell, 1.0, 0.0).astype(jnp.bfloat16)
    spot_ref[...] = jnp.zeros_like(spot_ref)
    spot_ref[0:3, 0:P_OWN] = place_ref[...].astype(jnp.float32)
    spot_ref[3:6, 0:P_OWN] = normal_ref[...].astype(jnp.float32)
    fresh_ref[...] = jnp.zeros_like(fresh_ref)

    def swap(source_of, into_ref, send_sems, got_sems, distance):
        peer = lax.rem(me + distance, blocks)
        return pltpu.make_async_remote_copy(
            src_ref=source_of(distance, peer),
            dst_ref=into_ref.at[me],
            send_sem=send_sems.at[distance],
            recv_sem=got_sems.at[distance],
            device_id=(peer, side),
            device_id_type=mesh_ids,
        )

    def every(action):
        def visit(distance, inner):
            action(distance)
            return inner

        lax.fori_loop(1, blocks, visit, 0)

    def past_copy(distance):
        return swap(lambda _, peer: past_send.at[peer], past_got, past_send_sem, past_got_sem, distance)

    def fresh_copy(distance):
        return swap(lambda _, peer: fresh_send.at[peer], fresh_got, fresh_send_sem, fresh_got_sem, distance)

    def ring_copies(source_ref, into_ref, send_sems, got_sems):
        return [
            pltpu.make_async_remote_copy(
                src_ref=source_ref,
                dst_ref=into_ref.at[side],
                send_sem=send_sems.at[distance],
                recv_sem=got_sems.at[distance],
                device_id=(me, lax.rem(side + distance, ring)),
                device_id_type=mesh_ids,
            )
            for distance in range(1, ring)
        ]

    def note(step):
        gained = pressure_gain * reading_of(density_ref.at[step], cell_ref, probe_ref)
        if step == 0:
            last = jnp.where(lane_of((8, 2 * SAMPLES)) == SAMPLES - 1, 1.0, 0.0)
            before = joined(last, history_ref[...], 1, 1)[0:1]
        else:
            before = fresh_ref[step - 1 : step, :]
        fresh_ref[step : step + 1, :] = gained
        fresh_ref[STEPS + step : STEPS + step + 1, :] = gained - before

    def one_step(step):
        got_ref = got_odd if step % 2 else got_even
        collide_all(field_ref, rolled_ref, moving_ref, edge_ref, draft_ref)
        if step == 0:
            pl.semaphore_wait(barrier, blocks + ring - 2)
        edges = [
            pltpu.make_async_remote_copy(
                src_ref=edge_ref.at[way],
                dst_ref=near_ref.at[step, way],
                send_sem=edge_send.at[step, way],
                recv_sem=edge_got.at[step, way],
                device_id=(me, beside),
                device_id_type=mesh_ids,
            )
            for way, beside in enumerate([right, left])
        ]
        for copy in edges:
            copy.start()
        for copy in edges:
            copy.wait()
        pack_moving(moving_ref, near_ref.at[step], draft_ref, piece_ref)

        def copy_to(distance):
            return swap(
                lambda number, _: send_ref.at[number], got_ref, send_sem.at[step], got_sem.at[step], distance
            )

        def begin(distance):
            peer = lax.rem(me + distance, blocks)
            up = (peer == face[1]) | (peer == edge[2]) | (peer == edge[3])
            piece = jnp.where(peer == face[3], 3, jnp.where(peer == face[2], 2, up.astype(jnp.int32)))
            send_ref[distance] = piece_ref[piece]
            copy_to(distance).start()

        every(begin)
        roll_moving(rolled_ref, moving_ref, near_ref.at[step])
        if step == 0:
            every(lambda distance: past_copy(distance).start())
            for copy in ring_copies(spot_ref, spot_got, spot_send_sem, spot_got_sem):
                copy.start()
            past_got[me] = past_send[me]
        else:
            note(step - 1)
        if step == 2:
            every(lambda distance: past_copy(distance).wait())
            settle_history(past_got, flat_ref, choose_ref, table_ref, partial_ref)
        every(lambda distance: copy_to(distance).wait())
        finish_step(face, edge, got_ref, rolled_ref, field_ref, density_ref.at[step])

    for step in range(STEPS):
        one_step(step)
    note(STEPS - 1)
    fresh = joined(select_ref[...], fresh_ref[...], 1, 1)
    room = fresh_send.shape[1]
    for block in range(blocks):
        fresh_send[block] = fresh[block * room : (block + 1) * room].astype(jnp.bfloat16)
    every(lambda distance: fresh_copy(distance).start())
    fresh_got[me] = fresh_send[me]
    for copy in ring_copies(spot_ref, spot_got, spot_send_sem, spot_got_sem):
        copy.wait()
    spot_got[side] = spot_ref[...]
    place_out_ref[...] = spot_got[...]
    every(lambda distance: fresh_copy(distance).wait())
    unpacked(fresh_got, fresh_flat)
    newest = joined(choose_ref[...], fresh_flat[...], 0, 0)
    total = partial_ref[...] + joined(newest, tail_ref[...], 1, 0)
    done_ref[...] = total.astype(jnp.bfloat16)
    copies = ring_copies(done_ref, done_got, done_send_sem, done_got_sem)
    for copy in copies:
        copy.start()
    done_got[side] = done_ref[...]
    for copy in copies:
        copy.wait()
    spectra_ref[...] = done_got[...].astype(jnp.float32)


def transform_tables():
    moments = np.arange(SAMPLES)[:, None]
    harmonics = np.arange(BINS)[None, :] + 1
    turns = moments * harmonics % SAMPLES
    phases = turns.astype(np.float32) * np.float32(2.0 * math.pi / SAMPLES)
    table = np.concatenate([np.cos(phases), -np.sin(phases)], axis=1).astype(jnp.bfloat16)
    past = np.zeros_like(table)
    past[STEPS:] = table[: SAMPLES - STEPS]
    tail = np.zeros((LANES, 4 * BINS), table.dtype)
    for field in range(2):
        rows = slice(field * STEPS, (field + 1) * STEPS)
        tail[rows, field * 2 * BINS : (field + 1) * 2 * BINS] = table[SAMPLES - STEPS :]
    return jnp.asarray(past), jnp.asarray(tail)


def greet_peers(blocks):
    me = lax.axis_index("blk")
    side = lax.axis_index("obs")
    barrier = pltpu.get_barrier_semaphore()

    def greet(distance, carry):
        pl.semaphore_signal(
            barrier, inc=1, device_id=(lax.rem(me + distance, blocks), side),
            device_id_type=pl.DeviceIdType.MESH,
        )
        return carry

    lax.fori_loop(1, blocks, greet, 0)
    return barrier


def swap_pieces(blocks, send_ref, got_ref, send_sem, got_sem):
    me = lax.axis_index("blk")
    side = lax.axis_index("obs")

    def copy_to(distance):
        peer = lax.rem(me + distance, blocks)
        return pltpu.make_async_remote_copy(
            src_ref=send_ref.at[peer],
            dst_ref=got_ref.at[me],
            send_sem=send_sem.at[distance],
            recv_sem=got_sem.at[distance],
            device_id=(peer, side),
            device_id_type=pl.DeviceIdType.MESH,
        )

    def begin(distance, inner):
        copy_to(distance).start()
        return inner

    def finish(distance, inner):
        copy_to(distance).wait()
        return inner

    lax.fori_loop(1, blocks, begin, 0)
    lax.fori_loop(1, blocks, finish, 0)


def radiate_kernel(
    blocks, panel_ref, listen_ref, out_ref,
    real_ref, imag_ref, full_ref, send_ref, got_ref, send_sem, got_sem,
):
    barrier = greet_peers(blocks)
    listeners = listen_ref.shape[1]
    real_ref[...] = jnp.zeros_like(real_ref)
    imag_ref[...] = jnp.zeros_like(imag_ref)
    step_angle = 2.0 * math.pi / SAMPLES / sound_speed

    def accumulate(block_number, carry):
        begin = pl.multiple_of(block_number * 8, 8)
        panel = panel_ref[pl.ds(begin, 8), :]
        distance_sq = None
        facing = None
        for axis in range(3):
            at = 4 * BINS + axis
            offset = listen_ref[axis : axis + 1, :] - panel[:, at : at + 1]
            square = offset * offset
            along = panel[:, at + 3 : at + 4] * offset
            distance_sq = square if distance_sq is None else distance_sq + square
            facing = along if facing is None else facing + along
        distance = jnp.sqrt(distance_sq)
        far_term = facing / (4.0 * math.pi * sound_speed * distance_sq)
        ratio = sound_speed / distance
        angle = step_angle * distance
        turn_cos = jnp.cos(angle)
        turn_sin = jnp.sin(angle)
        wave_cos = far_term * turn_cos
        wave_sin = far_term * turn_sin
        for k in range(BINS):
            press_real = panel[:, k : k + 1]
            press_imag = panel[:, BINS + k : BINS + k + 1]
            rate_real = panel[:, 2 * BINS + k : 2 * BINS + k + 1]
            rate_imag = panel[:, 3 * BINS + k : 3 * BINS + k + 1]
            mixed_real = rate_real + ratio * press_real
            mixed_imag = rate_imag + ratio * press_imag
            real_ref[k] += mixed_real * wave_cos + mixed_imag * wave_sin
            imag_ref[k] += mixed_imag * wave_cos - mixed_real * wave_sin
            if k + 1 < BINS:
                wave_cos, wave_sin = (
                    wave_cos * turn_cos - wave_sin * turn_sin,
                    wave_sin * turn_cos + wave_cos * turn_sin,
                )
        return carry

    lax.fori_loop(0, panel_ref.shape[0] // 8, accumulate, 0)
    both = jnp.concatenate([jnp.sum(real_ref[...], axis=1), jnp.sum(imag_ref[...], axis=1)], axis=0)
    full_ref[...] = both.T
    chunk = out_ref.shape[0]
    for number in range(blocks):
        send_ref[number] = full_ref[number * chunk : (number + 1) * chunk]
    me = lax.axis_index("blk")
    got_ref[me] = send_ref[me]
    pl.semaphore_wait(barrier, blocks - 1)
    swap_pieces(blocks, send_ref, got_ref, send_sem, got_sem)
    out_ref[...] = jnp.sum(got_ref[...], axis=0)


def body(
    populations,
    block_faces,
    block_edges,
    probe_cell,
    history,
    panel_count,
    panel_owner,
    panel_pos,
    panel_normal,
    observers,
):
    blocks = lax.axis_size("blk")
    lattice_state = populations[0]
    slab_depth = lattice_state.shape[1]
    lane_count = lattice_state.shape[2]
    ring = lax.axis_size("obs")
    tiles = lane_count // LANES
    vmem = pl.BlockSpec(memory_space=pltpu.VMEM)
    smem = pl.BlockSpec(memory_space=pltpu.SMEM)
    wide = jnp.float32
    half = jnp.bfloat16
    slots = panel_owner.shape[0]
    room = -(-slots // blocks)
    past, tail = transform_tables()
    dma = pltpu.SemaphoreType.DMA
    lattice_state, spectra, places = pl.pallas_call(
        functools.partial(window_kernel, blocks, ring),
        out_shape=[
            jax.ShapeDtypeStruct((19, slab_depth, lane_count), wide),
            jax.ShapeDtypeStruct((ring, P_OWN, 4 * BINS), wide),
            jax.ShapeDtypeStruct((ring, 8, LANES), wide),
        ],
        in_specs=[smem] * 3 + [vmem] * 8,
        out_specs=[vmem] * 3,
        scratch_shapes=[
            pltpu.VMEM((STEPS, slab_depth, lane_count), wide),
            pltpu.VMEM((tiles + 2, 19, slab_depth, LANES), wide),
            pltpu.VMEM((tiles, len(x_order), slab_depth, LANES), wide),
            pltpu.VMEM((2, 5, tiles, LANES), wide),
            pltpu.VMEM((STEPS, 2, 5, tiles, LANES), wide),
            pltpu.VMEM((4, slab_depth, FACE), wide),
            pltpu.VMEM((4, slab_depth, FACE), half),
            pltpu.VMEM((blocks, slab_depth, FACE), half),
            pltpu.VMEM((blocks, slab_depth, FACE), half),
            pltpu.VMEM((blocks, slab_depth, FACE), half),
            pltpu.VMEM((blocks * room, slots), half),
            pltpu.VMEM((lane_count, slots), half),
            pltpu.VMEM((blocks, room, 5 * LANES), half),
            pltpu.VMEM((blocks, room, 5 * LANES), half),
            pltpu.VMEM((blocks * room, 5 * LANES), wide),
            pltpu.VMEM((blocks * room, P_OWN), half),
            pltpu.VMEM((P_OWN, 4 * BINS), wide),
            pltpu.VMEM((LANES, slots), wide),
            pltpu.VMEM((blocks, room, LANES), half),
            pltpu.VMEM((blocks, room, LANES), half),
            pltpu.VMEM((blocks * room, LANES), wide),
            pltpu.VMEM((P_OWN, 4 * BINS), half),
            pltpu.VMEM((ring, P_OWN, 4 * BINS), half),
            pltpu.VMEM((8, LANES), wide),
            pltpu.VMEM((ring, 8, LANES), wide),
        ]
        + [dma((STEPS, 2))] * 2
        + [dma((STEPS, blocks))] * 2
        + [dma((blocks,))] * 4
        + [dma((ring,))] * 4,
        compiler_params=pltpu.CompilerParams(collective_id=0, has_side_effects=True),
    )(
        block_faces, block_edges, panel_count, lattice_state, panel_owner[None], probe_cell[None],
        history, panel_pos, panel_normal, past, tail,
    )
    populations_out = lattice_state.reshape(1, 19, slab_depth, lane_count)
    places = places[:, :, :P_OWN].transpose(0, 2, 1).reshape(ring * P_OWN, 8)
    gathered = jnp.concatenate([spectra.reshape(ring * P_OWN, 4 * BINS), places], axis=1)
    listeners = observers.shape[1]
    chunk = listeners // blocks
    spectrum = pl.pallas_call(
        functools.partial(radiate_kernel, blocks),
        out_shape=jax.ShapeDtypeStruct((chunk, 2 * BINS), jnp.float32),
        in_specs=[vmem, vmem],
        out_specs=vmem,
        scratch_shapes=[
            pltpu.VMEM(shape, jnp.float32)
            for shape in [
                (BINS, 8, listeners), (BINS, 8, listeners), (listeners, 2 * BINS),
                (blocks, chunk, 2 * BINS), (blocks, chunk, 2 * BINS),
            ]
        ]
        + [pltpu.SemaphoreType.DMA((blocks,))] * 2,
        compiler_params=pltpu.CompilerParams(collective_id=2, has_side_effects=True),
    )(gathered, observers)
    return (populations_out, spectrum[None])


def solution(mesh):
    placed = (
        P("blk", None, "obs", None),
        P("blk", None),
        P("blk", None),
        P(("blk", "obs")),
        P(("blk", "obs"), None),
        P(("blk", "obs")),
        P(("blk", "obs")),
        P(None, ("blk", "obs")),
        P(None, ("blk", "obs")),
        P(None, "obs"),
    )
    return jax.shard_map(
        body,
        mesh=mesh,
        in_specs=placed,
        out_specs=(P("blk", None, "obs", None), P("obs", "blk", None)),
        check_vma=False,
    )
```

```python
import functools
import math

import jax
import jax.numpy as jnp
import numpy as np
from jax import lax
from jax.experimental import pallas as pl
from jax.experimental.pallas import tpu as pltpu
from jax.sharding import PartitionSpec as P

BS = 32
STEPS = 4
SAMPLES = 256
BINS = 64
P_OWN = 64


velocity_list = [
    (0, 0, 0),
    (1, 0, 0),
    (-1, 0, 0),
    (0, 1, 0),
    (0, -1, 0),
    (0, 0, 1),
    (0, 0, -1),
    (1, 1, 0),
    (-1, -1, 0),
    (1, -1, 0),
    (-1, 1, 0),
    (1, 0, 1),
    (-1, 0, -1),
    (1, 0, -1),
    (-1, 0, 1),
    (0, 1, 1),
    (0, -1, -1),
    (0, 1, -1),
    (0, -1, 1),
]
weight_list = [1.0 / 3.0] + [1.0 / 18.0] * 6 + [1.0 / 36.0] * 12
x_moving = [1, 2, 7, 8, 9, 10, 11, 12, 13, 14]
y_upward = [3, 7, 10, 15, 17]
y_downward = [4, 8, 9, 16, 18]
z_upward = [5, 11, 14, 15, 18]
z_downward = [6, 12, 13, 16, 17]
relax_rate = 1.6
pressure_gain = 60.0
sound_speed = 0.5


x_plus = [1, 7, 9, 11, 13]
x_minus = [2, 8, 10, 12, 14]
x_order = x_plus + x_minus
still = [0, 3, 4, 5, 6, 15, 16, 17, 18]
LANES = 128
FACE = 256


def collide_tile(f):
    sums = [None] * 19
    gaps = [None] * 19
    for number in range(1, 19, 2):
        sums[number] = f[number] + f[number + 1]
        gaps[number] = f[number] - f[number + 1]
    density = f[0]
    for number in range(1, 19, 2):
        density = density + sums[number]
    speeds = []
    for axis in range(3):
        total = None
        for number in range(1, 19, 2):
            sign = velocity_list[number][axis]
            if sign == 0:
                continue
            if total is None:
                total = gaps[number]
            elif sign == 1:
                total = total + gaps[number]
            else:
                total = total - gaps[number]
        speeds.append(total)
    inverse = 1.0 / density
    speeds = [speed * inverse for speed in speeds]
    squared = speeds[0] * speeds[0] + speeds[1] * speeds[1] + speeds[2] * speeds[2]
    base = 1.0 - 1.5 * squared
    keep = 1.0 - relax_rate
    out = [None] * 19
    out[0] = keep * f[0] + ((relax_rate * weight_list[0]) * density) * base
    scaled = {}
    thrice = {}
    for weight in sorted(set(weight_list[1:])):
        scaled[weight] = (relax_rate * weight) * density
        thrice[weight] = 3.0 * scaled[weight]
    for number in range(1, 19, 2):
        projected = None
        for axis in range(3):
            sign = velocity_list[number][axis]
            if sign == 0:
                continue
            if projected is None:
                projected = speeds[axis]
            elif sign == 1:
                projected = projected + speeds[axis]
            else:
                projected = projected - speeds[axis]
        weight = weight_list[number]
        even = scaled[weight] * (base + 4.5 * (projected * projected))
        odd = thrice[weight] * projected
        out[number] = keep * f[number] + (even + odd)
        out[number + 1] = keep * f[number + 1] + (even - odd)
    return out


def lane_of(shape):
    return lax.broadcasted_iota(jnp.int32, shape, 1)


def turned(value, amount):
    amount = amount % value.shape[1]
    return value if amount == 0 else pltpu.roll(value, amount, 1)


def pushed(value, low, high, sign):
    if sign == 1:
        return jnp.concatenate([low, value[:-1]], axis=0)
    return jnp.concatenate([value[1:], high], axis=0)


def shift_of(number):
    return velocity_list[number][1] * BS + velocity_list[number][2]


face_sets = [y_downward, y_upward, z_downward, z_upward]


def pack_tile(values, tile, tiles, chosen_numbers, columns, rows):
    depth = values[chosen_numbers[0]].shape[0]
    spot = lane_of((depth, LANES)) % BS
    quarter = lane_of((depth, LANES)) // BS
    u = tile % 4
    for side, (chosen, begin) in enumerate([(z_downward, 0), (z_upward, BS - 1)]):
        for j, number in enumerate(chosen):
            if number in chosen_numbers:
                moved = turned(values[number] - weight_list[number], 8 * u + j - begin)
                columns[side] = jnp.where(spot == 8 * u + j, moved, columns[side])
    for side, (chosen, at, begin) in enumerate(
        [(y_downward, 0, 0), (y_upward, tiles - 1, LANES - BS)]
    ):
        if tile != at:
            continue
        for j, number in enumerate(chosen):
            if number in chosen_numbers:
                moved = turned(values[number] - weight_list[number], j % 4 * BS - begin)
                rows[side][j // 4] = jnp.where(quarter == j % 4, moved, rows[side][j // 4])


def collide_all(field_ref, rolled_ref, moving_ref, edge_ref, draft_ref):
    depth = field_ref.shape[1]
    tiles = field_ref.shape[2] // LANES
    blank = jnp.zeros((depth, LANES), jnp.float32)
    rows = [[blank, blank], [blank, blank]]
    for half in range(tiles // 4):
        columns = [blank, blank]
        for u in range(4):
            tile = half * 4 + u
            lanes = slice(tile * LANES, (tile + 1) * LANES)
            out = collide_tile([field_ref[number, :, lanes] for number in range(19)])
            for number in range(19):
                if number in still:
                    rolled_ref[tile + 1, number] = turned(out[number], shift_of(number))
                else:
                    moving_ref[tile, x_order.index(number)] = out[number]
            for place, number in enumerate(x_plus):
                edge_ref[0, place, tile : tile + 1, :] = out[number][depth - 1 : depth]
            for place, number in enumerate(x_minus):
                edge_ref[1, place, tile : tile + 1, :] = out[number][0:1]
            pack_tile(out, tile, tiles, still, columns, rows)
        for side in range(2):
            draft_ref[2 + side, :, half * LANES : (half + 1) * LANES] = columns[side]
    for side in range(2):
        for half in range(2):
            draft_ref[side, :, half * LANES : (half + 1) * LANES] = rows[side][half]


def shifted(moving_ref, near_ref, tile, number):
    place = x_order.index(number)
    low = near_ref[0, place % 5, tile : tile + 1, :]
    high = near_ref[1, place % 5, tile : tile + 1, :]
    return pushed(moving_ref[tile, place], low, high, velocity_list[number][0])


def pack_moving(moving_ref, near_ref, draft_ref, piece_ref):
    tiles = moving_ref.shape[0]
    crossing = x_order[1:5] + x_order[6:]

    def draft(piece, half):
        return draft_ref[piece, :, half * LANES : (half + 1) * LANES]

    rows = [[draft(side, half) for half in range(2)] for side in range(2)]
    for half in range(tiles // 4):
        columns = [draft(2 + side, half) for side in range(2)]
        for u in range(4):
            tile = half * 4 + u
            values = {}
            for number in crossing:
                if velocity_list[number][1] == 0 or tile in (0, tiles - 1):
                    values[number] = shifted(moving_ref, near_ref, tile, number)
            pack_tile(values, tile, tiles, list(values), columns, rows)
        for side in range(2):
            piece_ref[2 + side, :, half * LANES : (half + 1) * LANES] = columns[side].astype(jnp.bfloat16)
    for side in range(2):
        for half in range(2):
            piece_ref[side, :, half * LANES : (half + 1) * LANES] = rows[side][half].astype(jnp.bfloat16)


def roll_moving(rolled_ref, moving_ref, near_ref):
    tiles = moving_ref.shape[0]
    for tile in range(tiles):
        for number in x_order:
            value = shifted(moving_ref, near_ref, tile, number)
            rolled_ref[tile + 1, number] = turned(value, shift_of(number))


def finish_step(face, edge, got_ref, rolled_ref, field_ref, density_ref):
    depth = field_ref.shape[1]
    tiles = field_ref.shape[2] // LANES
    lane = lane_of((depth, LANES))
    spot = lane % BS

    def arrived(source, half):
        return got_ref[source, :, half * LANES : (half + 1) * LANES].astype(jnp.float32)

    corners = {15: (0, 0, 1), 17: (1, 1, 31), 18: (2, 1, 65), 16: (3, 0, 31)}
    corner_lane = {15: 0, 17: BS - 1, 18: LANES - BS, 16: LANES - 1}
    for piece, source, pad, begin in [(1, face[0], 0, 0), (0, face[1], tiles + 1, LANES - BS)]:
        halves = [arrived(source, half) for half in range(2)]
        for j, number in enumerate(face_sets[piece]):
            shift_z = velocity_list[number][2]
            value = turned(halves[j // 4], begin + shift_z - j % 4 * BS)
            if number in corners:
                which, half, amount = corners[number]
                corner = turned(arrived(edge[which], half), amount)
                value = jnp.where(lane == corner_lane[number], corner, value)
            rolled_ref[pad, number] = value + weight_list[number]
    columns = {}
    for piece, source, rim in [(3, face[2], 0), (2, face[3], BS - 1)]:
        chosen = face_sets[piece]
        halves = [arrived(source, half) for half in range(2)]
        for tile in range(tiles):
            for j, number in enumerate(chosen):
                shift_y = velocity_list[number][1]
                amount = rim - 8 * (tile % 4) - j + BS * shift_y
                column = turned(halves[tile // 4], amount) + weight_list[number]
                value = jnp.where(spot == rim, column, rolled_ref[tile + 1, number])
                if shift_y != 0:
                    rolled_ref[tile + 1, number] = value
                else:
                    columns[tile, number] = value
                    field_ref[number, :, tile * LANES : (tile + 1) * LANES] = value
    for tile in range(tiles):
        lanes = slice(tile * LANES, (tile + 1) * LANES)
        total = None
        for number, (_, shift_y, shift_z) in enumerate(velocity_list):
            if shift_y == 0 and shift_z != 0:
                value = field_ref[number, :, lanes]
            else:
                value = rolled_ref[tile + 1, number]
                if shift_y == 1:
                    value = jnp.where(lane < BS, rolled_ref[tile, number], value)
                elif shift_y == -1:
                    value = jnp.where(lane >= LANES - BS, rolled_ref[tile + 2, number], value)
                field_ref[number, :, lanes] = value
            total = value if total is None else total + value
        density_ref[:, lanes] = total


def joined(left, right, left_axis, right_axis):
    return lax.dot_general(
        left.astype(jnp.bfloat16), right.astype(jnp.bfloat16),
        (((left_axis,), (right_axis,)), ((), ())), preferred_element_type=jnp.float32,
    )


def rows_of(shape):
    return lax.broadcasted_iota(jnp.int32, shape, 0)


def route(blocks, owner_ref, count, history_ref, select_ref, send_ref):
    slots = owner_ref.shape[1]
    room = send_ref.shape[1]
    width = history_ref.shape[1]
    owner = owner_ref[...]
    alive = lane_of((1, slots)) < count
    target = lax.shift_right_logical(owner, P_OWN.bit_length() - 1)
    spot = lax.bitwise_and(owner, P_OWN - 1)
    member = jnp.where((rows_of((blocks, slots)) == target) & alive, 1.0, 0.0)
    earlier = jnp.where(rows_of((slots, slots)) < lane_of((slots, slots)), 1.0, 0.0)
    before = joined(member, earlier, 1, 0)
    order = jnp.sum(before * member, axis=0, keepdims=True).astype(jnp.int32)
    label = jnp.where(alive, target * room + order, -1)
    select = jnp.where(rows_of((blocks * room, slots)) == label, 1.0, 0.0)
    select_ref[...] = select.astype(jnp.bfloat16)
    moved = joined(select, history_ref[...], 1, 0)
    spots = joined(select, jnp.where(rows_of((P_OWN, slots)) == spot, 1.0, 0.0), 1, 1)
    for block in range(blocks):
        rows = slice(block * room, (block + 1) * room)
        send_ref[block, :, 0:width] = moved[rows].astype(jnp.bfloat16)
        send_ref[block, :, width : width + P_OWN] = spots[rows].astype(jnp.bfloat16)


def unpacked(got_ref, flat_ref):
    blocks, room = got_ref.shape[0], got_ref.shape[1]
    for block in range(blocks):
        flat_ref[block * room : (block + 1) * room, :] = got_ref[block].astype(jnp.float32)


def settle_history(got_ref, flat_ref, choose_ref, table_ref, partial_ref):
    unpacked(got_ref, flat_ref)
    choose = flat_ref[:, 2 * SAMPLES : 2 * SAMPLES + P_OWN].astype(jnp.bfloat16)
    choose_ref[...] = choose
    owned = joined(choose, flat_ref[:, 0 : 2 * SAMPLES], 0, 0)
    for field in range(2):
        partial_ref[:, field * 2 * BINS : (field + 1) * 2 * BINS] = joined(
            owned[:, field * SAMPLES : (field + 1) * SAMPLES], table_ref[...], 1, 0
        )


def reading_of(density_ref, cell_ref, probe_ref):
    depth = density_ref.shape[0]
    count = density_ref.shape[1]
    excess = density_ref[...] - 1.0
    parts = []
    for _ in range(3):
        part = excess.astype(jnp.bfloat16).astype(jnp.float32)
        parts.append(part)
        excess = excess - part
    found = joined(jnp.concatenate(parts, axis=0), cell_ref[...], 1, 0)
    layers = found[0:depth] + found[depth : 2 * depth] + found[2 * depth : 3 * depth]
    layer = lax.div(probe_ref[...], count)
    mine = rows_of(layers.shape) == layer
    return jnp.sum(jnp.where(mine, layers, 0.0), axis=0, keepdims=True)


def prepare_waves(spot_got, listen_ref, wave_ref):
    ring = spot_got.shape[0]
    tiles = wave_ref.shape[0]
    angle_step = 2.0 * math.pi / SAMPLES / sound_speed
    for owner in range(ring):
        columns = spot_got[owner].T

        def one_group(group, columns=columns):
            rows = slice(group * 8, (group + 1) * 8)
            for tile in range(tiles):
                lanes = slice(tile * LANES, (tile + 1) * LANES)
                distance_sq = None
                facing = None
                for axis in range(3):
                    offset = listen_ref[axis : axis + 1, lanes] - columns[rows, axis : axis + 1]
                    square = offset * offset
                    along = columns[rows, axis + 3 : axis + 4] * offset
                    distance_sq = square if distance_sq is None else distance_sq + square
                    facing = along if facing is None else facing + along
                distance = jnp.sqrt(distance_sq)
                far = facing / (4.0 * math.pi * sound_speed * distance_sq)
                angle = angle_step * distance
                turn = jnp.cos(angle)
                at = owner * (P_OWN // 8) + group
                wave_ref[tile, at, 0] = far
                wave_ref[tile, at, 1] = jnp.zeros_like(far)
                wave_ref[tile, at, 2] = far * turn
                wave_ref[tile, at, 3] = far * jnp.sin(angle)
                wave_ref[tile, at, 4] = 2.0 * turn
                wave_ref[tile, at, 5] = sound_speed / distance

        for group in range(P_OWN // 8):
            one_group(group)


def spread_panels(panel_ref, wide_ref, first):
    groups, count = wide_ref.shape[0], wide_ref.shape[1]
    together = 4

    def some_groups(index, carry):
        at = index * together
        panels = [
            panel_ref[pl.ds(pl.multiple_of((at + step) * 8, 8), 8), :] for step in range(together)
        ]
        for part in range(4):
            for number in range(count):
                column = part * BINS + first + number
                for step in range(together):
                    wide_ref[at + step, number, part] = jnp.broadcast_to(
                        panels[step][:, column : column + 1], (8, LANES)
                    )
        return carry

    lax.fori_loop(0, groups // together, some_groups, 0)


def radiate_tile(wave_ref, panel_ref, wide_ref, sums_ref, total_ref):
    groups = wave_ref.shape[0]
    held = wide_ref.shape[1]
    span = 8
    unroll = 4
    for first in range(0, BINS, span):
        if held < BINS and first % held == 0:
            spread_panels(panel_ref, wide_ref, first)

        def add_groups(index, sums, first=first):
            sums = list(sums)
            for step in range(unroll):
                at = index * unroll + step
                old_cos, old_sin, now_cos, now_sin, twice, ratio = [wave_ref[at, i] for i in range(6)]
                for number in range(span):
                    k = first + number
                    press_real, press_imag, rate_real, rate_imag = [
                        wide_ref[at, k % held, part] for part in range(4)
                    ]
                    mixed_real = rate_real + ratio * press_real
                    mixed_imag = rate_imag + ratio * press_imag
                    real = mixed_real * now_cos + mixed_imag * now_sin
                    imag = mixed_imag * now_cos - mixed_real * now_sin
                    sums[number] = sums[number] + real
                    sums[span + number] = sums[span + number] + imag
                    if k + 1 < BINS:
                        old_cos, now_cos = now_cos, twice * now_cos - old_cos
                        old_sin, now_sin = now_sin, twice * now_sin - old_sin
                if first + span < BINS:
                    for i, value in enumerate([old_cos, old_sin, now_cos, now_sin]):
                        wave_ref[at, i] = value
            return tuple(sums)

        blank = jnp.zeros((8, LANES), jnp.float32)
        sums = lax.fori_loop(0, groups // unroll, add_groups, (blank,) * (2 * span))
        for number in range(span):
            k = first + number
            sums_ref[k * 8 : (k + 1) * 8, :] = sums[number]
            sums_ref[(BINS + k) * 8 : (BINS + k + 1) * 8, :] = sums[span + number]
    total = sums_ref[pl.ds(0, 2 * BINS, stride=8), :]
    for row in range(1, 8):
        total = total + sums_ref[pl.ds(row, 2 * BINS, stride=8), :]
    total_ref[...] = total


def window_kernel(
    blocks, ring, face_ref, rim_face_ref, count_ref, start_hbm, owner_ref, probe_ref, history_ref,
    place_ref, normal_ref, listen_ref, table_ref, tail_ref, final_hbm, out_ref,
    field_ref, density_ref, rolled_ref, moving_ref, edge_ref, near_ref, draft_ref, piece_ref,
    send_ref, got_even, got_odd, select_ref, cell_ref, past_send, past_got, flat_ref, choose_ref,
    partial_ref, fresh_ref, fresh_send, fresh_got, fresh_flat, done_ref, done_got, spot_ref, spot_got,
    wave_ref, panel_ref, wide_ref, sums_ref, total_ref, part_send, part_got,
    edge_send, edge_got, send_sem, got_sem, past_send_sem, past_got_sem, fresh_send_sem, fresh_got_sem,
    done_send_sem, done_got_sem, spot_send_sem, spot_got_sem,
    part_send_sem, part_got_sem, local_sem,
):
    mesh_ids = pl.DeviceIdType.MESH
    me = lax.axis_index("blk")
    side = lax.axis_index("obs")
    right = lax.rem(side + 1, ring)
    left = lax.rem(side + ring - 1, ring)
    barrier = pltpu.get_barrier_semaphore()
    slots = owner_ref.shape[1]

    def greet(distance, carry):
        peer = lax.rem(me + distance, blocks)
        pl.semaphore_signal(barrier, inc=1, device_id=(peer, side), device_id_type=mesh_ids)
        return carry

    for distance in range(1, ring):
        beside = lax.rem(side + distance, ring)
        pl.semaphore_signal(barrier, inc=1, device_id=(me, beside), device_id_type=mesh_ids)
    lax.fori_loop(1, blocks, greet, 0)
    face = [face_ref[0, k] for k in range(4)]
    edge = [rim_face_ref[0, k] for k in range(4)]
    load = pltpu.make_async_copy(start_hbm, field_ref, local_sem.at[0])
    load.start()
    route(blocks, owner_ref, count_ref[0], history_ref, select_ref, past_send)
    cell = lax.rem(probe_ref[...], field_ref.shape[2])
    cell_ref[...] = jnp.where(rows_of(cell_ref.shape) == cell, 1.0, 0.0).astype(jnp.bfloat16)
    spot_ref[...] = jnp.zeros_like(spot_ref)
    spot_ref[0:3, 0:P_OWN] = place_ref[...].astype(jnp.float32)
    spot_ref[3:6, 0:P_OWN] = normal_ref[...].astype(jnp.float32)
    fresh_ref[...] = jnp.zeros_like(fresh_ref)
    load.wait()

    def swap(source_of, into_ref, send_sems, got_sems, distance):
        peer = lax.rem(me + distance, blocks)
        return pltpu.make_async_remote_copy(
            src_ref=source_of(distance, peer),
            dst_ref=into_ref.at[me],
            send_sem=send_sems.at[distance],
            recv_sem=got_sems.at[distance],
            device_id=(peer, side),
            device_id_type=mesh_ids,
        )

    def every(action):
        def visit(distance, inner):
            action(distance)
            return inner

        lax.fori_loop(1, blocks, visit, 0)

    def past_copy(distance):
        return swap(lambda _, peer: past_send.at[peer], past_got, past_send_sem, past_got_sem, distance)

    def fresh_copy(distance):
        return swap(lambda _, peer: fresh_send.at[peer], fresh_got, fresh_send_sem, fresh_got_sem, distance)

    def ring_copies(source_ref, into_ref, send_sems, got_sems):
        return [
            pltpu.make_async_remote_copy(
                src_ref=source_ref,
                dst_ref=into_ref.at[side],
                send_sem=send_sems.at[distance],
                recv_sem=got_sems.at[distance],
                device_id=(me, lax.rem(side + distance, ring)),
                device_id_type=mesh_ids,
            )
            for distance in range(1, ring)
        ]

    def note(step):
        gained = pressure_gain * reading_of(density_ref.at[step], cell_ref, probe_ref)
        if step == 0:
            last = jnp.where(lane_of((8, 2 * SAMPLES)) == SAMPLES - 1, 1.0, 0.0)
            before = joined(last, history_ref[...], 1, 1)[0:1]
        else:
            before = fresh_ref[step - 1 : step, :]
        fresh_ref[step : step + 1, :] = gained
        fresh_ref[STEPS + step : STEPS + step + 1, :] = gained - before

    def one_step(step):
        got_ref = got_odd if step % 2 else got_even
        collide_all(field_ref, rolled_ref, moving_ref, edge_ref, draft_ref)
        if step == 0:
            pl.semaphore_wait(barrier, blocks + ring - 2)
        edges = [
            pltpu.make_async_remote_copy(
                src_ref=edge_ref.at[way],
                dst_ref=near_ref.at[step, way],
                send_sem=edge_send.at[step, way],
                recv_sem=edge_got.at[step, way],
                device_id=(me, beside),
                device_id_type=mesh_ids,
            )
            for way, beside in enumerate([right, left])
        ]
        for copy in edges:
            copy.start()
        for copy in edges:
            copy.wait()
        pack_moving(moving_ref, near_ref.at[step], draft_ref, piece_ref)

        def copy_to(distance):
            return swap(
                lambda number, _: send_ref.at[number], got_ref, send_sem.at[step], got_sem.at[step], distance
            )

        def begin(distance):
            peer = lax.rem(me + distance, blocks)
            up = (peer == face[1]) | (peer == edge[2]) | (peer == edge[3])
            piece = jnp.where(peer == face[3], 3, jnp.where(peer == face[2], 2, up.astype(jnp.int32)))
            send_ref[distance] = piece_ref[piece]
            copy_to(distance).start()

        every(begin)
        roll_moving(rolled_ref, moving_ref, near_ref.at[step])
        if step == 0:
            every(lambda distance: past_copy(distance).start())
            for copy in ring_copies(spot_ref, spot_got, spot_send_sem, spot_got_sem):
                copy.start()
            past_got[me] = past_send[me]
            spot_got[side] = spot_ref[...]
        else:
            note(step - 1)
        if step == 1:
            for copy in ring_copies(spot_ref, spot_got, spot_send_sem, spot_got_sem):
                copy.wait()
            prepare_waves(spot_got, listen_ref, wave_ref)
        if step == 2:
            every(lambda distance: past_copy(distance).wait())
            settle_history(past_got, flat_ref, choose_ref, table_ref, partial_ref)
        every(lambda distance: copy_to(distance).wait())
        finish_step(face, edge, got_ref, rolled_ref, field_ref, density_ref.at[step])

    for step in range(STEPS):
        one_step(step)
    unload = pltpu.make_async_copy(field_ref, final_hbm, local_sem.at[1])
    unload.start()
    note(STEPS - 1)
    fresh = joined(select_ref[...], fresh_ref[...], 1, 1)
    room = fresh_send.shape[1]
    for block in range(blocks):
        fresh_send[block] = fresh[block * room : (block + 1) * room].astype(jnp.bfloat16)
    every(lambda distance: fresh_copy(distance).start())
    fresh_got[me] = fresh_send[me]
    every(lambda distance: fresh_copy(distance).wait())
    unpacked(fresh_got, fresh_flat)
    newest = joined(choose_ref[...], fresh_flat[...], 0, 0)
    total = partial_ref[...] + joined(newest, tail_ref[...], 1, 0)
    done_ref[...] = total.astype(jnp.bfloat16)
    copies = ring_copies(done_ref, done_got, done_send_sem, done_got_sem)
    for copy in copies:
        copy.start()
    done_got[side] = done_ref[...]
    for copy in copies:
        copy.wait()
    for owner in range(ring):
        panel_ref[owner * P_OWN : (owner + 1) * P_OWN, :] = done_got[owner].astype(jnp.float32)
    if wide_ref.shape[1] == BINS:
        spread_panels(panel_ref, wide_ref, 0)
    chunk = out_ref.shape[0]
    tiles = wave_ref.shape[0]
    share = LANES // chunk

    def part_copy(peer):
        distance = lax.rem(peer - me + blocks, blocks)
        return pltpu.make_async_remote_copy(
            src_ref=part_send.at[peer],
            dst_ref=part_got.at[me],
            send_sem=part_send_sem.at[distance],
            recv_sem=part_got_sem.at[distance],
            device_id=(peer, side),
            device_id_type=mesh_ids,
        )

    def one_tile(turn, carry):
        tile = lax.rem(me // share + 1 + turn, tiles)
        radiate_tile(wave_ref.at[tile], panel_ref, wide_ref, sums_ref, total_ref)
        both = total_ref[...].T
        for number in range(share):
            part_send[tile * share + number] = both[number * chunk : (number + 1) * chunk]

        def launch(number, inner):
            peer = tile * share + number

            @pl.when(peer != me)
            def _():
                part_copy(peer).start()

            return inner

        lax.fori_loop(0, share, launch, 0)
        return carry

    lax.fori_loop(0, tiles, one_tile, 0)
    part_got[me] = part_send[me]
    every(lambda distance: part_copy(lax.rem(me + distance, blocks)).wait())
    out_ref[...] = jnp.sum(part_got[...], axis=0)
    unload.wait()


def transform_tables():
    moments = np.arange(SAMPLES)[:, None]
    harmonics = np.arange(BINS)[None, :] + 1
    turns = moments * harmonics % SAMPLES
    phases = turns.astype(np.float32) * np.float32(2.0 * math.pi / SAMPLES)
    table = np.concatenate([np.cos(phases), -np.sin(phases)], axis=1).astype(jnp.bfloat16)
    past = np.zeros_like(table)
    past[STEPS:] = table[: SAMPLES - STEPS]
    tail = np.zeros((LANES, 4 * BINS), table.dtype)
    for field in range(2):
        rows = slice(field * STEPS, (field + 1) * STEPS)
        tail[rows, field * 2 * BINS : (field + 1) * 2 * BINS] = table[SAMPLES - STEPS :]
    return jnp.asarray(past), jnp.asarray(tail)


def body(
    populations,
    block_faces,
    block_edges,
    probe_cell,
    history,
    panel_count,
    panel_owner,
    panel_pos,
    panel_normal,
    observers,
):
    blocks = lax.axis_size("blk")
    lattice_state = populations[0]
    slab_depth = lattice_state.shape[1]
    lane_count = lattice_state.shape[2]
    ring = lax.axis_size("obs")
    tiles = lane_count // LANES
    vmem = pl.BlockSpec(memory_space=pltpu.VMEM)
    smem = pl.BlockSpec(memory_space=pltpu.SMEM)
    anywhere = pl.BlockSpec(memory_space=pl.ANY)
    wide = jnp.float32
    half = jnp.bfloat16
    slots = panel_owner.shape[0]
    room = -(-slots // blocks)
    past, tail = transform_tables()
    dma = pltpu.SemaphoreType.DMA
    listeners = observers.shape[1]
    chunk = listeners // blocks
    held = BINS if ring * P_OWN <= 2 * LANES else BINS // 4
    lattice_state, spectrum = pl.pallas_call(
        functools.partial(window_kernel, blocks, ring),
        out_shape=[
            jax.ShapeDtypeStruct((19, slab_depth, lane_count), wide),
            jax.ShapeDtypeStruct((chunk, 2 * BINS), wide),
        ],
        in_specs=[smem] * 3 + [anywhere] + [vmem] * 8,
        out_specs=[anywhere, vmem],
        scratch_shapes=[
            pltpu.VMEM((19, slab_depth, lane_count), wide),
            pltpu.VMEM((STEPS, slab_depth, lane_count), wide),
            pltpu.VMEM((tiles + 2, 19, slab_depth, LANES), wide),
            pltpu.VMEM((tiles, len(x_order), slab_depth, LANES), wide),
            pltpu.VMEM((2, 5, tiles, LANES), wide),
            pltpu.VMEM((STEPS, 2, 5, tiles, LANES), wide),
            pltpu.VMEM((4, slab_depth, FACE), wide),
            pltpu.VMEM((4, slab_depth, FACE), half),
            pltpu.VMEM((blocks, slab_depth, FACE), half),
            pltpu.VMEM((blocks, slab_depth, FACE), half),
            pltpu.VMEM((blocks, slab_depth, FACE), half),
            pltpu.VMEM((blocks * room, slots), half),
            pltpu.VMEM((lane_count, slots), half),
            pltpu.VMEM((blocks, room, 5 * LANES), half),
            pltpu.VMEM((blocks, room, 5 * LANES), half),
            pltpu.VMEM((blocks * room, 5 * LANES), wide),
            pltpu.VMEM((blocks * room, P_OWN), half),
            pltpu.VMEM((P_OWN, 4 * BINS), wide),
            pltpu.VMEM((LANES, slots), wide),
            pltpu.VMEM((blocks, room, LANES), half),
            pltpu.VMEM((blocks, room, LANES), half),
            pltpu.VMEM((blocks * room, LANES), wide),
            pltpu.VMEM((P_OWN, 4 * BINS), half),
            pltpu.VMEM((ring, P_OWN, 4 * BINS), half),
            pltpu.VMEM((8, LANES), wide),
            pltpu.VMEM((ring, 8, LANES), wide),
            pltpu.VMEM((listeners // LANES, ring * P_OWN // 8, 6, 8, LANES), wide),
            pltpu.VMEM((ring * P_OWN, 4 * BINS), wide),
            pltpu.VMEM((ring * P_OWN // 8, held, 4, 8, LANES), wide),
            pltpu.VMEM((2 * BINS * 8, LANES), wide),
            pltpu.VMEM((2 * BINS, LANES), wide),
            pltpu.VMEM((blocks, chunk, 2 * BINS), wide),
            pltpu.VMEM((blocks, chunk, 2 * BINS), wide),
        ]
        + [dma((STEPS, 2))] * 2
        + [dma((STEPS, blocks))] * 2
        + [dma((blocks,))] * 4
        + [dma((ring,))] * 4
        + [dma((blocks,))] * 2
        + [dma((2,))],
        compiler_params=pltpu.CompilerParams(collective_id=0, has_side_effects=True),
    )(
        block_faces, block_edges, panel_count, lattice_state, panel_owner[None], probe_cell[None],
        history, panel_pos, panel_normal, observers, past, tail,
    )
    populations_out = lattice_state.reshape(1, 19, slab_depth, lane_count)
    return (populations_out, spectrum[None])


def solution(mesh):
    placed = (
        P("blk", None, "obs", None),
        P("blk", None),
        P("blk", None),
        P(("blk", "obs")),
        P(("blk", "obs"), None),
        P(("blk", "obs")),
        P(("blk", "obs")),
        P(None, ("blk", "obs")),
        P(None, ("blk", "obs")),
        P(None, "obs"),
    )
    return jax.shard_map(
        body,
        mesh=mesh,
        in_specs=placed,
        out_specs=(P("blk", None, "obs", None), P("obs", "blk", None)),
        check_vma=False,
    )
```

```python
import functools
import math

import jax
import jax.numpy as jnp
import numpy as np
from jax import lax
from jax.experimental import pallas as pl
from jax.experimental.pallas import tpu as pltpu
from jax.sharding import PartitionSpec as P

BS = 32
STEPS = 4
SAMPLES = 256
BINS = 64
P_OWN = 64


velocity_list = [
    (0, 0, 0),
    (1, 0, 0),
    (-1, 0, 0),
    (0, 1, 0),
    (0, -1, 0),
    (0, 0, 1),
    (0, 0, -1),
    (1, 1, 0),
    (-1, -1, 0),
    (1, -1, 0),
    (-1, 1, 0),
    (1, 0, 1),
    (-1, 0, -1),
    (1, 0, -1),
    (-1, 0, 1),
    (0, 1, 1),
    (0, -1, -1),
    (0, 1, -1),
    (0, -1, 1),
]
weight_list = [1.0 / 3.0] + [1.0 / 18.0] * 6 + [1.0 / 36.0] * 12
x_moving = [1, 2, 7, 8, 9, 10, 11, 12, 13, 14]
y_upward = [3, 7, 10, 15, 17]
y_downward = [4, 8, 9, 16, 18]
z_upward = [5, 11, 14, 15, 18]
z_downward = [6, 12, 13, 16, 17]
relax_rate = 1.6
pressure_gain = 60.0
sound_speed = 0.5


x_plus = [1, 7, 9, 11, 13]
x_minus = [2, 8, 10, 12, 14]
x_order = x_plus + x_minus
still = [0, 3, 4, 5, 6, 15, 16, 17, 18]
LANES = 128
FACE = 256


def collide_tile(f):
    sums = [None] * 19
    gaps = [None] * 19
    for number in range(1, 19, 2):
        sums[number] = f[number] + f[number + 1]
        gaps[number] = f[number] - f[number + 1]
    density = f[0]
    for number in range(1, 19, 2):
        density = density + sums[number]
    speeds = []
    for axis in range(3):
        total = None
        for number in range(1, 19, 2):
            sign = velocity_list[number][axis]
            if sign == 0:
                continue
            if total is None:
                total = gaps[number]
            elif sign == 1:
                total = total + gaps[number]
            else:
                total = total - gaps[number]
        speeds.append(total)
    inverse = 1.0 / density
    speeds = [speed * inverse for speed in speeds]
    squared = speeds[0] * speeds[0] + speeds[1] * speeds[1] + speeds[2] * speeds[2]
    base = 1.0 - 1.5 * squared
    keep = 1.0 - relax_rate
    out = [None] * 19
    out[0] = keep * f[0] + ((relax_rate * weight_list[0]) * density) * base
    scaled = {}
    thrice = {}
    for weight in sorted(set(weight_list[1:])):
        scaled[weight] = (relax_rate * weight) * density
        thrice[weight] = 3.0 * scaled[weight]
    for number in range(1, 19, 2):
        projected = None
        for axis in range(3):
            sign = velocity_list[number][axis]
            if sign == 0:
                continue
            if projected is None:
                projected = speeds[axis]
            elif sign == 1:
                projected = projected + speeds[axis]
            else:
                projected = projected - speeds[axis]
        weight = weight_list[number]
        even = scaled[weight] * (base + 4.5 * (projected * projected))
        odd = thrice[weight] * projected
        out[number] = keep * f[number] + (even + odd)
        out[number + 1] = keep * f[number + 1] + (even - odd)
    return out


def lane_of(shape):
    return lax.broadcasted_iota(jnp.int32, shape, 1)


def turned(value, amount):
    amount = amount % value.shape[1]
    return value if amount == 0 else pltpu.roll(value, amount, 1)


def pushed(value, low, high, sign):
    if sign == 1:
        return jnp.concatenate([low, value[:-1]], axis=0)
    return jnp.concatenate([value[1:], high], axis=0)


def shift_of(number):
    return velocity_list[number][1] * BS + velocity_list[number][2]


face_sets = [y_downward, y_upward, z_downward, z_upward]


def pack_tile(values, tile, tiles, chosen_numbers, columns, rows):
    depth = values[chosen_numbers[0]].shape[0]
    spot = lane_of((depth, LANES)) % BS
    quarter = lane_of((depth, LANES)) // BS
    u = tile % 4
    for side, (chosen, begin) in enumerate([(z_downward, 0), (z_upward, BS - 1)]):
        for j, number in enumerate(chosen):
            if number in chosen_numbers:
                moved = turned(values[number] - weight_list[number], 8 * u + j - begin)
                columns[side] = jnp.where(spot == 8 * u + j, moved, columns[side])
    for side, (chosen, at, begin) in enumerate(
        [(y_downward, 0, 0), (y_upward, tiles - 1, LANES - BS)]
    ):
        if tile != at:
            continue
        for j, number in enumerate(chosen):
            if number in chosen_numbers:
                moved = turned(values[number] - weight_list[number], j % 4 * BS - begin)
                rows[side][j // 4] = jnp.where(quarter == j % 4, moved, rows[side][j // 4])


def collide_all(field_ref, rolled_ref, moving_ref, edge_ref, draft_ref):
    depth = field_ref.shape[1]
    tiles = field_ref.shape[2] // LANES
    blank = jnp.zeros((depth, LANES), jnp.float32)
    rows = [[blank, blank], [blank, blank]]
    for half in range(tiles // 4):
        columns = [blank, blank]
        for u in range(4):
            tile = half * 4 + u
            lanes = slice(tile * LANES, (tile + 1) * LANES)
            out = collide_tile([field_ref[number, :, lanes] for number in range(19)])
            for number in range(19):
                if number in still:
                    rolled_ref[tile + 1, number] = turned(out[number], shift_of(number))
                else:
                    moving_ref[tile, x_order.index(number)] = out[number]
            for place, number in enumerate(x_plus):
                edge_ref[0, place, tile : tile + 1, :] = out[number][depth - 1 : depth]
            for place, number in enumerate(x_minus):
                edge_ref[1, place, tile : tile + 1, :] = out[number][0:1]
            pack_tile(out, tile, tiles, still, columns, rows)
        for side in range(2):
            draft_ref[2 + side, :, half * LANES : (half + 1) * LANES] = columns[side]
    for side in range(2):
        for half in range(2):
            draft_ref[side, :, half * LANES : (half + 1) * LANES] = rows[side][half]


def shifted(moving_ref, near_ref, tile, number):
    place = x_order.index(number)
    low = near_ref[0, place % 5, tile : tile + 1, :]
    high = near_ref[1, place % 5, tile : tile + 1, :]
    return pushed(moving_ref[tile, place], low, high, velocity_list[number][0])


def pack_moving(moving_ref, near_ref, draft_ref, piece_ref):
    tiles = moving_ref.shape[0]
    crossing = x_order[1:5] + x_order[6:]

    def draft(piece, half):
        return draft_ref[piece, :, half * LANES : (half + 1) * LANES]

    rows = [[draft(side, half) for half in range(2)] for side in range(2)]
    for half in range(tiles // 4):
        columns = [draft(2 + side, half) for side in range(2)]
        for u in range(4):
            tile = half * 4 + u
            values = {}
            for number in crossing:
                if velocity_list[number][1] == 0 or tile in (0, tiles - 1):
                    values[number] = shifted(moving_ref, near_ref, tile, number)
            pack_tile(values, tile, tiles, list(values), columns, rows)
        for side in range(2):
            piece_ref[2 + side, :, half * LANES : (half + 1) * LANES] = columns[side].astype(jnp.bfloat16)
    for side in range(2):
        for half in range(2):
            piece_ref[side, :, half * LANES : (half + 1) * LANES] = rows[side][half].astype(jnp.bfloat16)


def roll_moving(rolled_ref, moving_ref, near_ref):
    tiles = moving_ref.shape[0]
    for tile in range(tiles):
        for number in x_order:
            value = shifted(moving_ref, near_ref, tile, number)
            rolled_ref[tile + 1, number] = turned(value, shift_of(number))


def finish_step(face, edge, got_ref, rolled_ref, field_ref, density_ref):
    depth = field_ref.shape[1]
    tiles = field_ref.shape[2] // LANES
    lane = lane_of((depth, LANES))
    spot = lane % BS

    def arrived(source, half):
        return got_ref[source, :, half * LANES : (half + 1) * LANES].astype(jnp.float32)

    corners = {15: (0, 0, 1), 17: (1, 1, 31), 18: (2, 1, 65), 16: (3, 0, 31)}
    corner_lane = {15: 0, 17: BS - 1, 18: LANES - BS, 16: LANES - 1}
    for piece, source, pad, begin in [(1, face[0], 0, 0), (0, face[1], tiles + 1, LANES - BS)]:
        halves = [arrived(source, half) for half in range(2)]
        for j, number in enumerate(face_sets[piece]):
            shift_z = velocity_list[number][2]
            value = turned(halves[j // 4], begin + shift_z - j % 4 * BS)
            if number in corners:
                which, half, amount = corners[number]
                corner = turned(arrived(edge[which], half), amount)
                value = jnp.where(lane == corner_lane[number], corner, value)
            rolled_ref[pad, number] = value + weight_list[number]
    columns = {}
    for piece, source, rim in [(3, face[2], 0), (2, face[3], BS - 1)]:
        chosen = face_sets[piece]
        halves = [arrived(source, half) for half in range(2)]
        for tile in range(tiles):
            for j, number in enumerate(chosen):
                shift_y = velocity_list[number][1]
                amount = rim - 8 * (tile % 4) - j + BS * shift_y
                column = turned(halves[tile // 4], amount) + weight_list[number]
                value = jnp.where(spot == rim, column, rolled_ref[tile + 1, number])
                if shift_y != 0:
                    rolled_ref[tile + 1, number] = value
                else:
                    columns[tile, number] = value
                    field_ref[number, :, tile * LANES : (tile + 1) * LANES] = value
    for tile in range(tiles):
        lanes = slice(tile * LANES, (tile + 1) * LANES)
        total = None
        for number, (_, shift_y, shift_z) in enumerate(velocity_list):
            if shift_y == 0 and shift_z != 0:
                value = field_ref[number, :, lanes]
            else:
                value = rolled_ref[tile + 1, number]
                if shift_y == 1:
                    value = jnp.where(lane < BS, rolled_ref[tile, number], value)
                elif shift_y == -1:
                    value = jnp.where(lane >= LANES - BS, rolled_ref[tile + 2, number], value)
                field_ref[number, :, lanes] = value
            total = value if total is None else total + value
        density_ref[:, lanes] = total


def joined(left, right, left_axis, right_axis):
    return lax.dot_general(
        left.astype(jnp.bfloat16), right.astype(jnp.bfloat16),
        (((left_axis,), (right_axis,)), ((), ())), preferred_element_type=jnp.float32,
    )


def rows_of(shape):
    return lax.broadcasted_iota(jnp.int32, shape, 0)


def route(blocks, owner_ref, count, history_ref, select_ref, send_ref):
    slots = owner_ref.shape[1]
    room = send_ref.shape[1]
    width = history_ref.shape[1]
    owner = owner_ref[...]
    alive = lane_of((1, slots)) < count
    target = lax.shift_right_logical(owner, P_OWN.bit_length() - 1)
    spot = lax.bitwise_and(owner, P_OWN - 1)
    member = jnp.where((rows_of((blocks, slots)) == target) & alive, 1.0, 0.0)
    earlier = jnp.where(rows_of((slots, slots)) < lane_of((slots, slots)), 1.0, 0.0)
    before = joined(member, earlier, 1, 0)
    order = jnp.sum(before * member, axis=0, keepdims=True).astype(jnp.int32)
    label = jnp.where(alive, target * room + order, -1)
    select = jnp.where(rows_of((blocks * room, slots)) == label, 1.0, 0.0)
    select_ref[...] = select.astype(jnp.bfloat16)
    moved = joined(select, history_ref[...], 1, 0)
    spots = joined(select, jnp.where(rows_of((P_OWN, slots)) == spot, 1.0, 0.0), 1, 1)
    for block in range(blocks):
        rows = slice(block * room, (block + 1) * room)
        send_ref[block, :, 0:width] = moved[rows].astype(jnp.bfloat16)
        send_ref[block, :, width : width + P_OWN] = spots[rows].astype(jnp.bfloat16)


def unpacked(got_ref, flat_ref):
    blocks, room = got_ref.shape[0], got_ref.shape[1]
    for block in range(blocks):
        flat_ref[block * room : (block + 1) * room, :] = got_ref[block].astype(jnp.float32)


def settle_history(got_ref, flat_ref, choose_ref, table_ref, partial_ref):
    unpacked(got_ref, flat_ref)
    choose = flat_ref[:, 2 * SAMPLES : 2 * SAMPLES + P_OWN].astype(jnp.bfloat16)
    choose_ref[...] = choose
    owned = joined(choose, flat_ref[:, 0 : 2 * SAMPLES], 0, 0)
    for field in range(2):
        partial_ref[:, field * 2 * BINS : (field + 1) * 2 * BINS] = joined(
            owned[:, field * SAMPLES : (field + 1) * SAMPLES], table_ref[...], 1, 0
        )


def reading_of(density_ref, cell_ref, probe_ref):
    depth = density_ref.shape[0]
    count = density_ref.shape[1]
    excess = density_ref[...] - 1.0
    parts = []
    for _ in range(3):
        part = excess.astype(jnp.bfloat16).astype(jnp.float32)
        parts.append(part)
        excess = excess - part
    found = joined(jnp.concatenate(parts, axis=0), cell_ref[...], 1, 0)
    layers = found[0:depth] + found[depth : 2 * depth] + found[2 * depth : 3 * depth]
    layer = lax.div(probe_ref[...], count)
    mine = rows_of(layers.shape) == layer
    return jnp.sum(jnp.where(mine, layers, 0.0), axis=0, keepdims=True)


def prepare_waves(spot_got, listen_ref, wave_ref):
    ring = spot_got.shape[0]
    tiles, width = wave_ref.shape[0], wave_ref.shape[3]
    angle_step = 2.0 * math.pi / SAMPLES / sound_speed
    for owner in range(ring):
        columns = spot_got[owner].T[0:P_OWN]
        for group in range(P_OWN // 8):
            rows = slice(group * 8, (group + 1) * 8)
            into = slice(owner * P_OWN + group * 8, owner * P_OWN + (group + 1) * 8)
            for tile in range(tiles):
                lanes = slice(tile * width, (tile + 1) * width)
                distance_sq = None
                facing = None
                for axis in range(3):
                    offset = listen_ref[axis : axis + 1, lanes] - columns[rows, axis : axis + 1]
                    square = offset * offset
                    along = columns[rows, axis + 3 : axis + 4] * offset
                    distance_sq = square if distance_sq is None else distance_sq + square
                    facing = along if facing is None else facing + along
                distance = jnp.sqrt(distance_sq)
                far = facing / (4.0 * math.pi * sound_speed * distance_sq)
                angle = angle_step * distance
                turn = jnp.cos(angle)
                wave_ref[tile, 0, into] = far
                wave_ref[tile, 1, into] = jnp.zeros_like(far)
                wave_ref[tile, 2, into] = far * turn
                wave_ref[tile, 3, into] = far * jnp.sin(angle)
                wave_ref[tile, 4, into] = 2.0 * turn
                wave_ref[tile, 5, into] = sound_speed / distance


def weigh_panels(done_got, weight_ref):
    ring = done_got.shape[0]
    panels = ring * P_OWN
    values = jnp.concatenate([done_got[owner].astype(jnp.float32) for owner in range(ring)], axis=0).T
    press_real, press_imag, rate_real, rate_imag = [
        values[part * BINS : (part + 1) * BINS] for part in range(4)
    ]
    lines = [
        [rate_real, rate_imag, press_real, press_imag],
        [rate_imag, -rate_real, press_imag, -press_real],
    ]
    for row, line in enumerate(lines):
        for part, value in enumerate(line):
            for start in range(0, panels, LANES):
                at = (part * panels + start) // LANES
                weight_ref[at, pl.ds(row, BINS, stride=8), :] = value[:, start : start + LANES]


def radiate_tile(wave_ref, weight_ref, first_ref, second_ref, sums_ref, total_ref):
    panels = wave_ref.shape[1]
    span = first_ref.shape[0]
    for first in range(0, BINS, span):
        held_ref = second_ref if first // span % 2 else first_ref
        for start in range(0, panels, 32):
            rows = slice(start, start + 32)
            old_cos, old_sin, now_cos, now_sin, twice, ratio = [wave_ref[i, rows] for i in range(6)]
            for number in range(span):
                near = [now_cos, now_sin, ratio * now_cos, ratio * now_sin]
                for part, value in enumerate(near):
                    into = slice(part * panels + start, part * panels + start + 32)
                    held_ref[number, into] = value.astype(jnp.bfloat16)
                if first + number + 1 < BINS:
                    old_cos, now_cos = now_cos, twice * now_cos - old_cos
                    old_sin, now_sin = now_sin, twice * now_sin - old_sin
            if first + span < BINS:
                for i, value in enumerate([old_cos, old_sin, now_cos, now_sin]):
                    wave_ref[i, rows] = value
        for number in range(span):
            rows = slice((first + number) * 8, (first + number + 1) * 8)
            weights = jnp.concatenate(
                [weight_ref[at, rows, :] for at in range(weight_ref.shape[0])], axis=1
            )
            found = joined(weights, held_ref[number], 1, 0)
            for part in range(sums_ref.shape[0]):
                sums_ref[part, rows, :] = found[:, part * LANES : (part + 1) * LANES]
    for part in range(sums_ref.shape[0]):
        total_ref[part, 0:BINS] = sums_ref[part, pl.ds(0, BINS, stride=8), :]
        total_ref[part, BINS : 2 * BINS] = sums_ref[part, pl.ds(1, BINS, stride=8), :]


def window_kernel(
    blocks, ring, face_ref, rim_face_ref, count_ref, start_hbm, owner_ref, probe_ref, history_ref,
    place_ref, normal_ref, listen_ref, table_ref, tail_ref, final_hbm, out_ref,
    field_ref, density_ref, rolled_ref, moving_ref, edge_ref, near_ref, draft_ref, piece_ref,
    send_ref, got_even, got_odd, select_ref, cell_ref, past_send, past_got, flat_ref, choose_ref,
    partial_ref, fresh_ref, fresh_send, fresh_got, fresh_flat, done_ref, done_got, spot_ref, spot_got,
    wave_ref, weight_ref, first_ref, second_ref, sums_ref, total_ref, part_send, part_got,
    edge_send, edge_got, send_sem, got_sem, past_send_sem, past_got_sem, fresh_send_sem, fresh_got_sem,
    done_send_sem, done_got_sem, spot_send_sem, spot_got_sem,
    part_send_sem, part_got_sem, local_sem,
):
    mesh_ids = pl.DeviceIdType.MESH
    me = lax.axis_index("blk")
    side = lax.axis_index("obs")
    right = lax.rem(side + 1, ring)
    left = lax.rem(side + ring - 1, ring)
    barrier = pltpu.get_barrier_semaphore()
    slots = owner_ref.shape[1]

    def greet(distance, carry):
        peer = lax.rem(me + distance, blocks)
        pl.semaphore_signal(barrier, inc=1, device_id=(peer, side), device_id_type=mesh_ids)
        return carry

    for distance in range(1, ring):
        beside = lax.rem(side + distance, ring)
        pl.semaphore_signal(barrier, inc=1, device_id=(me, beside), device_id_type=mesh_ids)
    lax.fori_loop(1, blocks, greet, 0)
    face = [face_ref[0, k] for k in range(4)]
    edge = [rim_face_ref[0, k] for k in range(4)]
    load = pltpu.make_async_copy(start_hbm, field_ref, local_sem.at[0])
    load.start()
    route(blocks, owner_ref, count_ref[0], history_ref, select_ref, past_send)
    cell = lax.rem(probe_ref[...], field_ref.shape[2])
    cell_ref[...] = jnp.where(rows_of(cell_ref.shape) == cell, 1.0, 0.0).astype(jnp.bfloat16)
    spot_ref[...] = jnp.zeros_like(spot_ref)
    spot_ref[0:3, 0:P_OWN] = place_ref[...].astype(jnp.float32)
    spot_ref[3:6, 0:P_OWN] = normal_ref[...].astype(jnp.float32)
    fresh_ref[...] = jnp.zeros_like(fresh_ref)
    load.wait()

    def swap(source_of, into_ref, send_sems, got_sems, distance):
        peer = lax.rem(me + distance, blocks)
        return pltpu.make_async_remote_copy(
            src_ref=source_of(distance, peer),
            dst_ref=into_ref.at[me],
            send_sem=send_sems.at[distance],
            recv_sem=got_sems.at[distance],
            device_id=(peer, side),
            device_id_type=mesh_ids,
        )

    def every(action):
        def visit(distance, inner):
            action(distance)
            return inner

        lax.fori_loop(1, blocks, visit, 0)

    def past_copy(distance):
        return swap(lambda _, peer: past_send.at[peer], past_got, past_send_sem, past_got_sem, distance)

    def fresh_copy(distance):
        return swap(lambda _, peer: fresh_send.at[peer], fresh_got, fresh_send_sem, fresh_got_sem, distance)

    def ring_copies(source_ref, into_ref, send_sems, got_sems):
        return [
            pltpu.make_async_remote_copy(
                src_ref=source_ref,
                dst_ref=into_ref.at[side],
                send_sem=send_sems.at[distance],
                recv_sem=got_sems.at[distance],
                device_id=(me, lax.rem(side + distance, ring)),
                device_id_type=mesh_ids,
            )
            for distance in range(1, ring)
        ]

    def note(step):
        gained = pressure_gain * reading_of(density_ref.at[step], cell_ref, probe_ref)
        if step == 0:
            last = jnp.where(lane_of((8, 2 * SAMPLES)) == SAMPLES - 1, 1.0, 0.0)
            before = joined(last, history_ref[...], 1, 1)[0:1]
        else:
            before = fresh_ref[step - 1 : step, :]
        fresh_ref[step : step + 1, :] = gained
        fresh_ref[STEPS + step : STEPS + step + 1, :] = gained - before

    def one_step(step):
        got_ref = got_odd if step % 2 else got_even
        collide_all(field_ref, rolled_ref, moving_ref, edge_ref, draft_ref)
        if step == 0:
            pl.semaphore_wait(barrier, blocks + ring - 2)
        edges = [
            pltpu.make_async_remote_copy(
                src_ref=edge_ref.at[way],
                dst_ref=near_ref.at[step, way],
                send_sem=edge_send.at[step, way],
                recv_sem=edge_got.at[step, way],
                device_id=(me, beside),
                device_id_type=mesh_ids,
            )
            for way, beside in enumerate([right, left])
        ]
        for copy in edges:
            copy.start()
        for copy in edges:
            copy.wait()
        pack_moving(moving_ref, near_ref.at[step], draft_ref, piece_ref)

        def copy_to(distance):
            return swap(
                lambda number, _: send_ref.at[number], got_ref, send_sem.at[step], got_sem.at[step], distance
            )

        def begin(distance):
            peer = lax.rem(me + distance, blocks)
            up = (peer == face[1]) | (peer == edge[2]) | (peer == edge[3])
            piece = jnp.where(peer == face[3], 3, jnp.where(peer == face[2], 2, up.astype(jnp.int32)))
            send_ref[distance] = piece_ref[piece]
            copy_to(distance).start()

        every(begin)
        roll_moving(rolled_ref, moving_ref, near_ref.at[step])
        if step == 0:
            every(lambda distance: past_copy(distance).start())
            for copy in ring_copies(spot_ref, spot_got, spot_send_sem, spot_got_sem):
                copy.start()
            past_got[me] = past_send[me]
            spot_got[side] = spot_ref[...]
        else:
            note(step - 1)
        if step == 1:
            for copy in ring_copies(spot_ref, spot_got, spot_send_sem, spot_got_sem):
                copy.wait()
            prepare_waves(spot_got, listen_ref, wave_ref)
        if step == 2:
            every(lambda distance: past_copy(distance).wait())
            settle_history(past_got, flat_ref, choose_ref, table_ref, partial_ref)
        every(lambda distance: copy_to(distance).wait())
        finish_step(face, edge, got_ref, rolled_ref, field_ref, density_ref.at[step])

    for step in range(STEPS):
        one_step(step)
    unload = pltpu.make_async_copy(field_ref, final_hbm, local_sem.at[1])
    unload.start()
    note(STEPS - 1)
    fresh = joined(select_ref[...], fresh_ref[...], 1, 1)
    room = fresh_send.shape[1]
    for block in range(blocks):
        fresh_send[block] = fresh[block * room : (block + 1) * room].astype(jnp.bfloat16)
    every(lambda distance: fresh_copy(distance).start())
    fresh_got[me] = fresh_send[me]
    every(lambda distance: fresh_copy(distance).wait())
    unpacked(fresh_got, fresh_flat)
    newest = joined(choose_ref[...], fresh_flat[...], 0, 0)
    total = partial_ref[...] + joined(newest, tail_ref[...], 1, 0)
    done_ref[...] = total.astype(jnp.bfloat16)
    copies = ring_copies(done_ref, done_got, done_send_sem, done_got_sem)
    for copy in copies:
        copy.start()
    done_got[side] = done_ref[...]
    for copy in copies:
        copy.wait()
    weigh_panels(done_got, weight_ref)
    chunk = out_ref.shape[0]
    tiles = wave_ref.shape[0]
    share = wave_ref.shape[3] // chunk

    def part_copy(peer):
        distance = lax.rem(peer - me + blocks, blocks)
        return pltpu.make_async_remote_copy(
            src_ref=part_send.at[peer],
            dst_ref=part_got.at[me],
            send_sem=part_send_sem.at[distance],
            recv_sem=part_got_sem.at[distance],
            device_id=(peer, side),
            device_id_type=mesh_ids,
        )

    def one_tile(turn, carry):
        tile = lax.rem(me // share + 1 + turn, tiles)
        radiate_tile(wave_ref.at[tile], weight_ref, first_ref, second_ref, sums_ref, total_ref)
        each = LANES // chunk
        for part in range(total_ref.shape[0]):
            both = total_ref[part].T
            for number in range(each):
                rows = slice(number * chunk, (number + 1) * chunk)
                part_send[tile * share + part * each + number] = both[rows]

        def launch(number, inner):
            peer = tile * share + number

            @pl.when(peer != me)
            def _():
                part_copy(peer).start()

            return inner

        lax.fori_loop(0, share, launch, 0)
        return carry

    lax.fori_loop(0, tiles, one_tile, 0)
    part_got[me] = part_send[me]
    every(lambda distance: part_copy(lax.rem(me + distance, blocks)).wait())
    out_ref[...] = jnp.sum(part_got[...], axis=0)
    unload.wait()


def transform_tables():
    moments = np.arange(SAMPLES)[:, None]
    harmonics = np.arange(BINS)[None, :] + 1
    turns = moments * harmonics % SAMPLES
    phases = turns.astype(np.float32) * np.float32(2.0 * math.pi / SAMPLES)
    table = np.concatenate([np.cos(phases), -np.sin(phases)], axis=1).astype(jnp.bfloat16)
    past = np.zeros_like(table)
    past[STEPS:] = table[: SAMPLES - STEPS]
    tail = np.zeros((LANES, 4 * BINS), table.dtype)
    for field in range(2):
        rows = slice(field * STEPS, (field + 1) * STEPS)
        tail[rows, field * 2 * BINS : (field + 1) * 2 * BINS] = table[SAMPLES - STEPS :]
    return jnp.asarray(past), jnp.asarray(tail)


def body(
    populations,
    block_faces,
    block_edges,
    probe_cell,
    history,
    panel_count,
    panel_owner,
    panel_pos,
    panel_normal,
    observers,
):
    blocks = lax.axis_size("blk")
    lattice_state = populations[0]
    slab_depth = lattice_state.shape[1]
    lane_count = lattice_state.shape[2]
    ring = lax.axis_size("obs")
    tiles = lane_count // LANES
    vmem = pl.BlockSpec(memory_space=pltpu.VMEM)
    smem = pl.BlockSpec(memory_space=pltpu.SMEM)
    anywhere = pl.BlockSpec(memory_space=pl.ANY)
    wide = jnp.float32
    half = jnp.bfloat16
    slots = panel_owner.shape[0]
    room = -(-slots // blocks)
    past, tail = transform_tables()
    dma = pltpu.SemaphoreType.DMA
    listeners = observers.shape[1]
    chunk = listeners // blocks
    width = min(2 * LANES, listeners)
    lattice_state, spectrum = pl.pallas_call(
        functools.partial(window_kernel, blocks, ring),
        out_shape=[
            jax.ShapeDtypeStruct((19, slab_depth, lane_count), wide),
            jax.ShapeDtypeStruct((chunk, 2 * BINS), wide),
        ],
        in_specs=[smem] * 3 + [anywhere] + [vmem] * 8,
        out_specs=[anywhere, vmem],
        scratch_shapes=[
            pltpu.VMEM((19, slab_depth, lane_count), wide),
            pltpu.VMEM((STEPS, slab_depth, lane_count), wide),
            pltpu.VMEM((tiles + 2, 19, slab_depth, LANES), wide),
            pltpu.VMEM((tiles, len(x_order), slab_depth, LANES), wide),
            pltpu.VMEM((2, 5, tiles, LANES), wide),
            pltpu.VMEM((STEPS, 2, 5, tiles, LANES), wide),
            pltpu.VMEM((4, slab_depth, FACE), wide),
            pltpu.VMEM((4, slab_depth, FACE), half),
            pltpu.VMEM((blocks, slab_depth, FACE), half),
            pltpu.VMEM((blocks, slab_depth, FACE), half),
            pltpu.VMEM((blocks, slab_depth, FACE), half),
            pltpu.VMEM((blocks * room, slots), half),
            pltpu.VMEM((lane_count, slots), half),
            pltpu.VMEM((blocks, room, 5 * LANES), half),
            pltpu.VMEM((blocks, room, 5 * LANES), half),
            pltpu.VMEM((blocks * room, 5 * LANES), wide),
            pltpu.VMEM((blocks * room, P_OWN), half),
            pltpu.VMEM((P_OWN, 4 * BINS), wide),
            pltpu.VMEM((LANES, slots), wide),
            pltpu.VMEM((blocks, room, LANES), half),
            pltpu.VMEM((blocks, room, LANES), half),
            pltpu.VMEM((blocks * room, LANES), wide),
            pltpu.VMEM((P_OWN, 4 * BINS), half),
            pltpu.VMEM((ring, P_OWN, 4 * BINS), half),
            pltpu.VMEM((8, LANES), wide),
            pltpu.VMEM((ring, 8, LANES), wide),
            pltpu.VMEM((listeners // width, 6, ring * P_OWN, width), wide),
            pltpu.VMEM((4 * ring * P_OWN // LANES, BINS * 8, LANES), wide),
            pltpu.VMEM((8, 4 * ring * P_OWN, width), half),
            pltpu.VMEM((8, 4 * ring * P_OWN, width), half),
            pltpu.VMEM((width // LANES, BINS * 8, LANES), wide),
            pltpu.VMEM((width // LANES, 2 * BINS, LANES), wide),
            pltpu.VMEM((blocks, chunk, 2 * BINS), wide),
            pltpu.VMEM((blocks, chunk, 2 * BINS), wide),
        ]
        + [dma((STEPS, 2))] * 2
        + [dma((STEPS, blocks))] * 2
        + [dma((blocks,))] * 4
        + [dma((ring,))] * 4
        + [dma((blocks,))] * 2
        + [dma((2,))],
        compiler_params=pltpu.CompilerParams(collective_id=0, has_side_effects=True),
    )(
        block_faces, block_edges, panel_count, lattice_state, panel_owner[None], probe_cell[None],
        history, panel_pos, panel_normal, observers, past, tail,
    )
    populations_out = lattice_state.reshape(1, 19, slab_depth, lane_count)
    return (populations_out, spectrum[None])


def solution(mesh):
    placed = (
        P("blk", None, "obs", None),
        P("blk", None),
        P("blk", None),
        P(("blk", "obs")),
        P(("blk", "obs"), None),
        P(("blk", "obs")),
        P(("blk", "obs")),
        P(None, ("blk", "obs")),
        P(None, ("blk", "obs")),
        P(None, "obs"),
    )
    return jax.shard_map(
        body,
        mesh=mesh,
        in_specs=placed,
        out_specs=(P("blk", None, "obs", None), P("obs", "blk", None)),
        check_vma=False,
    )
```

```python
import functools
import math

import jax
import jax.numpy as jnp
import numpy as np
from jax import lax
from jax.experimental import pallas as pl
from jax.experimental.pallas import tpu as pltpu
from jax.sharding import PartitionSpec as P

BS = 32
STEPS = 4
SAMPLES = 256
BINS = 64
P_OWN = 64


velocity_list = [
    (0, 0, 0),
    (1, 0, 0),
    (-1, 0, 0),
    (0, 1, 0),
    (0, -1, 0),
    (0, 0, 1),
    (0, 0, -1),
    (1, 1, 0),
    (-1, -1, 0),
    (1, -1, 0),
    (-1, 1, 0),
    (1, 0, 1),
    (-1, 0, -1),
    (1, 0, -1),
    (-1, 0, 1),
    (0, 1, 1),
    (0, -1, -1),
    (0, 1, -1),
    (0, -1, 1),
]
weight_list = [1.0 / 3.0] + [1.0 / 18.0] * 6 + [1.0 / 36.0] * 12
x_moving = [1, 2, 7, 8, 9, 10, 11, 12, 13, 14]
y_upward = [3, 7, 10, 15, 17]
y_downward = [4, 8, 9, 16, 18]
z_upward = [5, 11, 14, 15, 18]
z_downward = [6, 12, 13, 16, 17]
relax_rate = 1.6
pressure_gain = 60.0
sound_speed = 0.5


x_plus = [1, 7, 9, 11, 13]
x_minus = [2, 8, 10, 12, 14]
x_order = x_plus + x_minus
still = [0, 3, 4, 5, 6, 15, 16, 17, 18]
LANES = 128
FACE = 256


def collide_tile(f):
    sums = [None] * 19
    gaps = [None] * 19
    for number in range(1, 19, 2):
        sums[number] = f[number] + f[number + 1]
        gaps[number] = f[number] - f[number + 1]
    density = f[0]
    for number in range(1, 19, 2):
        density = density + sums[number]
    speeds = []
    for axis in range(3):
        total = None
        for number in range(1, 19, 2):
            sign = velocity_list[number][axis]
            if sign == 0:
                continue
            if total is None:
                total = gaps[number]
            elif sign == 1:
                total = total + gaps[number]
            else:
                total = total - gaps[number]
        speeds.append(total)
    inverse = 1.0 / density
    speeds = [speed * inverse for speed in speeds]
    squared = speeds[0] * speeds[0] + speeds[1] * speeds[1] + speeds[2] * speeds[2]
    base = 1.0 - 1.5 * squared
    keep = 1.0 - relax_rate
    out = [None] * 19
    out[0] = keep * f[0] + ((relax_rate * weight_list[0]) * density) * base
    scaled = {}
    thrice = {}
    for weight in sorted(set(weight_list[1:])):
        scaled[weight] = (relax_rate * weight) * density
        thrice[weight] = 3.0 * scaled[weight]
    for number in range(1, 19, 2):
        projected = None
        for axis in range(3):
            sign = velocity_list[number][axis]
            if sign == 0:
                continue
            if projected is None:
                projected = speeds[axis]
            elif sign == 1:
                projected = projected + speeds[axis]
            else:
                projected = projected - speeds[axis]
        weight = weight_list[number]
        even = scaled[weight] * (base + 4.5 * (projected * projected))
        odd = thrice[weight] * projected
        out[number] = keep * f[number] + (even + odd)
        out[number + 1] = keep * f[number + 1] + (even - odd)
    return out


def lane_of(shape):
    return lax.broadcasted_iota(jnp.int32, shape, 1)


def turned(value, amount):
    amount = amount % value.shape[1]
    return value if amount == 0 else pltpu.roll(value, amount, 1)


def pushed(value, low, high, sign):
    if sign == 1:
        return jnp.concatenate([low, value[:-1]], axis=0)
    return jnp.concatenate([value[1:], high], axis=0)


def shift_of(number):
    return velocity_list[number][1] * BS + velocity_list[number][2]


face_sets = [y_downward, y_upward, z_downward, z_upward]


def pack_tile(values, tile, tiles, chosen_numbers, columns, rows):
    depth = values[chosen_numbers[0]].shape[0]
    spot = lane_of((depth, LANES)) % BS
    quarter = lane_of((depth, LANES)) // BS
    u = tile % 4
    for side, (chosen, begin) in enumerate([(z_downward, 0), (z_upward, BS - 1)]):
        for j, number in enumerate(chosen):
            if number in chosen_numbers:
                moved = turned(values[number] - weight_list[number], 8 * u + j - begin)
                columns[side] = jnp.where(spot == 8 * u + j, moved, columns[side])
    for side, (chosen, at, begin) in enumerate(
        [(y_downward, 0, 0), (y_upward, tiles - 1, LANES - BS)]
    ):
        if tile != at:
            continue
        for j, number in enumerate(chosen):
            if number in chosen_numbers:
                moved = turned(values[number] - weight_list[number], j % 4 * BS - begin)
                rows[side][j // 4] = jnp.where(quarter == j % 4, moved, rows[side][j // 4])


def collide_all(field_ref, rolled_ref, moving_ref, draft_ref):
    depth = field_ref.shape[1]
    tiles = field_ref.shape[2] // LANES
    blank = jnp.zeros((depth, LANES), jnp.float32)
    rows = [[blank, blank], [blank, blank]]
    for half in range(tiles // 4):
        columns = [blank, blank]
        for u in range(4):
            tile = half * 4 + u
            lanes = slice(tile * LANES, (tile + 1) * LANES)
            out = collide_tile([field_ref[number, :, lanes] for number in range(19)])
            for number in range(19):
                if number in still:
                    rolled_ref[tile + 1, number] = turned(out[number], shift_of(number))
                else:
                    moving_ref[tile, x_order.index(number)] = out[number]
            pack_tile(out, tile, tiles, still, columns, rows)
        for side in range(2):
            draft_ref[2 + side, :, half * LANES : (half + 1) * LANES] = columns[side]
    for side in range(2):
        for half in range(2):
            draft_ref[side, :, half * LANES : (half + 1) * LANES] = rows[side][half]


def keep_rim(rim_ref, number, tile, value):
    depth = value.shape[0]
    tiles = rim_ref.shape[1] // 2
    rim_ref[number, tile : tile + 1, :] = value[depth - 1 : depth]
    rim_ref[number, tiles + tile : tiles + tile + 1, :] = value[0:1]


def collide_rim(rim_ref, edge_ref):
    tiles = rim_ref.shape[1] // 2
    out = collide_tile([rim_ref[number] for number in range(19)])
    for place, number in enumerate(x_plus):
        edge_ref[0, place] = out[number][0:tiles]
    for place, number in enumerate(x_minus):
        edge_ref[1, place] = out[number][tiles : 2 * tiles]


def shifted(moving_ref, near_ref, tile, number):
    place = x_order.index(number)
    low = near_ref[0, place % 5, tile : tile + 1, :]
    high = near_ref[1, place % 5, tile : tile + 1, :]
    return pushed(moving_ref[tile, place], low, high, velocity_list[number][0])


def pack_moving(moving_ref, near_ref, draft_ref, piece_ref):
    tiles = moving_ref.shape[0]
    crossing = x_order[1:5] + x_order[6:]

    def draft(piece, half):
        return draft_ref[piece, :, half * LANES : (half + 1) * LANES]

    rows = [[draft(side, half) for half in range(2)] for side in range(2)]
    for half in range(tiles // 4):
        columns = [draft(2 + side, half) for side in range(2)]
        for u in range(4):
            tile = half * 4 + u
            values = {}
            for number in crossing:
                if velocity_list[number][1] == 0 or tile in (0, tiles - 1):
                    values[number] = shifted(moving_ref, near_ref, tile, number)
            pack_tile(values, tile, tiles, list(values), columns, rows)
        for side in range(2):
            piece_ref[2 + side, :, half * LANES : (half + 1) * LANES] = columns[side].astype(jnp.bfloat16)
    for side in range(2):
        for half in range(2):
            piece_ref[side, :, half * LANES : (half + 1) * LANES] = rows[side][half].astype(jnp.bfloat16)


def roll_moving(rolled_ref, moving_ref, near_ref):
    tiles = moving_ref.shape[0]
    for tile in range(tiles):
        for number in x_order:
            value = shifted(moving_ref, near_ref, tile, number)
            rolled_ref[tile + 1, number] = turned(value, shift_of(number))


def finish_step(face, edge, got_ref, rolled_ref, field_ref, rim_ref, density_ref, last):
    depth = field_ref.shape[1]
    tiles = field_ref.shape[2] // LANES
    lane = lane_of((depth, LANES))
    spot = lane % BS

    def arrived(source, half):
        return got_ref[source, :, half * LANES : (half + 1) * LANES].astype(jnp.float32)

    corners = {15: (0, 0, 1), 17: (1, 1, 31), 18: (2, 1, 65), 16: (3, 0, 31)}
    corner_lane = {15: 0, 17: BS - 1, 18: LANES - BS, 16: LANES - 1}
    for piece, source, pad, begin in [(1, face[0], 0, 0), (0, face[1], tiles + 1, LANES - BS)]:
        halves = [arrived(source, half) for half in range(2)]
        for j, number in enumerate(face_sets[piece]):
            shift_z = velocity_list[number][2]
            value = turned(halves[j // 4], begin + shift_z - j % 4 * BS)
            if number in corners:
                which, half, amount = corners[number]
                corner = turned(arrived(edge[which], half), amount)
                value = jnp.where(lane == corner_lane[number], corner, value)
            rolled_ref[pad, number] = value + weight_list[number]
    columns = {}
    for piece, source, rim in [(3, face[2], 0), (2, face[3], BS - 1)]:
        chosen = face_sets[piece]
        halves = [arrived(source, half) for half in range(2)]
        for tile in range(tiles):
            for j, number in enumerate(chosen):
                shift_y = velocity_list[number][1]
                amount = rim - 8 * (tile % 4) - j + BS * shift_y
                column = turned(halves[tile // 4], amount) + weight_list[number]
                value = jnp.where(spot == rim, column, rolled_ref[tile + 1, number])
                if shift_y != 0:
                    rolled_ref[tile + 1, number] = value
                else:
                    columns[tile, number] = value
                    field_ref[number, :, tile * LANES : (tile + 1) * LANES] = value
    for tile in range(tiles):
        lanes = slice(tile * LANES, (tile + 1) * LANES)
        total = None
        for number, (_, shift_y, shift_z) in enumerate(velocity_list):
            if shift_y == 0 and shift_z != 0:
                value = field_ref[number, :, lanes]
            else:
                value = rolled_ref[tile + 1, number]
                if shift_y == 1:
                    value = jnp.where(lane < BS, rolled_ref[tile, number], value)
                elif shift_y == -1:
                    value = jnp.where(lane >= LANES - BS, rolled_ref[tile + 2, number], value)
                field_ref[number, :, lanes] = value
            if not last:
                keep_rim(rim_ref, number, tile, value)
            total = value if total is None else total + value
        density_ref[:, lanes] = total


def joined(left, right, left_axis, right_axis):
    return lax.dot_general(
        left.astype(jnp.bfloat16), right.astype(jnp.bfloat16),
        (((left_axis,), (right_axis,)), ((), ())), preferred_element_type=jnp.float32,
    )


def rows_of(shape):
    return lax.broadcasted_iota(jnp.int32, shape, 0)


def route(blocks, owner_ref, count, history_ref, select_ref, send_ref):
    slots = owner_ref.shape[1]
    room = send_ref.shape[1]
    width = history_ref.shape[1]
    owner = owner_ref[...]
    alive = lane_of((1, slots)) < count
    target = lax.shift_right_logical(owner, P_OWN.bit_length() - 1)
    spot = lax.bitwise_and(owner, P_OWN - 1)
    member = jnp.where((rows_of((blocks, slots)) == target) & alive, 1.0, 0.0)
    earlier = jnp.where(rows_of((slots, slots)) < lane_of((slots, slots)), 1.0, 0.0)
    before = joined(member, earlier, 1, 0)
    order = jnp.sum(before * member, axis=0, keepdims=True).astype(jnp.int32)
    label = jnp.where(alive, target * room + order, -1)
    select = jnp.where(rows_of((blocks * room, slots)) == label, 1.0, 0.0)
    select_ref[...] = select.astype(jnp.bfloat16)
    moved = joined(select, history_ref[...], 1, 0)
    spots = joined(select, jnp.where(rows_of((P_OWN, slots)) == spot, 1.0, 0.0), 1, 1)
    for block in range(blocks):
        rows = slice(block * room, (block + 1) * room)
        send_ref[block, :, 0:width] = moved[rows].astype(jnp.bfloat16)
        send_ref[block, :, width : width + P_OWN] = spots[rows].astype(jnp.bfloat16)


def unpacked(got_ref, flat_ref):
    blocks, room = got_ref.shape[0], got_ref.shape[1]
    for block in range(blocks):
        flat_ref[block * room : (block + 1) * room, :] = got_ref[block].astype(jnp.float32)


def settle_history(got_ref, flat_ref, choose_ref, table_ref, partial_ref):
    unpacked(got_ref, flat_ref)
    choose = flat_ref[:, 2 * SAMPLES : 2 * SAMPLES + P_OWN].astype(jnp.bfloat16)
    choose_ref[...] = choose
    owned = joined(choose, flat_ref[:, 0 : 2 * SAMPLES], 0, 0)
    for field in range(2):
        partial_ref[:, field * 2 * BINS : (field + 1) * 2 * BINS] = joined(
            owned[:, field * SAMPLES : (field + 1) * SAMPLES], table_ref[...], 1, 0
        )


def reading_of(density_ref, cell_ref, probe_ref):
    depth = density_ref.shape[0]
    count = density_ref.shape[1]
    excess = density_ref[...] - 1.0
    parts = []
    for _ in range(3):
        part = excess.astype(jnp.bfloat16).astype(jnp.float32)
        parts.append(part)
        excess = excess - part
    found = joined(jnp.concatenate(parts, axis=0), cell_ref[...], 1, 0)
    layers = found[0:depth] + found[depth : 2 * depth] + found[2 * depth : 3 * depth]
    layer = lax.div(probe_ref[...], count)
    mine = rows_of(layers.shape) == layer
    return jnp.sum(jnp.where(mine, layers, 0.0), axis=0, keepdims=True)


def prepare_waves(spot_got, listen_ref, wave_ref):
    ring = spot_got.shape[0]
    tiles, width = wave_ref.shape[0], wave_ref.shape[3]
    angle_step = 2.0 * math.pi / SAMPLES / sound_speed
    for owner in range(ring):
        columns = spot_got[owner].T[0:P_OWN]
        for group in range(P_OWN // 8):
            rows = slice(group * 8, (group + 1) * 8)
            into = slice(owner * P_OWN + group * 8, owner * P_OWN + (group + 1) * 8)
            for tile in range(tiles):
                lanes = slice(tile * width, (tile + 1) * width)
                distance_sq = None
                facing = None
                for axis in range(3):
                    offset = listen_ref[axis : axis + 1, lanes] - columns[rows, axis : axis + 1]
                    square = offset * offset
                    along = columns[rows, axis + 3 : axis + 4] * offset
                    distance_sq = square if distance_sq is None else distance_sq + square
                    facing = along if facing is None else facing + along
                distance = jnp.sqrt(distance_sq)
                far = facing / (4.0 * math.pi * sound_speed * distance_sq)
                angle = angle_step * distance
                turn = jnp.cos(angle)
                wave_ref[tile, 0, into] = far
                wave_ref[tile, 1, into] = jnp.zeros_like(far)
                wave_ref[tile, 2, into] = far * turn
                wave_ref[tile, 3, into] = far * jnp.sin(angle)
                wave_ref[tile, 4, into] = 2.0 * turn
                wave_ref[tile, 5, into] = sound_speed / distance


def weigh_panels(done_got, weight_ref):
    ring = done_got.shape[0]
    panels = ring * P_OWN
    values = jnp.concatenate([done_got[owner].astype(jnp.float32) for owner in range(ring)], axis=0).T
    press_real, press_imag, rate_real, rate_imag = [
        values[part * BINS : (part + 1) * BINS] for part in range(4)
    ]
    lines = [
        [rate_real, rate_imag, press_real, press_imag],
        [rate_imag, -rate_real, press_imag, -press_real],
    ]
    for row, line in enumerate(lines):
        for part, value in enumerate(line):
            for start in range(0, panels, LANES):
                at = (part * panels + start) // LANES
                weight_ref[at, pl.ds(row, BINS, stride=8), :] = value[:, start : start + LANES]


def radiate_tile(wave_ref, weight_ref, first_ref, second_ref, sums_ref, total_ref):
    panels = wave_ref.shape[1]
    span = first_ref.shape[0]
    for first in range(0, BINS, span):
        held_ref = second_ref if first // span % 2 else first_ref
        for start in range(0, panels, 32):
            rows = slice(start, start + 32)
            old_cos, old_sin, now_cos, now_sin, twice, ratio = [wave_ref[i, rows] for i in range(6)]
            for number in range(span):
                near = [now_cos, now_sin, ratio * now_cos, ratio * now_sin]
                for part, value in enumerate(near):
                    into = slice(part * panels + start, part * panels + start + 32)
                    held_ref[number, into] = value.astype(jnp.bfloat16)
                if first + number + 1 < BINS:
                    old_cos, now_cos = now_cos, twice * now_cos - old_cos
                    old_sin, now_sin = now_sin, twice * now_sin - old_sin
            if first + span < BINS:
                for i, value in enumerate([old_cos, old_sin, now_cos, now_sin]):
                    wave_ref[i, rows] = value
        for number in range(span):
            rows = slice((first + number) * 8, (first + number + 1) * 8)
            weights = jnp.concatenate(
                [weight_ref[at, rows, :] for at in range(weight_ref.shape[0])], axis=1
            )
            found = joined(weights, held_ref[number], 1, 0)
            for part in range(sums_ref.shape[0]):
                sums_ref[part, rows, :] = found[:, part * LANES : (part + 1) * LANES]
    for part in range(sums_ref.shape[0]):
        total_ref[part, 0:BINS] = sums_ref[part, pl.ds(0, BINS, stride=8), :]
        total_ref[part, BINS : 2 * BINS] = sums_ref[part, pl.ds(1, BINS, stride=8), :]


def window_kernel(
    blocks, ring, face_ref, rim_face_ref, count_ref, start_hbm, owner_ref, probe_ref, history_ref,
    place_ref, normal_ref, listen_ref, table_ref, tail_ref, final_hbm, out_ref,
    field_ref, density_ref, rolled_ref, moving_ref, rim_ref, edge_ref, near_ref, draft_ref, piece_ref,
    send_ref, got_even, got_odd, select_ref, cell_ref, past_send, past_got, flat_ref, choose_ref,
    partial_ref, fresh_ref, fresh_send, fresh_got, fresh_flat, done_ref, done_got, spot_ref, spot_got,
    wave_ref, weight_ref, first_ref, second_ref, sums_ref, total_ref, part_send, part_got,
    edge_send, edge_got, send_sem, got_sem, past_send_sem, past_got_sem, fresh_send_sem, fresh_got_sem,
    done_send_sem, done_got_sem, spot_send_sem, spot_got_sem,
    part_send_sem, part_got_sem, local_sem,
):
    mesh_ids = pl.DeviceIdType.MESH
    me = lax.axis_index("blk")
    side = lax.axis_index("obs")
    right = lax.rem(side + 1, ring)
    left = lax.rem(side + ring - 1, ring)
    barrier = pltpu.get_barrier_semaphore()
    slots = owner_ref.shape[1]

    def greet(distance, carry):
        peer = lax.rem(me + distance, blocks)
        pl.semaphore_signal(barrier, inc=1, device_id=(peer, side), device_id_type=mesh_ids)
        return carry

    for distance in range(1, ring):
        beside = lax.rem(side + distance, ring)
        pl.semaphore_signal(barrier, inc=1, device_id=(me, beside), device_id_type=mesh_ids)
    lax.fori_loop(1, blocks, greet, 0)
    face = [face_ref[0, k] for k in range(4)]
    edge = [rim_face_ref[0, k] for k in range(4)]
    load = pltpu.make_async_copy(start_hbm, field_ref, local_sem.at[0])
    load.start()
    route(blocks, owner_ref, count_ref[0], history_ref, select_ref, past_send)
    cell = lax.rem(probe_ref[...], field_ref.shape[2])
    cell_ref[...] = jnp.where(rows_of(cell_ref.shape) == cell, 1.0, 0.0).astype(jnp.bfloat16)
    spot_ref[...] = jnp.zeros_like(spot_ref)
    spot_ref[0:3, 0:P_OWN] = place_ref[...].astype(jnp.float32)
    spot_ref[3:6, 0:P_OWN] = normal_ref[...].astype(jnp.float32)
    fresh_ref[...] = jnp.zeros_like(fresh_ref)
    load.wait()
    for tile in range(field_ref.shape[2] // LANES):
        for number in range(19):
            lanes = slice(tile * LANES, (tile + 1) * LANES)
            keep_rim(rim_ref, number, tile, field_ref[number, :, lanes])

    def swap(source_of, into_ref, send_sems, got_sems, distance):
        peer = lax.rem(me + distance, blocks)
        return pltpu.make_async_remote_copy(
            src_ref=source_of(distance, peer),
            dst_ref=into_ref.at[me],
            send_sem=send_sems.at[distance],
            recv_sem=got_sems.at[distance],
            device_id=(peer, side),
            device_id_type=mesh_ids,
        )

    def every(action):
        def visit(distance, inner):
            action(distance)
            return inner

        lax.fori_loop(1, blocks, visit, 0)

    def past_copy(distance):
        return swap(lambda _, peer: past_send.at[peer], past_got, past_send_sem, past_got_sem, distance)

    def fresh_copy(distance):
        return swap(lambda _, peer: fresh_send.at[peer], fresh_got, fresh_send_sem, fresh_got_sem, distance)

    def ring_copies(source_ref, into_ref, send_sems, got_sems):
        return [
            pltpu.make_async_remote_copy(
                src_ref=source_ref,
                dst_ref=into_ref.at[side],
                send_sem=send_sems.at[distance],
                recv_sem=got_sems.at[distance],
                device_id=(me, lax.rem(side + distance, ring)),
                device_id_type=mesh_ids,
            )
            for distance in range(1, ring)
        ]

    def note(step):
        gained = pressure_gain * reading_of(density_ref.at[step], cell_ref, probe_ref)
        if step == 0:
            last = jnp.where(lane_of((8, 2 * SAMPLES)) == SAMPLES - 1, 1.0, 0.0)
            before = joined(last, history_ref[...], 1, 1)[0:1]
        else:
            before = fresh_ref[step - 1 : step, :]
        fresh_ref[step : step + 1, :] = gained
        fresh_ref[STEPS + step : STEPS + step + 1, :] = gained - before

    def one_step(step):
        got_ref = got_odd if step % 2 else got_even
        collide_rim(rim_ref, edge_ref)
        if step == 0:
            collide_all(field_ref, rolled_ref, moving_ref, draft_ref)
        if step == 0:
            pl.semaphore_wait(barrier, blocks + ring - 2)
        edges = [
            pltpu.make_async_remote_copy(
                src_ref=edge_ref.at[way],
                dst_ref=near_ref.at[step, way],
                send_sem=edge_send.at[step, way],
                recv_sem=edge_got.at[step, way],
                device_id=(me, beside),
                device_id_type=mesh_ids,
            )
            for way, beside in enumerate([right, left])
        ]
        for copy in edges:
            copy.start()
        if step > 0:
            collide_all(field_ref, rolled_ref, moving_ref, draft_ref)
        for copy in edges:
            copy.wait()
        pack_moving(moving_ref, near_ref.at[step], draft_ref, piece_ref)

        def copy_to(distance):
            return swap(
                lambda number, _: send_ref.at[number], got_ref, send_sem.at[step], got_sem.at[step], distance
            )

        def begin(distance):
            peer = lax.rem(me + distance, blocks)
            up = (peer == face[1]) | (peer == edge[2]) | (peer == edge[3])
            piece = jnp.where(peer == face[3], 3, jnp.where(peer == face[2], 2, up.astype(jnp.int32)))
            send_ref[distance] = piece_ref[piece]
            copy_to(distance).start()

        every(begin)
        roll_moving(rolled_ref, moving_ref, near_ref.at[step])
        if step == 0:
            every(lambda distance: past_copy(distance).start())
            for copy in ring_copies(spot_ref, spot_got, spot_send_sem, spot_got_sem):
                copy.start()
            past_got[me] = past_send[me]
            spot_got[side] = spot_ref[...]
        else:
            note(step - 1)
        if step == 1:
            for copy in ring_copies(spot_ref, spot_got, spot_send_sem, spot_got_sem):
                copy.wait()
            prepare_waves(spot_got, listen_ref, wave_ref)
        if step == 2:
            every(lambda distance: past_copy(distance).wait())
            settle_history(past_got, flat_ref, choose_ref, table_ref, partial_ref)
        every(lambda distance: copy_to(distance).wait())
        finish_step(
            face, edge, got_ref, rolled_ref, field_ref, rim_ref, density_ref.at[step], step == STEPS - 1
        )

    for step in range(STEPS):
        one_step(step)
    unload = pltpu.make_async_copy(field_ref, final_hbm, local_sem.at[1])
    unload.start()
    note(STEPS - 1)
    fresh = joined(select_ref[...], fresh_ref[...], 1, 1)
    room = fresh_send.shape[1]
    for block in range(blocks):
        fresh_send[block] = fresh[block * room : (block + 1) * room].astype(jnp.bfloat16)
    every(lambda distance: fresh_copy(distance).start())
    fresh_got[me] = fresh_send[me]
    every(lambda distance: fresh_copy(distance).wait())
    unpacked(fresh_got, fresh_flat)
    newest = joined(choose_ref[...], fresh_flat[...], 0, 0)
    total = partial_ref[...] + joined(newest, tail_ref[...], 1, 0)
    done_ref[...] = total.astype(jnp.bfloat16)
    copies = ring_copies(done_ref, done_got, done_send_sem, done_got_sem)
    for copy in copies:
        copy.start()
    done_got[side] = done_ref[...]
    for copy in copies:
        copy.wait()
    weigh_panels(done_got, weight_ref)
    chunk = out_ref.shape[0]
    tiles = wave_ref.shape[0]
    share = wave_ref.shape[3] // chunk

    def part_copy(peer):
        distance = lax.rem(peer - me + blocks, blocks)
        return pltpu.make_async_remote_copy(
            src_ref=part_send.at[peer],
            dst_ref=part_got.at[me],
            send_sem=part_send_sem.at[distance],
            recv_sem=part_got_sem.at[distance],
            device_id=(peer, side),
            device_id_type=mesh_ids,
        )

    def one_tile(turn, carry):
        tile = lax.rem(me // share + 1 + turn, tiles)
        radiate_tile(wave_ref.at[tile], weight_ref, first_ref, second_ref, sums_ref, total_ref)
        each = LANES // chunk
        for part in range(total_ref.shape[0]):
            both = total_ref[part].T
            for number in range(each):
                rows = slice(number * chunk, (number + 1) * chunk)
                part_send[tile * share + part * each + number] = both[rows]

        def launch(number, inner):
            peer = tile * share + number

            @pl.when(peer != me)
            def _():
                part_copy(peer).start()

            return inner

        lax.fori_loop(0, share, launch, 0)
        return carry

    lax.fori_loop(0, tiles, one_tile, 0)
    part_got[me] = part_send[me]
    every(lambda distance: part_copy(lax.rem(me + distance, blocks)).wait())
    out_ref[...] = jnp.sum(part_got[...], axis=0)
    unload.wait()


def transform_tables():
    moments = np.arange(SAMPLES)[:, None]
    harmonics = np.arange(BINS)[None, :] + 1
    turns = moments * harmonics % SAMPLES
    phases = turns.astype(np.float32) * np.float32(2.0 * math.pi / SAMPLES)
    table = np.concatenate([np.cos(phases), -np.sin(phases)], axis=1).astype(jnp.bfloat16)
    past = np.zeros_like(table)
    past[STEPS:] = table[: SAMPLES - STEPS]
    tail = np.zeros((LANES, 4 * BINS), table.dtype)
    for field in range(2):
        rows = slice(field * STEPS, (field + 1) * STEPS)
        tail[rows, field * 2 * BINS : (field + 1) * 2 * BINS] = table[SAMPLES - STEPS :]
    return jnp.asarray(past), jnp.asarray(tail)


def body(
    populations,
    block_faces,
    block_edges,
    probe_cell,
    history,
    panel_count,
    panel_owner,
    panel_pos,
    panel_normal,
    observers,
):
    blocks = lax.axis_size("blk")
    lattice_state = populations[0]
    slab_depth = lattice_state.shape[1]
    lane_count = lattice_state.shape[2]
    ring = lax.axis_size("obs")
    tiles = lane_count // LANES
    vmem = pl.BlockSpec(memory_space=pltpu.VMEM)
    smem = pl.BlockSpec(memory_space=pltpu.SMEM)
    anywhere = pl.BlockSpec(memory_space=pl.ANY)
    wide = jnp.float32
    half = jnp.bfloat16
    slots = panel_owner.shape[0]
    room = -(-slots // blocks)
    past, tail = transform_tables()
    dma = pltpu.SemaphoreType.DMA
    listeners = observers.shape[1]
    chunk = listeners // blocks
    width = min(2 * LANES, listeners)
    lattice_state, spectrum = pl.pallas_call(
        functools.partial(window_kernel, blocks, ring),
        out_shape=[
            jax.ShapeDtypeStruct((19, slab_depth, lane_count), wide),
            jax.ShapeDtypeStruct((chunk, 2 * BINS), wide),
        ],
        in_specs=[smem] * 3 + [anywhere] + [vmem] * 8,
        out_specs=[anywhere, vmem],
        scratch_shapes=[
            pltpu.VMEM((19, slab_depth, lane_count), wide),
            pltpu.VMEM((STEPS, slab_depth, lane_count), wide),
            pltpu.VMEM((tiles + 2, 19, slab_depth, LANES), wide),
            pltpu.VMEM((tiles, len(x_order), slab_depth, LANES), wide),
            pltpu.VMEM((19, 2 * tiles, LANES), wide),
            pltpu.VMEM((2, 5, tiles, LANES), wide),
            pltpu.VMEM((STEPS, 2, 5, tiles, LANES), wide),
            pltpu.VMEM((4, slab_depth, FACE), wide),
            pltpu.VMEM((4, slab_depth, FACE), half),
            pltpu.VMEM((blocks, slab_depth, FACE), half),
            pltpu.VMEM((blocks, slab_depth, FACE), half),
            pltpu.VMEM((blocks, slab_depth, FACE), half),
            pltpu.VMEM((blocks * room, slots), half),
            pltpu.VMEM((lane_count, slots), half),
            pltpu.VMEM((blocks, room, 5 * LANES), half),
            pltpu.VMEM((blocks, room, 5 * LANES), half),
            pltpu.VMEM((blocks * room, 5 * LANES), wide),
            pltpu.VMEM((blocks * room, P_OWN), half),
            pltpu.VMEM((P_OWN, 4 * BINS), wide),
            pltpu.VMEM((LANES, slots), wide),
            pltpu.VMEM((blocks, room, LANES), half),
            pltpu.VMEM((blocks, room, LANES), half),
            pltpu.VMEM((blocks * room, LANES), wide),
            pltpu.VMEM((P_OWN, 4 * BINS), half),
            pltpu.VMEM((ring, P_OWN, 4 * BINS), half),
            pltpu.VMEM((8, LANES), wide),
            pltpu.VMEM((ring, 8, LANES), wide),
            pltpu.VMEM((listeners // width, 6, ring * P_OWN, width), wide),
            pltpu.VMEM((4 * ring * P_OWN // LANES, BINS * 8, LANES), wide),
            pltpu.VMEM((8, 4 * ring * P_OWN, width), half),
            pltpu.VMEM((8, 4 * ring * P_OWN, width), half),
            pltpu.VMEM((width // LANES, BINS * 8, LANES), wide),
            pltpu.VMEM((width // LANES, 2 * BINS, LANES), wide),
            pltpu.VMEM((blocks, chunk, 2 * BINS), wide),
            pltpu.VMEM((blocks, chunk, 2 * BINS), wide),
        ]
        + [dma((STEPS, 2))] * 2
        + [dma((STEPS, blocks))] * 2
        + [dma((blocks,))] * 4
        + [dma((ring,))] * 4
        + [dma((blocks,))] * 2
        + [dma((2,))],
        compiler_params=pltpu.CompilerParams(collective_id=0, has_side_effects=True),
    )(
        block_faces, block_edges, panel_count, lattice_state, panel_owner[None], probe_cell[None],
        history, panel_pos, panel_normal, observers, past, tail,
    )
    populations_out = lattice_state.reshape(1, 19, slab_depth, lane_count)
    return (populations_out, spectrum[None])


def solution(mesh):
    placed = (
        P("blk", None, "obs", None),
        P("blk", None),
        P("blk", None),
        P(("blk", "obs")),
        P(("blk", "obs"), None),
        P(("blk", "obs")),
        P(("blk", "obs")),
        P(None, ("blk", "obs")),
        P(None, ("blk", "obs")),
        P(None, "obs"),
    )
    return jax.shard_map(
        body,
        mesh=mesh,
        in_specs=placed,
        out_specs=(P("blk", None, "obs", None), P("obs", "blk", None)),
        check_vma=False,
    )
```

```python
import functools
import math

import jax
import jax.numpy as jnp
import numpy as np
from jax import lax
from jax.experimental import pallas as pl
from jax.experimental.pallas import tpu as pltpu
from jax.sharding import PartitionSpec as P

BS = 32
STEPS = 4
SAMPLES = 256
BINS = 64
P_OWN = 64


velocity_list = [
    (0, 0, 0),
    (1, 0, 0),
    (-1, 0, 0),
    (0, 1, 0),
    (0, -1, 0),
    (0, 0, 1),
    (0, 0, -1),
    (1, 1, 0),
    (-1, -1, 0),
    (1, -1, 0),
    (-1, 1, 0),
    (1, 0, 1),
    (-1, 0, -1),
    (1, 0, -1),
    (-1, 0, 1),
    (0, 1, 1),
    (0, -1, -1),
    (0, 1, -1),
    (0, -1, 1),
]
weight_list = [1.0 / 3.0] + [1.0 / 18.0] * 6 + [1.0 / 36.0] * 12
x_moving = [1, 2, 7, 8, 9, 10, 11, 12, 13, 14]
y_upward = [3, 7, 10, 15, 17]
y_downward = [4, 8, 9, 16, 18]
z_upward = [5, 11, 14, 15, 18]
z_downward = [6, 12, 13, 16, 17]
relax_rate = 1.6
pressure_gain = 60.0
sound_speed = 0.5


x_plus = [1, 7, 9, 11, 13]
x_minus = [2, 8, 10, 12, 14]
x_order = x_plus + x_minus
still = [0, 3, 4, 5, 6, 15, 16, 17, 18]
LANES = 128
FACE = 256


def collide_tile(f):
    sums = [None] * 19
    gaps = [None] * 19
    for number in range(1, 19, 2):
        sums[number] = f[number] + f[number + 1]
        gaps[number] = f[number] - f[number + 1]
    density = f[0]
    for number in range(1, 19, 2):
        density = density + sums[number]
    speeds = []
    for axis in range(3):
        total = None
        for number in range(1, 19, 2):
            sign = velocity_list[number][axis]
            if sign == 0:
                continue
            if total is None:
                total = gaps[number]
            elif sign == 1:
                total = total + gaps[number]
            else:
                total = total - gaps[number]
        speeds.append(total)
    inverse = 1.0 / density
    speeds = [speed * inverse for speed in speeds]
    squared = speeds[0] * speeds[0] + speeds[1] * speeds[1] + speeds[2] * speeds[2]
    base = 1.0 - 1.5 * squared
    keep = 1.0 - relax_rate
    out = [None] * 19
    out[0] = keep * f[0] + ((relax_rate * weight_list[0]) * density) * base
    scaled = {}
    thrice = {}
    for weight in sorted(set(weight_list[1:])):
        scaled[weight] = (relax_rate * weight) * density
        thrice[weight] = 3.0 * scaled[weight]
    for number in range(1, 19, 2):
        projected = None
        for axis in range(3):
            sign = velocity_list[number][axis]
            if sign == 0:
                continue
            if projected is None:
                projected = speeds[axis]
            elif sign == 1:
                projected = projected + speeds[axis]
            else:
                projected = projected - speeds[axis]
        weight = weight_list[number]
        even = scaled[weight] * (base + 4.5 * (projected * projected))
        odd = thrice[weight] * projected
        out[number] = keep * f[number] + (even + odd)
        out[number + 1] = keep * f[number + 1] + (even - odd)
    return out


def lane_of(shape):
    return lax.broadcasted_iota(jnp.int32, shape, 1)


def turned(value, amount):
    amount = amount % value.shape[1]
    return value if amount == 0 else pltpu.roll(value, amount, 1)


def pushed(value, low, high, sign):
    if sign == 1:
        return jnp.concatenate([low, value[:-1]], axis=0)
    return jnp.concatenate([value[1:], high], axis=0)


def shift_of(number):
    return velocity_list[number][1] * BS + velocity_list[number][2]


face_sets = [y_downward, y_upward, z_downward, z_upward]


def pack_tile(values, tile, tiles, chosen_numbers, columns, rows):
    depth = values[chosen_numbers[0]].shape[0]
    spot = lane_of((depth, LANES)) % BS
    quarter = lane_of((depth, LANES)) // BS
    u = tile % 4
    for side, (chosen, begin) in enumerate([(z_downward, 0), (z_upward, BS - 1)]):
        for j, number in enumerate(chosen):
            if number in chosen_numbers:
                moved = turned(values[number] - weight_list[number], 8 * u + j - begin)
                columns[side] = jnp.where(spot == 8 * u + j, moved, columns[side])
    for side, (chosen, at, begin) in enumerate(
        [(y_downward, 0, 0), (y_upward, tiles - 1, LANES - BS)]
    ):
        if tile != at:
            continue
        for j, number in enumerate(chosen):
            if number in chosen_numbers:
                moved = turned(values[number] - weight_list[number], j % 4 * BS - begin)
                rows[side][j // 4] = jnp.where(quarter == j % 4, moved, rows[side][j // 4])


def collide_all(field_ref, rolled_ref, moving_ref, draft_ref):
    depth = field_ref.shape[1]
    tiles = field_ref.shape[2] // LANES
    blank = jnp.zeros((depth, LANES), jnp.float32)
    rows = [[blank, blank], [blank, blank]]
    for half in range(tiles // 4):
        columns = [blank, blank]
        for u in range(4):
            tile = half * 4 + u
            lanes = slice(tile * LANES, (tile + 1) * LANES)
            out = collide_tile([field_ref[number, :, lanes] for number in range(19)])
            for number in range(19):
                if number in still:
                    rolled_ref[tile + 1, number] = turned(out[number], shift_of(number))
                else:
                    moving_ref[tile, x_order.index(number)] = out[number]
            pack_tile(out, tile, tiles, still, columns, rows)
        for side in range(2):
            draft_ref[2 + side, :, half * LANES : (half + 1) * LANES] = columns[side]
    for side in range(2):
        for half in range(2):
            draft_ref[side, :, half * LANES : (half + 1) * LANES] = rows[side][half]


def keep_rim(rim_ref, number, tile, value):
    depth = value.shape[0]
    tiles = rim_ref.shape[1] // 2
    rim_ref[number, tile : tile + 1, :] = value[depth - 1 : depth]
    rim_ref[number, tiles + tile : tiles + tile + 1, :] = value[0:1]


def collide_rim(rim_ref, edge_ref):
    tiles = rim_ref.shape[1] // 2
    out = collide_tile([rim_ref[number] for number in range(19)])
    for place, number in enumerate(x_plus):
        edge_ref[0, place] = out[number][0:tiles]
    for place, number in enumerate(x_minus):
        edge_ref[1, place] = out[number][tiles : 2 * tiles]


def shifted(moving_ref, near_ref, tile, number):
    place = x_order.index(number)
    low = near_ref[0, place % 5, tile : tile + 1, :]
    high = near_ref[1, place % 5, tile : tile + 1, :]
    return pushed(moving_ref[tile, place], low, high, velocity_list[number][0])


def pack_moving(moving_ref, near_ref, draft_ref, piece_ref):
    tiles = moving_ref.shape[0]
    crossing = x_order[1:5] + x_order[6:]

    def draft(piece, half):
        return draft_ref[piece, :, half * LANES : (half + 1) * LANES]

    rows = [[draft(side, half) for half in range(2)] for side in range(2)]
    for half in range(tiles // 4):
        columns = [draft(2 + side, half) for side in range(2)]
        for u in range(4):
            tile = half * 4 + u
            values = {}
            for number in crossing:
                if velocity_list[number][1] == 0 or tile in (0, tiles - 1):
                    values[number] = shifted(moving_ref, near_ref, tile, number)
            pack_tile(values, tile, tiles, list(values), columns, rows)
        for side in range(2):
            piece_ref[2 + side, :, half * LANES : (half + 1) * LANES] = columns[side].astype(jnp.bfloat16)
    for side in range(2):
        for half in range(2):
            piece_ref[side, :, half * LANES : (half + 1) * LANES] = rows[side][half].astype(jnp.bfloat16)


def roll_moving(rolled_ref, moving_ref, near_ref):
    tiles = moving_ref.shape[0]
    for tile in range(tiles):
        for number in x_order:
            value = shifted(moving_ref, near_ref, tile, number)
            rolled_ref[tile + 1, number] = turned(value, shift_of(number))


def finish_step(face, edge, got_ref, rolled_ref, field_ref, rim_ref, density_ref, last):
    depth = field_ref.shape[1]
    tiles = field_ref.shape[2] // LANES
    lane = lane_of((depth, LANES))
    spot = lane % BS

    def arrived(source, half):
        return got_ref[source, :, half * LANES : (half + 1) * LANES].astype(jnp.float32)

    corners = {15: (0, 0, 1), 17: (1, 1, 31), 18: (2, 1, 65), 16: (3, 0, 31)}
    corner_lane = {15: 0, 17: BS - 1, 18: LANES - BS, 16: LANES - 1}
    for piece, source, pad, begin in [(1, face[0], 0, 0), (0, face[1], tiles + 1, LANES - BS)]:
        halves = [arrived(source, half) for half in range(2)]
        for j, number in enumerate(face_sets[piece]):
            shift_z = velocity_list[number][2]
            value = turned(halves[j // 4], begin + shift_z - j % 4 * BS)
            if number in corners:
                which, half, amount = corners[number]
                corner = turned(arrived(edge[which], half), amount)
                value = jnp.where(lane == corner_lane[number], corner, value)
            rolled_ref[pad, number] = value + weight_list[number]
    columns = {}
    for piece, source, rim in [(3, face[2], 0), (2, face[3], BS - 1)]:
        chosen = face_sets[piece]
        halves = [arrived(source, half) for half in range(2)]
        for tile in range(tiles):
            for j, number in enumerate(chosen):
                shift_y = velocity_list[number][1]
                amount = rim - 8 * (tile % 4) - j + BS * shift_y
                column = turned(halves[tile // 4], amount) + weight_list[number]
                value = jnp.where(spot == rim, column, rolled_ref[tile + 1, number])
                if shift_y != 0:
                    rolled_ref[tile + 1, number] = value
                else:
                    columns[tile, number] = value
                    field_ref[number, :, tile * LANES : (tile + 1) * LANES] = value
    for tile in range(tiles):
        lanes = slice(tile * LANES, (tile + 1) * LANES)
        total = None
        for number, (_, shift_y, shift_z) in enumerate(velocity_list):
            if shift_y == 0 and shift_z != 0:
                value = field_ref[number, :, lanes]
            else:
                value = rolled_ref[tile + 1, number]
                if shift_y == 1:
                    value = jnp.where(lane < BS, rolled_ref[tile, number], value)
                elif shift_y == -1:
                    value = jnp.where(lane >= LANES - BS, rolled_ref[tile + 2, number], value)
                field_ref[number, :, lanes] = value
            if not last:
                keep_rim(rim_ref, number, tile, value)
            total = value if total is None else total + value
        density_ref[:, lanes] = total


def joined(left, right, left_axis, right_axis):
    return lax.dot_general(
        left.astype(jnp.bfloat16), right.astype(jnp.bfloat16),
        (((left_axis,), (right_axis,)), ((), ())), preferred_element_type=jnp.float32,
    )


def rows_of(shape):
    return lax.broadcasted_iota(jnp.int32, shape, 0)


def route(blocks, owner_ref, count, history_ref, select_ref, send_ref):
    slots = owner_ref.shape[1]
    room = send_ref.shape[1]
    width = history_ref.shape[1]
    owner = owner_ref[...]
    alive = lane_of((1, slots)) < count
    target = lax.shift_right_logical(owner, P_OWN.bit_length() - 1)
    spot = lax.bitwise_and(owner, P_OWN - 1)
    member = jnp.where((rows_of((blocks, slots)) == target) & alive, 1.0, 0.0)
    earlier = jnp.where(rows_of((slots, slots)) < lane_of((slots, slots)), 1.0, 0.0)
    before = joined(member, earlier, 1, 0)
    order = jnp.sum(before * member, axis=0, keepdims=True).astype(jnp.int32)
    label = jnp.where(alive, target * room + order, -1)
    select = jnp.where(rows_of((blocks * room, slots)) == label, 1.0, 0.0)
    select_ref[...] = select.astype(jnp.bfloat16)
    moved = joined(select, history_ref[...], 1, 0)
    spots = joined(select, jnp.where(rows_of((P_OWN, slots)) == spot, 1.0, 0.0), 1, 1)
    for block in range(blocks):
        rows = slice(block * room, (block + 1) * room)
        send_ref[block, :, 0:width] = moved[rows].astype(jnp.bfloat16)
        send_ref[block, :, width : width + P_OWN] = spots[rows].astype(jnp.bfloat16)


def unpacked(got_ref, flat_ref):
    blocks, room = got_ref.shape[0], got_ref.shape[1]
    for block in range(blocks):
        flat_ref[block * room : (block + 1) * room, :] = got_ref[block].astype(jnp.float32)


def settle_history(got_ref, flat_ref, choose_ref, table_ref, partial_ref):
    unpacked(got_ref, flat_ref)
    choose = flat_ref[:, 2 * SAMPLES : 2 * SAMPLES + P_OWN].astype(jnp.bfloat16)
    choose_ref[...] = choose
    owned = joined(choose, flat_ref[:, 0 : 2 * SAMPLES], 0, 0)
    for field in range(2):
        partial_ref[:, field * 2 * BINS : (field + 1) * 2 * BINS] = joined(
            owned[:, field * SAMPLES : (field + 1) * SAMPLES], table_ref[...], 1, 0
        )


def reading_of(density_ref, cell_ref, probe_ref):
    depth = density_ref.shape[0]
    count = density_ref.shape[1]
    excess = density_ref[...] - 1.0
    parts = []
    for _ in range(3):
        part = excess.astype(jnp.bfloat16).astype(jnp.float32)
        parts.append(part)
        excess = excess - part
    found = joined(jnp.concatenate(parts, axis=0), cell_ref[...], 1, 0)
    layers = found[0:depth] + found[depth : 2 * depth] + found[2 * depth : 3 * depth]
    layer = lax.div(probe_ref[...], count)
    mine = rows_of(layers.shape) == layer
    return jnp.sum(jnp.where(mine, layers, 0.0), axis=0, keepdims=True)


def prepare_waves(spot_got, listen_ref, wave_ref):
    ring = spot_got.shape[0]
    tiles, width = wave_ref.shape[0], wave_ref.shape[3]
    angle_step = 2.0 * math.pi / SAMPLES / sound_speed
    for owner in range(ring):
        columns = spot_got[owner].T[0:P_OWN]
        for group in range(P_OWN // 8):
            rows = slice(group * 8, (group + 1) * 8)
            into = slice(owner * P_OWN + group * 8, owner * P_OWN + (group + 1) * 8)
            for tile in range(tiles):
                lanes = slice(tile * width, (tile + 1) * width)
                distance_sq = None
                facing = None
                for axis in range(3):
                    offset = listen_ref[axis : axis + 1, lanes] - columns[rows, axis : axis + 1]
                    square = offset * offset
                    along = columns[rows, axis + 3 : axis + 4] * offset
                    distance_sq = square if distance_sq is None else distance_sq + square
                    facing = along if facing is None else facing + along
                distance = jnp.sqrt(distance_sq)
                far = facing / (4.0 * math.pi * sound_speed * distance_sq)
                angle = angle_step * distance
                turn = jnp.cos(angle)
                wave_ref[tile, 0, into] = far
                wave_ref[tile, 1, into] = jnp.zeros_like(far)
                wave_ref[tile, 2, into] = far * turn
                wave_ref[tile, 3, into] = far * jnp.sin(angle)
                wave_ref[tile, 4, into] = 2.0 * turn
                wave_ref[tile, 5, into] = sound_speed / distance


def weigh_panels(done_got, weight_ref):
    ring = done_got.shape[0]
    panels = ring * P_OWN
    values = jnp.concatenate([done_got[owner].astype(jnp.float32) for owner in range(ring)], axis=0).T
    press_real, press_imag, rate_real, rate_imag = [
        values[part * BINS : (part + 1) * BINS] for part in range(4)
    ]
    lines = [
        [rate_real, rate_imag, press_real, press_imag],
        [rate_imag, -rate_real, press_imag, -press_real],
    ]
    for row, line in enumerate(lines):
        for part, value in enumerate(line):
            for start in range(0, panels, LANES):
                at = (part * panels + start) // LANES
                weight_ref[at, pl.ds(row, BINS, stride=8), :] = value[:, start : start + LANES]


def radiate_tile(wave_ref, weight_ref, first_ref, second_ref, sums_ref, total_ref):
    panels = wave_ref.shape[1]
    span = first_ref.shape[0]
    for first in range(0, BINS, span):
        held_ref = second_ref if first // span % 2 else first_ref
        for start in range(0, panels, 32):
            rows = slice(start, start + 32)
            old_cos, old_sin, now_cos, now_sin, twice, ratio = [wave_ref[i, rows] for i in range(6)]
            nearer = ratio.astype(jnp.bfloat16)
            for number in range(span):
                pair = [now_cos.astype(jnp.bfloat16), now_sin.astype(jnp.bfloat16)]
                for part, value in enumerate(pair + [nearer * value for value in pair]):
                    into = slice(part * panels + start, part * panels + start + 32)
                    held_ref[number, into] = value
                if first + number + 1 < BINS:
                    old_cos, now_cos = now_cos, twice * now_cos - old_cos
                    old_sin, now_sin = now_sin, twice * now_sin - old_sin
            if first + span < BINS:
                for i, value in enumerate([old_cos, old_sin, now_cos, now_sin]):
                    wave_ref[i, rows] = value
        for number in range(span):
            rows = slice((first + number) * 8, (first + number + 1) * 8)
            weights = jnp.concatenate(
                [weight_ref[at, rows, :] for at in range(weight_ref.shape[0])], axis=1
            )
            found = joined(weights, held_ref[number], 1, 0)
            for part in range(sums_ref.shape[0]):
                sums_ref[part, rows, :] = found[:, part * LANES : (part + 1) * LANES]
    for part in range(sums_ref.shape[0]):
        total_ref[part, 0:BINS] = sums_ref[part, pl.ds(0, BINS, stride=8), :]
        total_ref[part, BINS : 2 * BINS] = sums_ref[part, pl.ds(1, BINS, stride=8), :]


def window_kernel(
    blocks, ring, face_ref, rim_face_ref, count_ref, start_hbm, owner_ref, probe_ref, history_ref,
    place_ref, normal_ref, listen_ref, table_ref, tail_ref, final_hbm, out_ref,
    field_ref, density_ref, rolled_ref, moving_ref, rim_ref, edge_ref, near_ref, draft_ref, piece_ref,
    send_ref, got_even, got_odd, select_ref, cell_ref, past_send, past_got, flat_ref, choose_ref,
    partial_ref, fresh_ref, fresh_send, fresh_got, fresh_flat, done_ref, done_got, spot_ref, spot_got,
    wave_ref, weight_ref, first_ref, second_ref, sums_ref, total_ref, part_send, part_got,
    edge_send, edge_got, send_sem, got_sem, past_send_sem, past_got_sem, fresh_send_sem, fresh_got_sem,
    done_send_sem, done_got_sem, spot_send_sem, spot_got_sem,
    part_send_sem, part_got_sem, local_sem,
):
    mesh_ids = pl.DeviceIdType.MESH
    me = lax.axis_index("blk")
    side = lax.axis_index("obs")
    right = lax.rem(side + 1, ring)
    left = lax.rem(side + ring - 1, ring)
    barrier = pltpu.get_barrier_semaphore()
    slots = owner_ref.shape[1]

    def greet(distance, carry):
        peer = lax.rem(me + distance, blocks)
        pl.semaphore_signal(barrier, inc=1, device_id=(peer, side), device_id_type=mesh_ids)
        return carry

    for distance in range(1, ring):
        beside = lax.rem(side + distance, ring)
        pl.semaphore_signal(barrier, inc=1, device_id=(me, beside), device_id_type=mesh_ids)
    lax.fori_loop(1, blocks, greet, 0)
    face = [face_ref[0, k] for k in range(4)]
    edge = [rim_face_ref[0, k] for k in range(4)]
    load = pltpu.make_async_copy(start_hbm, field_ref, local_sem.at[0])
    load.start()
    route(blocks, owner_ref, count_ref[0], history_ref, select_ref, past_send)
    cell = lax.rem(probe_ref[...], field_ref.shape[2])
    cell_ref[...] = jnp.where(rows_of(cell_ref.shape) == cell, 1.0, 0.0).astype(jnp.bfloat16)
    spot_ref[...] = jnp.zeros_like(spot_ref)
    spot_ref[0:3, 0:P_OWN] = place_ref[...].astype(jnp.float32)
    spot_ref[3:6, 0:P_OWN] = normal_ref[...].astype(jnp.float32)
    fresh_ref[...] = jnp.zeros_like(fresh_ref)
    load.wait()
    for tile in range(field_ref.shape[2] // LANES):
        for number in range(19):
            lanes = slice(tile * LANES, (tile + 1) * LANES)
            keep_rim(rim_ref, number, tile, field_ref[number, :, lanes])

    def swap(source_of, into_ref, send_sems, got_sems, distance):
        peer = lax.rem(me + distance, blocks)
        return pltpu.make_async_remote_copy(
            src_ref=source_of(distance, peer),
            dst_ref=into_ref.at[me],
            send_sem=send_sems.at[distance],
            recv_sem=got_sems.at[distance],
            device_id=(peer, side),
            device_id_type=mesh_ids,
        )

    def every(action):
        def visit(distance, inner):
            action(distance)
            return inner

        lax.fori_loop(1, blocks, visit, 0)

    def past_copy(distance):
        return swap(lambda _, peer: past_send.at[peer], past_got, past_send_sem, past_got_sem, distance)

    def fresh_copy(distance):
        return swap(lambda _, peer: fresh_send.at[peer], fresh_got, fresh_send_sem, fresh_got_sem, distance)

    def ring_copies(source_ref, into_ref, send_sems, got_sems):
        return [
            pltpu.make_async_remote_copy(
                src_ref=source_ref,
                dst_ref=into_ref.at[side],
                send_sem=send_sems.at[distance],
                recv_sem=got_sems.at[distance],
                device_id=(me, lax.rem(side + distance, ring)),
                device_id_type=mesh_ids,
            )
            for distance in range(1, ring)
        ]

    def note(step):
        gained = pressure_gain * reading_of(density_ref.at[step], cell_ref, probe_ref)
        if step == 0:
            last = jnp.where(lane_of((8, 2 * SAMPLES)) == SAMPLES - 1, 1.0, 0.0)
            before = joined(last, history_ref[...], 1, 1)[0:1]
        else:
            before = fresh_ref[step - 1 : step, :]
        fresh_ref[step : step + 1, :] = gained
        fresh_ref[STEPS + step : STEPS + step + 1, :] = gained - before

    def one_step(step):
        got_ref = got_odd if step % 2 else got_even
        collide_rim(rim_ref, edge_ref)
        if step == 0:
            collide_all(field_ref, rolled_ref, moving_ref, draft_ref)
        if step == 0:
            pl.semaphore_wait(barrier, blocks + ring - 2)
        edges = [
            pltpu.make_async_remote_copy(
                src_ref=edge_ref.at[way],
                dst_ref=near_ref.at[step, way],
                send_sem=edge_send.at[step, way],
                recv_sem=edge_got.at[step, way],
                device_id=(me, beside),
                device_id_type=mesh_ids,
            )
            for way, beside in enumerate([right, left])
        ]
        for copy in edges:
            copy.start()
        if step > 0:
            collide_all(field_ref, rolled_ref, moving_ref, draft_ref)
        for copy in edges:
            copy.wait()
        pack_moving(moving_ref, near_ref.at[step], draft_ref, piece_ref)

        def copy_to(distance):
            return swap(
                lambda number, _: send_ref.at[number], got_ref, send_sem.at[step], got_sem.at[step], distance
            )

        def begin(distance):
            peer = lax.rem(me + distance, blocks)
            up = (peer == face[1]) | (peer == edge[2]) | (peer == edge[3])
            piece = jnp.where(peer == face[3], 3, jnp.where(peer == face[2], 2, up.astype(jnp.int32)))
            send_ref[distance] = piece_ref[piece]
            copy_to(distance).start()

        every(begin)
        roll_moving(rolled_ref, moving_ref, near_ref.at[step])
        if step == 0:
            every(lambda distance: past_copy(distance).start())
            for copy in ring_copies(spot_ref, spot_got, spot_send_sem, spot_got_sem):
                copy.start()
            past_got[me] = past_send[me]
            spot_got[side] = spot_ref[...]
        else:
            note(step - 1)
        if step == 1:
            for copy in ring_copies(spot_ref, spot_got, spot_send_sem, spot_got_sem):
                copy.wait()
            prepare_waves(spot_got, listen_ref, wave_ref)
        if step == 2:
            every(lambda distance: past_copy(distance).wait())
            settle_history(past_got, flat_ref, choose_ref, table_ref, partial_ref)
        every(lambda distance: copy_to(distance).wait())
        finish_step(
            face, edge, got_ref, rolled_ref, field_ref, rim_ref, density_ref.at[step], step == STEPS - 1
        )

    for step in range(STEPS):
        one_step(step)
    unload = pltpu.make_async_copy(field_ref, final_hbm, local_sem.at[1])
    unload.start()
    note(STEPS - 1)
    fresh = joined(select_ref[...], fresh_ref[...], 1, 1)
    room = fresh_send.shape[1]
    for block in range(blocks):
        fresh_send[block] = fresh[block * room : (block + 1) * room].astype(jnp.bfloat16)
    every(lambda distance: fresh_copy(distance).start())
    fresh_got[me] = fresh_send[me]
    every(lambda distance: fresh_copy(distance).wait())
    unpacked(fresh_got, fresh_flat)
    newest = joined(choose_ref[...], fresh_flat[...], 0, 0)
    total = partial_ref[...] + joined(newest, tail_ref[...], 1, 0)
    done_ref[...] = total.astype(jnp.bfloat16)
    copies = ring_copies(done_ref, done_got, done_send_sem, done_got_sem)
    for copy in copies:
        copy.start()
    done_got[side] = done_ref[...]
    for copy in copies:
        copy.wait()
    weigh_panels(done_got, weight_ref)
    chunk = out_ref.shape[0]
    tiles = wave_ref.shape[0]
    share = wave_ref.shape[3] // chunk

    def part_copy(peer):
        distance = lax.rem(peer - me + blocks, blocks)
        return pltpu.make_async_remote_copy(
            src_ref=part_send.at[peer],
            dst_ref=part_got.at[me],
            send_sem=part_send_sem.at[distance],
            recv_sem=part_got_sem.at[distance],
            device_id=(peer, side),
            device_id_type=mesh_ids,
        )

    def one_tile(turn, carry):
        tile = lax.rem(me // share + 1 + turn, tiles)
        radiate_tile(wave_ref.at[tile], weight_ref, first_ref, second_ref, sums_ref, total_ref)
        each = LANES // chunk
        for part in range(total_ref.shape[0]):
            both = total_ref[part].T
            for number in range(each):
                rows = slice(number * chunk, (number + 1) * chunk)
                part_send[tile * share + part * each + number] = both[rows]

        def launch(number, inner):
            peer = tile * share + number

            @pl.when(peer != me)
            def _():
                part_copy(peer).start()

            return inner

        lax.fori_loop(0, share, launch, 0)
        return carry

    lax.fori_loop(0, tiles, one_tile, 0)
    part_got[me] = part_send[me]
    every(lambda distance: part_copy(lax.rem(me + distance, blocks)).wait())
    out_ref[...] = jnp.sum(part_got[...], axis=0)
    unload.wait()


def transform_tables():
    moments = np.arange(SAMPLES)[:, None]
    harmonics = np.arange(BINS)[None, :] + 1
    turns = moments * harmonics % SAMPLES
    phases = turns.astype(np.float32) * np.float32(2.0 * math.pi / SAMPLES)
    table = np.concatenate([np.cos(phases), -np.sin(phases)], axis=1).astype(jnp.bfloat16)
    past = np.zeros_like(table)
    past[STEPS:] = table[: SAMPLES - STEPS]
    tail = np.zeros((LANES, 4 * BINS), table.dtype)
    for field in range(2):
        rows = slice(field * STEPS, (field + 1) * STEPS)
        tail[rows, field * 2 * BINS : (field + 1) * 2 * BINS] = table[SAMPLES - STEPS :]
    return jnp.asarray(past), jnp.asarray(tail)


def body(
    populations,
    block_faces,
    block_edges,
    probe_cell,
    history,
    panel_count,
    panel_owner,
    panel_pos,
    panel_normal,
    observers,
):
    blocks = lax.axis_size("blk")
    lattice_state = populations[0]
    slab_depth = lattice_state.shape[1]
    lane_count = lattice_state.shape[2]
    ring = lax.axis_size("obs")
    tiles = lane_count // LANES
    vmem = pl.BlockSpec(memory_space=pltpu.VMEM)
    smem = pl.BlockSpec(memory_space=pltpu.SMEM)
    anywhere = pl.BlockSpec(memory_space=pl.ANY)
    wide = jnp.float32
    half = jnp.bfloat16
    slots = panel_owner.shape[0]
    room = -(-slots // blocks)
    past, tail = transform_tables()
    dma = pltpu.SemaphoreType.DMA
    listeners = observers.shape[1]
    chunk = listeners // blocks
    width = min(2 * LANES, listeners)
    lattice_state, spectrum = pl.pallas_call(
        functools.partial(window_kernel, blocks, ring),
        out_shape=[
            jax.ShapeDtypeStruct((19, slab_depth, lane_count), wide),
            jax.ShapeDtypeStruct((chunk, 2 * BINS), wide),
        ],
        in_specs=[smem] * 3 + [anywhere] + [vmem] * 8,
        out_specs=[anywhere, vmem],
        scratch_shapes=[
            pltpu.VMEM((19, slab_depth, lane_count), wide),
            pltpu.VMEM((STEPS, slab_depth, lane_count), wide),
            pltpu.VMEM((tiles + 2, 19, slab_depth, LANES), wide),
            pltpu.VMEM((tiles, len(x_order), slab_depth, LANES), wide),
            pltpu.VMEM((19, 2 * tiles, LANES), wide),
            pltpu.VMEM((2, 5, tiles, LANES), wide),
            pltpu.VMEM((STEPS, 2, 5, tiles, LANES), wide),
            pltpu.VMEM((4, slab_depth, FACE), wide),
            pltpu.VMEM((4, slab_depth, FACE), half),
            pltpu.VMEM((blocks, slab_depth, FACE), half),
            pltpu.VMEM((blocks, slab_depth, FACE), half),
            pltpu.VMEM((blocks, slab_depth, FACE), half),
            pltpu.VMEM((blocks * room, slots), half),
            pltpu.VMEM((lane_count, slots), half),
            pltpu.VMEM((blocks, room, 5 * LANES), half),
            pltpu.VMEM((blocks, room, 5 * LANES), half),
            pltpu.VMEM((blocks * room, 5 * LANES), wide),
            pltpu.VMEM((blocks * room, P_OWN), half),
            pltpu.VMEM((P_OWN, 4 * BINS), wide),
            pltpu.VMEM((LANES, slots), wide),
            pltpu.VMEM((blocks, room, LANES), half),
            pltpu.VMEM((blocks, room, LANES), half),
            pltpu.VMEM((blocks * room, LANES), wide),
            pltpu.VMEM((P_OWN, 4 * BINS), half),
            pltpu.VMEM((ring, P_OWN, 4 * BINS), half),
            pltpu.VMEM((8, LANES), wide),
            pltpu.VMEM((ring, 8, LANES), wide),
            pltpu.VMEM((listeners // width, 6, ring * P_OWN, width), wide),
            pltpu.VMEM((4 * ring * P_OWN // LANES, BINS * 8, LANES), wide),
            pltpu.VMEM((8, 4 * ring * P_OWN, width), half),
            pltpu.VMEM((8, 4 * ring * P_OWN, width), half),
            pltpu.VMEM((width // LANES, BINS * 8, LANES), wide),
            pltpu.VMEM((width // LANES, 2 * BINS, LANES), wide),
            pltpu.VMEM((blocks, chunk, 2 * BINS), wide),
            pltpu.VMEM((blocks, chunk, 2 * BINS), wide),
        ]
        + [dma((STEPS, 2))] * 2
        + [dma((STEPS, blocks))] * 2
        + [dma((blocks,))] * 4
        + [dma((ring,))] * 4
        + [dma((blocks,))] * 2
        + [dma((2,))],
        compiler_params=pltpu.CompilerParams(collective_id=0, has_side_effects=True),
    )(
        block_faces, block_edges, panel_count, lattice_state, panel_owner[None], probe_cell[None],
        history, panel_pos, panel_normal, observers, past, tail,
    )
    populations_out = lattice_state.reshape(1, 19, slab_depth, lane_count)
    return (populations_out, spectrum[None])


def solution(mesh):
    placed = (
        P("blk", None, "obs", None),
        P("blk", None),
        P("blk", None),
        P(("blk", "obs")),
        P(("blk", "obs"), None),
        P(("blk", "obs")),
        P(("blk", "obs")),
        P(None, ("blk", "obs")),
        P(None, ("blk", "obs")),
        P(None, "obs"),
    )
    return jax.shard_map(
        body,
        mesh=mesh,
        in_specs=placed,
        out_specs=(P("blk", None, "obs", None), P("obs", "blk", None)),
        check_vma=False,
    )
```

```python
import functools
import math

import jax
import jax.numpy as jnp
import numpy as np
from jax import lax
from jax.experimental import pallas as pl
from jax.experimental.pallas import tpu as pltpu
from jax.sharding import PartitionSpec as P

BS = 32
STEPS = 4
SAMPLES = 256
BINS = 64
P_OWN = 64


velocity_list = [
    (0, 0, 0),
    (1, 0, 0),
    (-1, 0, 0),
    (0, 1, 0),
    (0, -1, 0),
    (0, 0, 1),
    (0, 0, -1),
    (1, 1, 0),
    (-1, -1, 0),
    (1, -1, 0),
    (-1, 1, 0),
    (1, 0, 1),
    (-1, 0, -1),
    (1, 0, -1),
    (-1, 0, 1),
    (0, 1, 1),
    (0, -1, -1),
    (0, 1, -1),
    (0, -1, 1),
]
weight_list = [1.0 / 3.0] + [1.0 / 18.0] * 6 + [1.0 / 36.0] * 12
x_moving = [1, 2, 7, 8, 9, 10, 11, 12, 13, 14]
y_upward = [3, 7, 10, 15, 17]
y_downward = [4, 8, 9, 16, 18]
z_upward = [5, 11, 14, 15, 18]
z_downward = [6, 12, 13, 16, 17]
relax_rate = 1.6
pressure_gain = 60.0
sound_speed = 0.5


x_plus = [1, 7, 9, 11, 13]
x_minus = [2, 8, 10, 12, 14]
x_order = x_plus + x_minus
still = [0, 3, 4, 5, 6, 15, 16, 17, 18]
LANES = 128
FACE = 256


def collide_tile(f):
    sums = [None] * 19
    gaps = [None] * 19
    for number in range(1, 19, 2):
        sums[number] = f[number] + f[number + 1]
        gaps[number] = f[number] - f[number + 1]
    density = f[0]
    for number in range(1, 19, 2):
        density = density + sums[number]
    speeds = []
    for axis in range(3):
        total = None
        for number in range(1, 19, 2):
            sign = velocity_list[number][axis]
            if sign == 0:
                continue
            if total is None:
                total = gaps[number]
            elif sign == 1:
                total = total + gaps[number]
            else:
                total = total - gaps[number]
        speeds.append(total)
    inverse = 1.0 / density
    speeds = [speed * inverse for speed in speeds]
    squared = speeds[0] * speeds[0] + speeds[1] * speeds[1] + speeds[2] * speeds[2]
    base = 1.0 - 1.5 * squared
    keep = 1.0 - relax_rate
    out = [None] * 19
    out[0] = keep * f[0] + ((relax_rate * weight_list[0]) * density) * base
    scaled = {}
    thrice = {}
    for weight in sorted(set(weight_list[1:])):
        scaled[weight] = (relax_rate * weight) * density
        thrice[weight] = 3.0 * scaled[weight]
    for number in range(1, 19, 2):
        projected = None
        for axis in range(3):
            sign = velocity_list[number][axis]
            if sign == 0:
                continue
            if projected is None:
                projected = speeds[axis]
            elif sign == 1:
                projected = projected + speeds[axis]
            else:
                projected = projected - speeds[axis]
        weight = weight_list[number]
        even = scaled[weight] * (base + 4.5 * (projected * projected))
        odd = thrice[weight] * projected
        out[number] = keep * f[number] + (even + odd)
        out[number + 1] = keep * f[number + 1] + (even - odd)
    return out


def lane_of(shape):
    return lax.broadcasted_iota(jnp.int32, shape, 1)


def turned(value, amount):
    amount = amount % value.shape[1]
    return value if amount == 0 else pltpu.roll(value, amount, 1)


def pushed(value, low, high, sign):
    if sign == 1:
        return jnp.concatenate([low, value[:-1]], axis=0)
    return jnp.concatenate([value[1:], high], axis=0)


def shift_of(number):
    return velocity_list[number][1] * BS + velocity_list[number][2]


face_sets = [y_downward, y_upward, z_downward, z_upward]


def pack_tile(values, tile, tiles, chosen_numbers, columns, rows):
    depth = values[chosen_numbers[0]].shape[0]
    spot = lane_of((depth, LANES)) % BS
    quarter = lane_of((depth, LANES)) // BS
    u = tile % 4
    for side, (chosen, begin) in enumerate([(z_downward, 0), (z_upward, BS - 1)]):
        for j, number in enumerate(chosen):
            if number in chosen_numbers:
                moved = turned(values[number] - weight_list[number], 8 * u + j - begin)
                columns[side] = jnp.where(spot == 8 * u + j, moved, columns[side])
    for side, (chosen, at, begin) in enumerate(
        [(y_downward, 0, 0), (y_upward, tiles - 1, LANES - BS)]
    ):
        if tile != at:
            continue
        for j, number in enumerate(chosen):
            if number in chosen_numbers:
                moved = turned(values[number] - weight_list[number], j % 4 * BS - begin)
                rows[side][j // 4] = jnp.where(quarter == j % 4, moved, rows[side][j // 4])


def collide_all(field_ref, rolled_ref, moving_ref, draft_ref):
    depth = field_ref.shape[1]
    tiles = field_ref.shape[2] // LANES
    blank = jnp.zeros((depth, LANES), jnp.float32)
    rows = [[blank, blank], [blank, blank]]
    for half in range(tiles // 4):
        columns = [blank, blank]
        for u in range(4):
            tile = half * 4 + u
            lanes = slice(tile * LANES, (tile + 1) * LANES)
            out = collide_tile([field_ref[number, :, lanes] for number in range(19)])
            for number in range(19):
                if number in still:
                    rolled_ref[tile + 1, number] = turned(out[number], shift_of(number))
                else:
                    moving_ref[tile, x_order.index(number)] = out[number]
            pack_tile(out, tile, tiles, still, columns, rows)
        for side in range(2):
            draft_ref[2 + side, :, half * LANES : (half + 1) * LANES] = columns[side]
    for side in range(2):
        for half in range(2):
            draft_ref[side, :, half * LANES : (half + 1) * LANES] = rows[side][half]


def keep_rim(rim_ref, number, tile, value):
    depth = value.shape[0]
    tiles = rim_ref.shape[1] // 2
    rim_ref[number, tile : tile + 1, :] = value[depth - 1 : depth]
    rim_ref[number, tiles + tile : tiles + tile + 1, :] = value[0:1]


def collide_rim(rim_ref, edge_ref):
    tiles = rim_ref.shape[1] // 2
    out = collide_tile([rim_ref[number] for number in range(19)])
    for place, number in enumerate(x_plus):
        edge_ref[0, place] = out[number][0:tiles]
    for place, number in enumerate(x_minus):
        edge_ref[1, place] = out[number][tiles : 2 * tiles]


def shifted(moving_ref, near_ref, tile, number):
    place = x_order.index(number)
    low = near_ref[0, place % 5, tile : tile + 1, :]
    high = near_ref[1, place % 5, tile : tile + 1, :]
    return pushed(moving_ref[tile, place], low, high, velocity_list[number][0])


def pack_moving(moving_ref, near_ref, draft_ref, piece_ref):
    tiles = moving_ref.shape[0]
    crossing = x_order[1:5] + x_order[6:]

    def draft(piece, half):
        return draft_ref[piece, :, half * LANES : (half + 1) * LANES]

    rows = [[draft(side, half) for half in range(2)] for side in range(2)]
    for half in range(tiles // 4):
        columns = [draft(2 + side, half) for side in range(2)]
        for u in range(4):
            tile = half * 4 + u
            values = {}
            for number in crossing:
                if velocity_list[number][1] == 0 or tile in (0, tiles - 1):
                    values[number] = shifted(moving_ref, near_ref, tile, number)
            pack_tile(values, tile, tiles, list(values), columns, rows)
        for side in range(2):
            piece_ref[2 + side, :, half * LANES : (half + 1) * LANES] = columns[side].astype(jnp.bfloat16)
    for side in range(2):
        for half in range(2):
            piece_ref[side, :, half * LANES : (half + 1) * LANES] = rows[side][half].astype(jnp.bfloat16)


def roll_moving(rolled_ref, moving_ref, near_ref):
    tiles = moving_ref.shape[0]
    for tile in range(tiles):
        for number in x_order:
            value = shifted(moving_ref, near_ref, tile, number)
            rolled_ref[tile + 1, number] = turned(value, shift_of(number))


def finish_step(face, edge, got_ref, rolled_ref, field_ref, rim_ref, density_ref, last):
    depth = field_ref.shape[1]
    tiles = field_ref.shape[2] // LANES
    lane = lane_of((depth, LANES))
    spot = lane % BS

    def arrived(source, half):
        return got_ref[source, :, half * LANES : (half + 1) * LANES].astype(jnp.float32)

    corners = {15: (0, 0, 1), 17: (1, 1, 31), 18: (2, 1, 65), 16: (3, 0, 31)}
    corner_lane = {15: 0, 17: BS - 1, 18: LANES - BS, 16: LANES - 1}
    for piece, source, pad, begin in [(1, face[0], 0, 0), (0, face[1], tiles + 1, LANES - BS)]:
        halves = [arrived(source, half) for half in range(2)]
        for j, number in enumerate(face_sets[piece]):
            shift_z = velocity_list[number][2]
            value = turned(halves[j // 4], begin + shift_z - j % 4 * BS)
            if number in corners:
                which, half, amount = corners[number]
                corner = turned(arrived(edge[which], half), amount)
                value = jnp.where(lane == corner_lane[number], corner, value)
            rolled_ref[pad, number] = value + weight_list[number]
    columns = {}
    for piece, source, rim in [(3, face[2], 0), (2, face[3], BS - 1)]:
        chosen = face_sets[piece]
        halves = [arrived(source, half) for half in range(2)]
        for tile in range(tiles):
            for j, number in enumerate(chosen):
                shift_y = velocity_list[number][1]
                amount = rim - 8 * (tile % 4) - j + BS * shift_y
                column = turned(halves[tile // 4], amount) + weight_list[number]
                value = jnp.where(spot == rim, column, rolled_ref[tile + 1, number])
                if shift_y != 0:
                    rolled_ref[tile + 1, number] = value
                else:
                    columns[tile, number] = value
                    field_ref[number, :, tile * LANES : (tile + 1) * LANES] = value
    for tile in range(tiles):
        lanes = slice(tile * LANES, (tile + 1) * LANES)
        total = None
        for number, (_, shift_y, shift_z) in enumerate(velocity_list):
            if shift_y == 0 and shift_z != 0:
                value = field_ref[number, :, lanes]
            else:
                value = rolled_ref[tile + 1, number]
                if shift_y == 1:
                    value = jnp.where(lane < BS, rolled_ref[tile, number], value)
                elif shift_y == -1:
                    value = jnp.where(lane >= LANES - BS, rolled_ref[tile + 2, number], value)
                field_ref[number, :, lanes] = value
            if not last:
                keep_rim(rim_ref, number, tile, value)
            total = value if total is None else total + value
        density_ref[:, lanes] = total


def joined(left, right, left_axis, right_axis):
    return lax.dot_general(
        left.astype(jnp.bfloat16), right.astype(jnp.bfloat16),
        (((left_axis,), (right_axis,)), ((), ())), preferred_element_type=jnp.float32,
    )


def rows_of(shape):
    return lax.broadcasted_iota(jnp.int32, shape, 0)


def route(blocks, owner_ref, count, history_ref, select_ref, send_ref):
    slots = owner_ref.shape[1]
    room = send_ref.shape[1]
    width = history_ref.shape[1]
    owner = owner_ref[...]
    alive = lane_of((1, slots)) < count
    target = lax.shift_right_logical(owner, P_OWN.bit_length() - 1)
    spot = lax.bitwise_and(owner, P_OWN - 1)
    member = jnp.where((rows_of((blocks, slots)) == target) & alive, 1.0, 0.0)
    earlier = jnp.where(rows_of((slots, slots)) < lane_of((slots, slots)), 1.0, 0.0)
    before = joined(member, earlier, 1, 0)
    order = jnp.sum(before * member, axis=0, keepdims=True).astype(jnp.int32)
    label = jnp.where(alive, target * room + order, -1)
    select = jnp.where(rows_of((blocks * room, slots)) == label, 1.0, 0.0)
    select_ref[...] = select.astype(jnp.bfloat16)
    moved = joined(select, history_ref[...], 1, 0)
    spots = joined(select, jnp.where(rows_of((P_OWN, slots)) == spot, 1.0, 0.0), 1, 1)
    for block in range(blocks):
        rows = slice(block * room, (block + 1) * room)
        send_ref[block, :, 0:width] = moved[rows].astype(jnp.bfloat16)
        send_ref[block, :, width : width + P_OWN] = spots[rows].astype(jnp.bfloat16)


def unpacked(got_ref, flat_ref):
    blocks, room = got_ref.shape[0], got_ref.shape[1]
    for block in range(blocks):
        flat_ref[block * room : (block + 1) * room, :] = got_ref[block].astype(jnp.float32)


def settle_history(got_ref, flat_ref, choose_ref, table_ref, partial_ref):
    unpacked(got_ref, flat_ref)
    choose = flat_ref[:, 2 * SAMPLES : 2 * SAMPLES + P_OWN].astype(jnp.bfloat16)
    choose_ref[...] = choose
    owned = joined(choose, flat_ref[:, 0 : 2 * SAMPLES], 0, 0)
    for field in range(2):
        partial_ref[:, field * 2 * BINS : (field + 1) * 2 * BINS] = joined(
            owned[:, field * SAMPLES : (field + 1) * SAMPLES], table_ref[...], 1, 0
        )


def reading_of(density_ref, cell_ref, probe_ref):
    depth = density_ref.shape[0]
    count = density_ref.shape[1]
    excess = density_ref[...] - 1.0
    parts = []
    for _ in range(3):
        part = excess.astype(jnp.bfloat16).astype(jnp.float32)
        parts.append(part)
        excess = excess - part
    found = joined(jnp.concatenate(parts, axis=0), cell_ref[...], 1, 0)
    layers = found[0:depth] + found[depth : 2 * depth] + found[2 * depth : 3 * depth]
    layer = lax.div(probe_ref[...], count)
    mine = rows_of(layers.shape) == layer
    return jnp.sum(jnp.where(mine, layers, 0.0), axis=0, keepdims=True)


def prepare_waves(spot_got, listen_ref, wave_ref):
    ring = spot_got.shape[0]
    tiles, width = wave_ref.shape[0], wave_ref.shape[3]
    angle_step = 2.0 * math.pi / SAMPLES / sound_speed
    for owner in range(ring):
        columns = spot_got[owner].T[0:P_OWN]
        for group in range(P_OWN // 8):
            rows = slice(group * 8, (group + 1) * 8)
            into = slice(owner * P_OWN + group * 8, owner * P_OWN + (group + 1) * 8)
            for tile in range(tiles):
                lanes = slice(tile * width, (tile + 1) * width)
                distance_sq = None
                facing = None
                for axis in range(3):
                    offset = listen_ref[axis : axis + 1, lanes] - columns[rows, axis : axis + 1]
                    square = offset * offset
                    along = columns[rows, axis + 3 : axis + 4] * offset
                    distance_sq = square if distance_sq is None else distance_sq + square
                    facing = along if facing is None else facing + along
                distance = jnp.sqrt(distance_sq)
                far = facing / (4.0 * math.pi * sound_speed * distance_sq)
                angle = angle_step * distance
                turn = jnp.cos(angle)
                wave_ref[tile, 0, into] = far
                wave_ref[tile, 1, into] = jnp.zeros_like(far)
                wave_ref[tile, 2, into] = far * turn
                wave_ref[tile, 3, into] = far * jnp.sin(angle)
                wave_ref[tile, 4, into] = 2.0 * turn
                wave_ref[tile, 5, into] = sound_speed / distance


def weigh_panels(done_got, weight_ref):
    ring = done_got.shape[0]
    panels = ring * P_OWN
    values = jnp.concatenate([done_got[owner].astype(jnp.float32) for owner in range(ring)], axis=0).T
    press_real, press_imag, rate_real, rate_imag = [
        values[part * BINS : (part + 1) * BINS] for part in range(4)
    ]
    lines = [
        [rate_real, rate_imag, press_real, press_imag],
        [rate_imag, -rate_real, press_imag, -press_real],
    ]
    for row, line in enumerate(lines):
        for part, value in enumerate(line):
            for start in range(0, panels, LANES):
                at = (part * panels + start) // LANES
                weight_ref[at, pl.ds(row, BINS, stride=8), :] = value[:, start : start + LANES]


def radiate_tile(wave_ref, weight_ref, first_ref, second_ref, sums_ref, total_ref):
    panels = wave_ref.shape[1]
    span = first_ref.shape[0]
    for first in range(0, BINS, span):
        held_ref = second_ref if first // span % 2 else first_ref
        for start in range(0, panels, 32):
            rows = slice(start, start + 32)
            old_cos, old_sin, now_cos, now_sin, twice, ratio = [wave_ref[i, rows] for i in range(6)]
            nearer = ratio.astype(jnp.bfloat16)
            for number in range(span):
                pair = [now_cos.astype(jnp.bfloat16), now_sin.astype(jnp.bfloat16)]
                for part, value in enumerate(pair + [nearer * value for value in pair]):
                    into = slice(part * panels + start, part * panels + start + 32)
                    held_ref[number, into] = value
                if first + number + 1 < BINS:
                    old_cos, now_cos = now_cos, twice * now_cos - old_cos
                    old_sin, now_sin = now_sin, twice * now_sin - old_sin
            if first + span < BINS:
                for i, value in enumerate([old_cos, old_sin, now_cos, now_sin]):
                    wave_ref[i, rows] = value
        for number in range(span):
            rows = slice((first + number) * 8, (first + number + 1) * 8)
            weights = jnp.concatenate(
                [weight_ref[at, rows, :] for at in range(weight_ref.shape[0])], axis=1
            )
            found = joined(weights, held_ref[number], 1, 0)
            for part in range(sums_ref.shape[0]):
                sums_ref[part, rows, :] = found[:, part * LANES : (part + 1) * LANES]
    for part in range(sums_ref.shape[0]):
        total_ref[part, 0:BINS] = sums_ref[part, pl.ds(0, BINS, stride=8), :]
        total_ref[part, BINS : 2 * BINS] = sums_ref[part, pl.ds(1, BINS, stride=8), :]


def window_kernel(
    blocks, ring, face_ref, rim_face_ref, count_ref, start_hbm, owner_ref, probe_ref, history_ref,
    place_ref, normal_ref, listen_ref, table_ref, tail_ref, final_hbm, out_ref,
    field_ref, density_ref, rolled_ref, moving_ref, rim_ref, edge_ref, near_ref, draft_ref, piece_ref,
    send_ref, got_even, got_odd, select_ref, cell_ref, past_send, past_got, flat_ref, choose_ref,
    partial_ref, fresh_ref, fresh_send, fresh_got, fresh_flat, done_ref, done_got, spot_ref, spot_got,
    wave_ref, weight_ref, first_ref, second_ref, sums_ref, total_ref, part_send, part_got,
    edge_send, edge_got, send_sem, got_sem, past_send_sem, past_got_sem, fresh_send_sem, fresh_got_sem,
    done_send_sem, done_got_sem, spot_send_sem, spot_got_sem,
    part_send_sem, part_got_sem, local_sem,
):
    mesh_ids = pl.DeviceIdType.MESH
    me = lax.axis_index("blk")
    side = lax.axis_index("obs")
    right = lax.rem(side + 1, ring)
    left = lax.rem(side + ring - 1, ring)
    barrier = pltpu.get_barrier_semaphore()
    slots = owner_ref.shape[1]

    def greet(distance, carry):
        peer = lax.rem(me + distance, blocks)
        pl.semaphore_signal(barrier, inc=1, device_id=(peer, side), device_id_type=mesh_ids)
        return carry

    for distance in range(1, ring):
        beside = lax.rem(side + distance, ring)
        pl.semaphore_signal(barrier, inc=1, device_id=(me, beside), device_id_type=mesh_ids)
    lax.fori_loop(1, blocks, greet, 0)
    face = [face_ref[0, k] for k in range(4)]
    edge = [rim_face_ref[0, k] for k in range(4)]
    load = pltpu.make_async_copy(start_hbm, field_ref, local_sem.at[0])
    load.start()
    route(blocks, owner_ref, count_ref[0], history_ref, select_ref, past_send)
    cell = lax.rem(probe_ref[...], field_ref.shape[2])
    cell_ref[...] = jnp.where(rows_of(cell_ref.shape) == cell, 1.0, 0.0).astype(jnp.bfloat16)
    spot_ref[...] = jnp.zeros_like(spot_ref)
    spot_ref[0:3, 0:P_OWN] = place_ref[...].astype(jnp.float32)
    spot_ref[3:6, 0:P_OWN] = normal_ref[...].astype(jnp.float32)
    fresh_ref[...] = jnp.zeros_like(fresh_ref)
    load.wait()
    for tile in range(field_ref.shape[2] // LANES):
        for number in range(19):
            lanes = slice(tile * LANES, (tile + 1) * LANES)
            keep_rim(rim_ref, number, tile, field_ref[number, :, lanes])

    def swap(source_of, into_ref, send_sems, got_sems, distance):
        peer = lax.rem(me + distance, blocks)
        return pltpu.make_async_remote_copy(
            src_ref=source_of(distance, peer),
            dst_ref=into_ref.at[me],
            send_sem=send_sems.at[distance],
            recv_sem=got_sems.at[distance],
            device_id=(peer, side),
            device_id_type=mesh_ids,
        )

    def every(action):
        def visit(distance, inner):
            action(distance)
            return inner

        lax.fori_loop(1, blocks, visit, 0)

    def past_copy(distance):
        return swap(lambda _, peer: past_send.at[peer], past_got, past_send_sem, past_got_sem, distance)

    def fresh_copy(distance):
        return swap(lambda _, peer: fresh_send.at[peer], fresh_got, fresh_send_sem, fresh_got_sem, distance)

    def ring_copies(source_ref, into_ref, send_sems, got_sems):
        return [
            pltpu.make_async_remote_copy(
                src_ref=source_ref,
                dst_ref=into_ref.at[side],
                send_sem=send_sems.at[distance],
                recv_sem=got_sems.at[distance],
                device_id=(me, lax.rem(side + distance, ring)),
                device_id_type=mesh_ids,
            )
            for distance in range(1, ring)
        ]

    def note(step):
        gained = pressure_gain * reading_of(density_ref.at[step], cell_ref, probe_ref)
        if step == 0:
            last = jnp.where(lane_of((8, 2 * SAMPLES)) == SAMPLES - 1, 1.0, 0.0)
            before = joined(last, history_ref[...], 1, 1)[0:1]
        else:
            before = fresh_ref[step - 1 : step, :]
        fresh_ref[step : step + 1, :] = gained
        fresh_ref[STEPS + step : STEPS + step + 1, :] = gained - before

    def one_step(step):
        got_ref = got_odd if step % 2 else got_even
        collide_rim(rim_ref, edge_ref)
        if step == 0:
            collide_all(field_ref, rolled_ref, moving_ref, draft_ref)
        if step == 0:
            pl.semaphore_wait(barrier, blocks + ring - 2)
        edges = [
            pltpu.make_async_remote_copy(
                src_ref=edge_ref.at[way],
                dst_ref=near_ref.at[step, way],
                send_sem=edge_send.at[step, way],
                recv_sem=edge_got.at[step, way],
                device_id=(me, beside),
                device_id_type=mesh_ids,
            )
            for way, beside in enumerate([right, left])
        ]
        for copy in edges:
            copy.start()
        if step > 0:
            collide_all(field_ref, rolled_ref, moving_ref, draft_ref)
        for copy in edges:
            copy.wait()
        pack_moving(moving_ref, near_ref.at[step], draft_ref, piece_ref)

        def copy_to(distance):
            return swap(
                lambda number, _: send_ref.at[number], got_ref, send_sem.at[step], got_sem.at[step], distance
            )

        def begin(distance):
            peer = lax.rem(me + distance, blocks)
            up = (peer == face[1]) | (peer == edge[2]) | (peer == edge[3])
            piece = jnp.where(peer == face[3], 3, jnp.where(peer == face[2], 2, up.astype(jnp.int32)))
            send_ref[distance] = piece_ref[piece]
            copy_to(distance).start()

        every(begin)
        roll_moving(rolled_ref, moving_ref, near_ref.at[step])
        if step == 0:
            every(lambda distance: past_copy(distance).start())
            for copy in ring_copies(spot_ref, spot_got, spot_send_sem, spot_got_sem):
                copy.start()
            past_got[me] = past_send[me]
            spot_got[side] = spot_ref[...]
        else:
            note(step - 1)
        if step == 1:
            for copy in ring_copies(spot_ref, spot_got, spot_send_sem, spot_got_sem):
                copy.wait()
            prepare_waves(spot_got, listen_ref, wave_ref)
        if step == 2:
            every(lambda distance: past_copy(distance).wait())
            settle_history(past_got, flat_ref, choose_ref, table_ref, partial_ref)
        every(lambda distance: copy_to(distance).wait())
        finish_step(
            face, edge, got_ref, rolled_ref, field_ref, rim_ref, density_ref.at[step], step == STEPS - 1
        )

    for step in range(STEPS):
        one_step(step)
    unload = pltpu.make_async_copy(field_ref, final_hbm, local_sem.at[1])
    unload.start()
    note(STEPS - 1)
    fresh = joined(select_ref[...], fresh_ref[...], 1, 1)
    room = fresh_send.shape[1]
    for block in range(blocks):
        fresh_send[block] = fresh[block * room : (block + 1) * room].astype(jnp.bfloat16)
    every(lambda distance: fresh_copy(distance).start())
    fresh_got[me] = fresh_send[me]
    every(lambda distance: fresh_copy(distance).wait())
    unpacked(fresh_got, fresh_flat)
    newest = joined(choose_ref[...], fresh_flat[...], 0, 0)
    total = partial_ref[...] + joined(newest, tail_ref[...], 1, 0)
    done_ref[...] = total.astype(jnp.bfloat16)
    copies = ring_copies(done_ref, done_got, done_send_sem, done_got_sem)
    for copy in copies:
        copy.start()
    done_got[side] = done_ref[...]
    for copy in copies:
        copy.wait()
    weigh_panels(done_got, weight_ref)
    chunk = out_ref.shape[0]
    tiles = wave_ref.shape[0]
    share = wave_ref.shape[3] // chunk

    def part_copy(peer):
        distance = lax.rem(peer - me + blocks, blocks)
        return pltpu.make_async_remote_copy(
            src_ref=part_send.at[peer],
            dst_ref=part_got.at[me],
            send_sem=part_send_sem.at[distance],
            recv_sem=part_got_sem.at[distance],
            device_id=(peer, side),
            device_id_type=mesh_ids,
        )

    def one_tile(turn, carry):
        tile = lax.rem(me // share + 1 + turn, tiles)
        radiate_tile(wave_ref.at[tile], weight_ref, first_ref, second_ref, sums_ref, total_ref)
        each = LANES // chunk
        for part in range(total_ref.shape[0]):
            both = total_ref[part].T
            for number in range(each):
                rows = slice(number * chunk, (number + 1) * chunk)
                part_send[tile * share + part * each + number] = both[rows]

        def launch(number, inner):
            peer = tile * share + number

            @pl.when(peer != me)
            def _():
                part_copy(peer).start()

            return inner

        lax.fori_loop(0, share, launch, 0)
        return carry

    lax.fori_loop(0, tiles, one_tile, 0)
    part_got[me] = part_send[me]
    every(lambda distance: part_copy(lax.rem(me + distance, blocks)).wait())
    out_ref[...] = jnp.sum(part_got[...], axis=0)
    unload.wait()


def transform_tables():
    moments = np.arange(SAMPLES)[:, None]
    harmonics = np.arange(BINS)[None, :] + 1
    turns = moments * harmonics % SAMPLES
    phases = turns.astype(np.float32) * np.float32(2.0 * math.pi / SAMPLES)
    table = np.concatenate([np.cos(phases), -np.sin(phases)], axis=1).astype(jnp.bfloat16)
    past = np.zeros_like(table)
    past[STEPS:] = table[: SAMPLES - STEPS]
    tail = np.zeros((LANES, 4 * BINS), table.dtype)
    for field in range(2):
        rows = slice(field * STEPS, (field + 1) * STEPS)
        tail[rows, field * 2 * BINS : (field + 1) * 2 * BINS] = table[SAMPLES - STEPS :]
    return jnp.asarray(past), jnp.asarray(tail)


def body(
    populations,
    block_faces,
    block_edges,
    probe_cell,
    history,
    panel_count,
    panel_owner,
    panel_pos,
    panel_normal,
    observers,
):
    blocks = lax.axis_size("blk")
    lattice_state = populations[0]
    slab_depth = lattice_state.shape[1]
    lane_count = lattice_state.shape[2]
    ring = lax.axis_size("obs")
    tiles = lane_count // LANES
    vmem = pl.BlockSpec(memory_space=pltpu.VMEM)
    smem = pl.BlockSpec(memory_space=pltpu.SMEM)
    anywhere = pl.BlockSpec(memory_space=pl.ANY)
    wide = jnp.float32
    half = jnp.bfloat16
    slots = panel_owner.shape[0]
    room = -(-slots // blocks)
    past, tail = transform_tables()
    dma = pltpu.SemaphoreType.DMA
    listeners = observers.shape[1]
    chunk = listeners // blocks
    width = min(2 * LANES, listeners)
    lattice_state, spectrum = pl.pallas_call(
        functools.partial(window_kernel, blocks, ring),
        out_shape=[
            jax.ShapeDtypeStruct((19, slab_depth, lane_count), wide),
            jax.ShapeDtypeStruct((chunk, 2 * BINS), wide),
        ],
        in_specs=[smem] * 3 + [anywhere] + [vmem] * 8,
        out_specs=[anywhere, vmem],
        scratch_shapes=[
            pltpu.VMEM((19, slab_depth, lane_count), wide),
            pltpu.VMEM((STEPS, slab_depth, lane_count), wide),
            pltpu.VMEM((tiles + 2, 19, slab_depth, LANES), wide),
            pltpu.VMEM((tiles, len(x_order), slab_depth, LANES), wide),
            pltpu.VMEM((19, 2 * tiles, LANES), wide),
            pltpu.VMEM((2, 5, tiles, LANES), wide),
            pltpu.VMEM((STEPS, 2, 5, tiles, LANES), wide),
            pltpu.VMEM((4, slab_depth, FACE), wide),
            pltpu.VMEM((4, slab_depth, FACE), half),
            pltpu.VMEM((blocks, slab_depth, FACE), half),
            pltpu.VMEM((blocks, slab_depth, FACE), half),
            pltpu.VMEM((blocks, slab_depth, FACE), half),
            pltpu.VMEM((blocks * room, slots), half),
            pltpu.VMEM((lane_count, slots), half),
            pltpu.VMEM((blocks, room, 5 * LANES), half),
            pltpu.VMEM((blocks, room, 5 * LANES), half),
            pltpu.VMEM((blocks * room, 5 * LANES), wide),
            pltpu.VMEM((blocks * room, P_OWN), half),
            pltpu.VMEM((P_OWN, 4 * BINS), wide),
            pltpu.VMEM((LANES, slots), wide),
            pltpu.VMEM((blocks, room, LANES), half),
            pltpu.VMEM((blocks, room, LANES), half),
            pltpu.VMEM((blocks * room, LANES), wide),
            pltpu.VMEM((P_OWN, 4 * BINS), half),
            pltpu.VMEM((ring, P_OWN, 4 * BINS), half),
            pltpu.VMEM((8, LANES), wide),
            pltpu.VMEM((ring, 8, LANES), wide),
            pltpu.VMEM((listeners // width, 6, ring * P_OWN, width), wide),
            pltpu.VMEM((4 * ring * P_OWN // LANES, BINS * 8 + 8, LANES), wide),
            pltpu.VMEM((8, 4 * ring * P_OWN, width), half),
            pltpu.VMEM((8, 4 * ring * P_OWN, width), half),
            pltpu.VMEM((width // LANES, BINS * 8 + 8, LANES), wide),
            pltpu.VMEM((width // LANES, 2 * BINS, LANES), wide),
            pltpu.VMEM((blocks, chunk, 2 * BINS), wide),
            pltpu.VMEM((blocks, chunk, 2 * BINS), wide),
        ]
        + [dma((STEPS, 2))] * 2
        + [dma((STEPS, blocks))] * 2
        + [dma((blocks,))] * 4
        + [dma((ring,))] * 4
        + [dma((blocks,))] * 2
        + [dma((2,))],
        compiler_params=pltpu.CompilerParams(collective_id=0, has_side_effects=True),
    )(
        block_faces, block_edges, panel_count, lattice_state, panel_owner[None], probe_cell[None],
        history, panel_pos, panel_normal, observers, past, tail,
    )
    populations_out = lattice_state.reshape(1, 19, slab_depth, lane_count)
    return (populations_out, spectrum[None])


def solution(mesh):
    placed = (
        P("blk", None, "obs", None),
        P("blk", None),
        P("blk", None),
        P(("blk", "obs")),
        P(("blk", "obs"), None),
        P(("blk", "obs")),
        P(("blk", "obs")),
        P(None, ("blk", "obs")),
        P(None, ("blk", "obs")),
        P(None, "obs"),
    )
    return jax.shard_map(
        body,
        mesh=mesh,
        in_specs=placed,
        out_specs=(P("blk", None, "obs", None), P("obs", "blk", None)),
        check_vma=False,
    )
```
